8 devices in a mesh: dp: 1 (over z), cp: 8 (over y, x, core).
Axes of the slice: x: 2, y: 2, z: 1, core: 2. Of those that a mesh axis runs over, the one named last changes fastest.
Arguments:
- x_in: bfloat16 [1024, 3072], P(('dp', 'cp'))
- d_y: bfloat16 [1024, 3072], P(('dp', 'cp'))
- w_q: bfloat16 [3072, 24, 128], replicated
- w_k: bfloat16 [3072, 8, 128], replicated
- w_v: bfloat16 [3072, 8, 128], replicated
- w_o: bfloat16 [24, 128, 3072], replicated
Outputs:
- output: bfloat16 [1024, 3072], P(('dp', 'cp'))
All inputs are finite; a program needn't handle non-finite values.
Results may differ from the reference program's by a relative error of at most 0.0114857.
Values are sent between devices in bfloat16 or wider.
A program may use at most 1 GiB of HBM per device.

```python
import jax
import jax.numpy as jnp
from jax import lax

D_MODEL = 3072
Q_HEADS = 24
KV_HEADS = 8
HEAD_DIM = 128
TOK_DEV = 128
CP_SIZE = 8
ROW_BLOCK = 32
SEQ_LEN = CP_SIZE * TOK_DEV
SEG_LEN = TOK_DEV // 2
Q_GROUP = Q_HEADS // KV_HEADS
SCORE_SCALE = HEAD_DIM ** -0.5
DY_SCALE = (SEQ_LEN / 16) ** 0.5


def token_positions(row_ids):
    dev_idx = row_ids // TOK_DEV
    row_off = row_ids % TOK_DEV
    seg_idx = jnp.where(row_off < SEG_LEN, dev_idx, 2 * CP_SIZE - 1 - dev_idx)
    return seg_idx * SEG_LEN + row_off % SEG_LEN


def setup_inputs(seed: int = 0, part: int = 0) -> dict:
    part_key = jax.random.fold_in(jax.random.key(seed), part)
    key_x, key_dy = jax.random.split(part_key)
    key_q, key_k, key_v, key_o = jax.random.split(jax.random.key(seed + 1), 4)
    x_in = jax.random.normal(key_x, (SEQ_LEN, D_MODEL), jnp.float32).astype(jnp.bfloat16)
    d_y = (jax.random.normal(key_dy, (SEQ_LEN, D_MODEL), jnp.float32) * DY_SCALE).astype(jnp.bfloat16)
    w_q = (jax.random.normal(key_q, (D_MODEL, Q_HEADS, HEAD_DIM), jnp.float32) * D_MODEL ** -0.5).astype(jnp.bfloat16)
    w_k = (jax.random.normal(key_k, (D_MODEL, KV_HEADS, HEAD_DIM), jnp.float32) * D_MODEL ** -0.5).astype(jnp.bfloat16)
    w_v = (jax.random.normal(key_v, (D_MODEL, KV_HEADS, HEAD_DIM), jnp.float32) * D_MODEL ** -0.5).astype(jnp.bfloat16)
    w_o = (jax.random.normal(key_o, (Q_HEADS, HEAD_DIM, D_MODEL), jnp.float32) * (Q_HEADS * HEAD_DIM) ** -0.5).astype(jnp.bfloat16)
    return {"x_in": x_in, "d_y": d_y, "w_q": w_q, "w_k": w_k, "w_v": w_v, "w_o": w_o}


def reference(x_in, d_y, w_q, w_k, w_v, w_o):
    wq_flat = w_q.reshape(D_MODEL, Q_HEADS * HEAD_DIM)
    wk_flat = w_k.reshape(D_MODEL, KV_HEADS * HEAD_DIM)
    wv_flat = w_v.reshape(D_MODEL, KV_HEADS * HEAD_DIM)
    wo_flat = w_o.reshape(Q_HEADS * HEAD_DIM, D_MODEL)
    q_proj = jnp.dot(x_in, wq_flat, preferred_element_type=jnp.float32).astype(jnp.bfloat16)
    k_proj = jnp.dot(x_in, wk_flat, preferred_element_type=jnp.float32).astype(jnp.bfloat16)
    v_proj = jnp.dot(x_in, wv_flat, preferred_element_type=jnp.float32).astype(jnp.bfloat16)
    do_proj = jnp.dot(d_y, wo_flat.T, preferred_element_type=jnp.float32).astype(jnp.bfloat16)
    queries = q_proj.astype(jnp.float32).reshape(SEQ_LEN, KV_HEADS, Q_GROUP, HEAD_DIM)
    key_all = k_proj.astype(jnp.float32).reshape(SEQ_LEN, KV_HEADS, HEAD_DIM)
    val_all = v_proj.astype(jnp.float32).reshape(SEQ_LEN, KV_HEADS, HEAD_DIM)
    d_out = do_proj.astype(jnp.float32).reshape(SEQ_LEN, KV_HEADS, Q_GROUP, HEAD_DIM)
    positions = token_positions(jnp.arange(SEQ_LEN))

    def block_step(acc_pair, blk_idx):
        dk_acc, dv_acc = acc_pair
        row_start = blk_idx * ROW_BLOCK
        q_blk = lax.dynamic_slice_in_dim(queries, row_start, ROW_BLOCK, 0)
        do_blk = lax.dynamic_slice_in_dim(d_out, row_start, ROW_BLOCK, 0)
        pos_blk = lax.dynamic_slice_in_dim(positions, row_start, ROW_BLOCK, 0)
        scores = jnp.einsum("rkge,ske->krgs", q_blk, key_all) * SCORE_SCALE
        causal = pos_blk[None, :, None, None] >= positions[None, None, None, :]
        scores = jnp.where(causal, scores, -jnp.inf)
        lse_blk = jax.nn.logsumexp(scores, axis=-1, keepdims=True)
        prob_blk = jnp.exp(scores - lse_blk).astype(jnp.bfloat16).astype(jnp.float32)
        out_blk = jnp.einsum("krgs,ske->krge", prob_blk, val_all).astype(jnp.bfloat16).astype(jnp.float32)
        row_delta = jnp.einsum("rkge,krge->krg", do_blk, out_blk)
        dp_blk = jnp.einsum("rkge,ske->krgs", do_blk, val_all)
        ds_blk = (prob_blk * (dp_blk - row_delta[..., None])).astype(jnp.bfloat16).astype(jnp.float32)
        dq_blk = (jnp.einsum("krgs,ske->rkge", ds_blk, key_all) * SCORE_SCALE).astype(jnp.bfloat16)
        dk_acc = dk_acc + jnp.einsum("krgs,rkge->ske", ds_blk, q_blk)
        dv_acc = dv_acc + jnp.einsum("krgs,rkge->ske", prob_blk, do_blk)
        return (dk_acc, dv_acc), dq_blk

    zero_acc = jnp.zeros((SEQ_LEN, KV_HEADS, HEAD_DIM), jnp.float32)
    (dk_sum, dv_sum), dq_blocks = lax.scan(block_step, (zero_acc, zero_acc), jnp.arange(SEQ_LEN // ROW_BLOCK))
    d_query = dq_blocks.reshape(SEQ_LEN, Q_HEADS * HEAD_DIM)
    d_key = (dk_sum * SCORE_SCALE).astype(jnp.bfloat16).reshape(SEQ_LEN, KV_HEADS * HEAD_DIM)
    d_value = dv_sum.astype(jnp.bfloat16).reshape(SEQ_LEN, KV_HEADS * HEAD_DIM)
    d_x = jnp.dot(d_query, wq_flat.T, preferred_element_type=jnp.float32)
    d_x = d_x + jnp.dot(d_key, wk_flat.T, preferred_element_type=jnp.float32)
    d_x = d_x + jnp.dot(d_value, wv_flat.T, preferred_element_type=jnp.float32)
    return d_x.astype(jnp.bfloat16)
```

```python
import functools
import math

import jax
import jax.numpy as jnp
from jax import lax
from jax.experimental import pallas as pl
from jax.experimental.pallas import tpu as pltpu
from jax.sharding import PartitionSpec as P

MESH = pl.DeviceIdType.MESH
BF16, F32 = jnp.bfloat16, jnp.float32
NT = (((1,), (1,)), ((), ()))

N_DEV, TOK, SEG = 8, 128, 64
SEQ = N_DEV * TOK
D = 3072
HD = 128
HQ, HKV, G = 24, 8, 3
BQ = 256
NB = SEQ // BQ
C = HD**-0.5
C2 = C * math.log2(math.e)
WO_SLOTS, W_SLOTS = 4, 4
U_DO, U_K, U_V, U_Q = 0, 3, 4, 5


def dot_nt(a, b):
    return lax.dot_general(a, b, NT, preferred_element_type=F32)


def dot(a, b):
    return jnp.dot(a, b, preferred_element_type=F32)


def kernel(x_hbm, dy_hbm, wq_hbm, wk_hbm, wv_hbm, wo_hbm, out_hbm,
           x_v, dy_v, wo_s, w_s, wrel, sbuf, recv, obuf, rin, acc, res,
           s_scr, p_scr, ds_scr, kt, vt, dk_acc, dv_acc,
           io_sem, wo_sem, w_sem, send_sem, recv_sem, osend_sem, orecv_sem, out_sem):
    me = lax.axis_index("cp")
    dp = lax.axis_index("dp")
    chip = me // 2

    barrier = pltpu.get_barrier_semaphore()
    for p in range(1, N_DEV):
        pl.semaphore_signal(barrier, inc=1, device_id=(dp, lax.rem(me + p, N_DEV)), device_id_type=MESH)

    x_cp = pltpu.make_async_copy(x_hbm, x_v, io_sem.at[0])
    dy_cp = pltpu.make_async_copy(dy_hbm, dy_v, io_sem.at[1])

    def wo_copy(s):
        cc = lax.rem(chip + s % 4 + 1, 4)
        slot = s % WO_SLOTS
        return pltpu.make_async_copy(wo_hbm.at[pl.ds(2 * cc, 2), s // 4], wo_s.at[slot], wo_sem.at[slot])

    def wkv_copy(w_hbm, i, slot):
        return pltpu.make_async_copy(w_hbm.at[pl.ds(i * 3, 3)], w_s.at[slot], w_sem.at[slot])

    def wq_copy(i, slot):
        return pltpu.make_async_copy(wq_hbm.at[i], w_s.at[slot], w_sem.at[slot])

    dy_cp.start()
    for s in range(WO_SLOTS):
        wo_copy(s).start()
    x_cp.start()
    for i in range(4):
        wkv_copy(wk_hbm, i, i).start()
    dk_acc[...] = jnp.zeros_like(dk_acc)
    dv_acc[...] = jnp.zeros_like(dv_acc)

    def send_block(unit, dest, val):
        @pl.when(dest != me)
        def _():
            sbuf[unit, dest] = val
            for half, seg in ((0, me), (1, 2 * N_DEV - 1 - me)):
                pltpu.make_async_remote_copy(
                    src_ref=sbuf.at[unit, dest, pl.ds(half * SEG, SEG)],
                    dst_ref=recv.at[unit, pl.ds(pl.multiple_of(seg * SEG, SEG), SEG)],
                    send_sem=send_sem, recv_sem=recv_sem.at[unit],
                    device_id=(dp, dest), device_id_type=MESH).start()

        @pl.when(dest == me)
        def _():
            recv[unit, pl.ds(pl.multiple_of(me * SEG, SEG), SEG), :] = val[:SEG]
            recv[unit, pl.ds(pl.multiple_of((2 * N_DEV - 1 - me) * SEG, SEG), SEG), :] = val[SEG:]

    dy_cp.wait()
    pl.semaphore_wait(barrier, N_DEV - 1)

    def do_step(s, _):
        cc = lax.rem(chip + s % 4 + 1, 4)
        slot = s % WO_SLOTS
        wo_copy(s).wait()
        w = wo_s[slot].reshape(2 * HD, D)
        val = dot_nt(dy_v[...], w).astype(BF16)
        for q in range(2):
            send_block(U_DO + s // 4, 2 * cc + q, val[:, q * HD:(q + 1) * HD])

        @pl.when(s + WO_SLOTS < 12)
        def _():
            wo_copy(s + WO_SLOTS).start()
        return 0

    lax.fori_loop(0, 12, do_step, 0)
    x_cp.wait()

    def relayout_kv(base, w_hbm, nxt, i, _):
        slot = i
        wkv_copy(w_hbm, i, slot).wait()
        blk = w_s[slot].reshape(3 * 256, 8, HD)
        wrel[pl.ds(base, 8), pl.ds(pl.multiple_of(i * 768, 768), 768), :] = jnp.swapaxes(blk, 0, 1)
        nxt(i, slot)
        return 0

    lax.fori_loop(0, 4, functools.partial(relayout_kv, HQ, wk_hbm, lambda i, slot: wkv_copy(wv_hbm, i, slot).start()), 0)
    lax.fori_loop(0, 4, functools.partial(relayout_kv, HQ + HKV, wv_hbm, lambda i, slot: wq_copy(i, slot).start()), 0)

    def kv_step(s, _):
        cc = lax.rem(chip + s % 4 + 1, 4)
        h0 = HQ + 8 * (s // 4) + 2 * cc
        w = jnp.concatenate([wrel[h0], wrel[h0 + 1]], axis=1)
        val = dot(x_v[...], w).astype(BF16)
        for q in range(2):
            send_block(U_K + s // 4, 2 * cc + q, val[:, q * HD:(q + 1) * HD])
        return 0

    lax.fori_loop(0, 8, kv_step, 0)

    def relayout_q(i, _):
        slot = i % W_SLOTS
        wq_copy(i, slot).wait()
        for t in range(3):
            wrel[pl.ds(8 * t, 8), pl.ds(pl.multiple_of(i * 256, 256), 256), :] = jnp.swapaxes(
                w_s[slot].reshape(256, 3, 8, HD)[:, t], 0, 1)

        @pl.when(i + W_SLOTS < 12)
        def _():
            wq_copy(i + W_SLOTS, slot).start()
        return 0

    lax.fori_loop(0, 12, relayout_q, 0)

    def q_step(s, _):
        cc = lax.rem(chip + s % 4 + 1, 4)
        g = s // 4
        h0 = 6 * cc + g
        w = jnp.concatenate([wrel[h0], wrel[h0 + 3]], axis=1)
        val = dot(x_v[...], w).astype(BF16)
        for q in range(2):
            send_block(U_Q + g, 2 * cc + q, val[:, q * HD:(q + 1) * HD])
        return 0

    lax.fori_loop(0, 12, q_step, 0)

    def wait_unit(u):
        part = recv.at[u, pl.ds(0, SEQ - TOK)]
        pltpu.make_async_copy(part, part, recv_sem.at[u]).wait()

    wait_unit(U_K)
    wait_unit(U_V)
    kt[...] = recv[U_K].T
    vt[...] = recv[U_V].T

    def send_out(u, head, seg):
        dest, half = (seg, 0) if seg < N_DEV else (2 * N_DEV - 1 - seg, 1)
        rows = pl.ds(seg * SEG, SEG)

        @pl.when(dest != me)
        def _():
            pltpu.make_async_remote_copy(
                src_ref=obuf.at[u, rows], dst_ref=rin.at[head, pl.ds(half * SEG, SEG)],
                send_sem=osend_sem, recv_sem=orecv_sem.at[u],
                device_id=(dp, dest), device_id_type=MESH).start()

        @pl.when(dest == me)
        def _():
            rin[head, half * SEG:(half + 1) * SEG, :] = obuf[u, rows, :]

    def attn_head(g, _):
        wait_unit(U_DO + g)
        wait_unit(U_Q + g)
        for b in reversed(range(NB)):
            n = (b + 1) * BQ
            rows = slice(b * BQ, (b + 1) * BQ)
            qb = recv[U_Q + g, rows, :]
            dob = recv[U_DO + g, rows, :]
            mx = None
            for kc in range(b + 1):
                ks = slice(kc * BQ, (kc + 1) * BQ)
                s = dot_nt(recv[U_K, ks, :], qb)
                if kc == b:
                    key = lax.broadcasted_iota(jnp.int32, (BQ, BQ), 0)
                    qry = lax.broadcasted_iota(jnp.int32, (BQ, BQ), 1)
                    s = jnp.where(key <= qry, s, -jnp.inf)
                s_scr[ks, :] = s
                mc = jnp.max(s.reshape(BQ // 8, 8, BQ), axis=0)
                mx = mc if mx is None else jnp.maximum(mx, mc)
            m2 = jnp.max(mx, axis=0, keepdims=True) * C2
            ls = None
            for kc in range(b + 1):
                ks = slice(kc * BQ, (kc + 1) * BQ)
                e = jnp.exp2(s_scr[ks, :] * C2 - m2)
                lc = jnp.sum(e.reshape(BQ // 8, 8, BQ), axis=0)
                ls = lc if ls is None else ls + lc
            lse2 = m2 + jnp.log2(jnp.sum(ls, axis=0, keepdims=True))
            for kc in range(b + 1):
                ks = slice(kc * BQ, (kc + 1) * BQ)
                p_scr[ks, :] = jnp.exp2(s_scr[ks, :] * C2 - lse2).astype(BF16)
            ot = dot(vt[:, :n], p_scr[:n, :]).astype(BF16)
            dot_t = dob.T
            delta = jnp.sum(dot_t.astype(F32) * ot.astype(F32), axis=0, keepdims=True)
            for kc in range(b + 1):
                ks = slice(kc * BQ, (kc + 1) * BQ)
                dpt = dot_nt(recv[U_V, ks, :], dob)
                ds = (p_scr[ks, :].astype(F32) * (dpt - delta)).astype(BF16)
                ds_scr[ks, :] = ds
                dk_acc[ks, :] += dot(ds, qb)
                dv_acc[ks, :] += dot(p_scr[ks, :], dob)
            dqt = (dot(kt[:, :n], ds_scr[:n, :]) * C).astype(BF16)
            obuf[g, rows, :] = dqt.T
            for i in range(BQ // SEG):
                send_out(g, G * me + g, b * (BQ // SEG) + i)

            @pl.when(g == G - 1)
            def _():
                obuf[3, rows, :] = (dk_acc[rows, :] * C).astype(BF16)
                obuf[4, rows, :] = dv_acc[rows, :].astype(BF16)
                for i in range(BQ // SEG):
                    send_out(3, HQ + me, b * (BQ // SEG) + i)
                    send_out(4, HQ + HKV + me, b * (BQ // SEG) + i)
        return 0

    lax.fori_loop(0, G, attn_head, 0)

    ND = 512
    for u in range(5):
        part = obuf.at[u, pl.ds(0, SEQ - TOK)]
        pltpu.make_async_copy(part, part, orecv_sem.at[u]).wait()
        heads = [G * j + u for j in range(8)] if u < 3 else [HQ + 8 * (u - 3) + j for j in range(8)]

        def dx_step(i, _, u=u, heads=heads):
            cols = pl.ds(pl.multiple_of(i * ND, ND), ND)
            lhs = jnp.concatenate([rin[h] for h in heads], axis=1)
            rhs = jnp.concatenate([wrel[h, cols, :] for h in heads], axis=1)
            t = dot_nt(lhs, rhs)
            if u > 0:
                t = t + acc[:, cols]
            if u < 4:
                acc[:, cols] = t
            else:
                res[:, cols] = t.astype(BF16)
                pltpu.make_async_copy(res.at[:, cols], out_hbm.at[:, cols], out_sem).start()
            return 0

        lax.fori_loop(0, D // ND, dx_step, 0)

    part = sbuf.at[pl.ds(0, 7)]
    pltpu.make_async_copy(part, part, send_sem).wait()
    part = obuf.at[:, pl.ds(0, SEQ - TOK)]
    pltpu.make_async_copy(part, part, osend_sem).wait()
    pltpu.make_async_copy(res, out_hbm, out_sem).wait()


def solution(mesh):
    row_spec = P(("dp", "cp"), None)

    def device_fn(x_in, d_y, w_q, w_k, w_v, w_o):
        dma = pltpu.SemaphoreType.DMA
        return pl.pallas_call(
            kernel,
            out_shape=jax.ShapeDtypeStruct((TOK, D), BF16),
            in_specs=[pl.BlockSpec(memory_space=pl.ANY)] * 6,
            out_specs=pl.BlockSpec(memory_space=pl.ANY),
            scratch_shapes=[
                pltpu.VMEM((TOK, D), BF16),
                pltpu.VMEM((TOK, D), BF16),
                pltpu.VMEM((WO_SLOTS, 2, HD, D), BF16),
                pltpu.VMEM((W_SLOTS, 3, 256, 8, HD), BF16),
                pltpu.VMEM((HQ + 2 * HKV, D, HD), BF16),
                pltpu.VMEM((8, N_DEV, TOK, HD), BF16),
                pltpu.VMEM((8, SEQ, HD), BF16),
                pltpu.VMEM((5, SEQ, HD), BF16),
                pltpu.VMEM((HQ + 2 * HKV, TOK, HD), BF16),
                pltpu.VMEM((TOK, D), F32),
                pltpu.VMEM((TOK, D), BF16),
                pltpu.VMEM((SEQ, BQ), F32),
                pltpu.VMEM((SEQ, BQ), BF16),
                pltpu.VMEM((SEQ, BQ), BF16),
                pltpu.VMEM((HD, SEQ), BF16),
                pltpu.VMEM((HD, SEQ), BF16),
                pltpu.VMEM((SEQ, HD), F32),
                pltpu.VMEM((SEQ, HD), F32),
                dma((2,)), dma((WO_SLOTS,)), dma((W_SLOTS,)),
                dma, dma((8,)), dma, dma((5,)), dma,
            ],
            compiler_params=pltpu.CompilerParams(
                collective_id=0, has_side_effects=True, vmem_limit_bytes=67_043_328),
        )(x_in, d_y, w_q.reshape(12, 3, 256, 8, HD),
          w_k.reshape(12, 256, 8, HD), w_v.reshape(12, 256, 8, HD),
          w_o.reshape(8, 3, HD, D))

    return jax.shard_map(device_fn, mesh=mesh, in_specs=(row_spec, row_spec, P(), P(), P(), P()),
                         out_specs=row_spec, check_vma=False)
```

```python
import math

import jax
import jax.numpy as jnp
from jax import lax
from jax.experimental import pallas as pl
from jax.experimental.pallas import tpu as pltpu
from jax.sharding import PartitionSpec as P

MESH = pl.DeviceIdType.MESH
BF16, F32 = jnp.bfloat16, jnp.float32
NT = (((1,), (1,)), ((), ()))

N_DEV, TOK, SEG = 8, 128, 64
SEQ = N_DEV * TOK
D = 3072
HD = 128
HQ, HKV, G = 24, 8, 3
BQ = 256
NB = SEQ // BQ
C = HD**-0.5
C2 = C * math.log2(math.e)
WO_SLOTS, W_SLOTS = 4, 4
RB = 128
U_DO, U_K, U_V, U_Q = 0, 3, 4, 5


scope = jax.named_scope


def dot_nt(a, b):
    return lax.dot_general(a, b, NT, preferred_element_type=F32)


def dot(a, b):
    return jnp.dot(a, b, preferred_element_type=F32)


def kernel(x_hbm, dy_hbm, wq_hbm, wk_hbm, wv_hbm, wo_hbm, out_hbm,
           x_v, dy_v, wo_s, w_s, wrel, sbuf, recv, obuf, rin, acc, res,
           s_scr, dp_scr, p_scr, ds_scr, kt, vt, dk_acc, dv_acc,
           io_sem, wo_sem, w_sem, send_sem, recv_sem, osend_sem, orecv_sem, out_sem):
    me = lax.axis_index("cp")
    dp = lax.axis_index("dp")
    chip = me // 2

    barrier = pltpu.get_barrier_semaphore()
    for p in range(1, N_DEV):
        pl.semaphore_signal(barrier, inc=1, device_id=(dp, lax.rem(me + p, N_DEV)), device_id_type=MESH)

    x_cp = pltpu.make_async_copy(x_hbm, x_v, io_sem.at[0])
    dy_cp = pltpu.make_async_copy(dy_hbm, dy_v, io_sem.at[1])

    def wo_copy(s):
        cc = lax.rem(chip + s % 4 + 1, 4)
        slot = s % WO_SLOTS
        return pltpu.make_async_copy(wo_hbm.at[pl.ds(2 * cc, 2), s // 4], wo_s.at[slot], wo_sem.at[slot])

    def w_copy(w_hbm, i, slot):
        return pltpu.make_async_copy(w_hbm.at[i], w_s.at[slot], w_sem.at[slot])

    dy_cp.start()
    for s in range(WO_SLOTS):
        wo_copy(s).start()
    x_cp.start()
    for i in range(4):
        w_copy(wk_hbm, i, i).start()
    dk_acc[...] = jnp.zeros_like(dk_acc)
    dv_acc[...] = jnp.zeros_like(dv_acc)

    def send_block(unit, dest, val):
        @pl.when(dest != me)
        def _():
            sbuf[unit, dest] = val
            for half, seg in ((0, me), (1, 2 * N_DEV - 1 - me)):
                pltpu.make_async_remote_copy(
                    src_ref=sbuf.at[unit, dest, pl.ds(half * SEG, SEG)],
                    dst_ref=recv.at[unit, pl.ds(pl.multiple_of(seg * SEG, SEG), SEG)],
                    send_sem=send_sem, recv_sem=recv_sem.at[unit],
                    device_id=(dp, dest), device_id_type=MESH).start()

        @pl.when(dest == me)
        def _():
            recv[unit, pl.ds(pl.multiple_of(me * SEG, SEG), SEG), :] = val[:SEG]
            recv[unit, pl.ds(pl.multiple_of((2 * N_DEV - 1 - me) * SEG, SEG), SEG), :] = val[SEG:]

    def send_pair(unit, cc, val):
        for q in range(2):
            send_block(unit, 2 * cc + q, val[:, q * HD:(q + 1) * HD])

    def do_dot(s):
        w = wo_s[s % WO_SLOTS].reshape(2 * HD, D)
        return dot_nt(dy_v[...], w).astype(BF16)

    def do_parts(s):
        acc_v = None
        for k in range(6):
            ks = slice(k * 512, (k + 1) * 512)
            t = dot_nt(dy_v[:, ks], wo_s[s % WO_SLOTS, :, :, ks].reshape(2 * HD, 512))
            acc_v = t if acc_v is None else acc_v + t
            yield acc_v

    def x_parts(h0, h1):
        acc_v = None
        for k in range(6):
            ks = slice(k * 512, (k + 1) * 512)
            t = dot(x_v[:, ks], jnp.concatenate([wrel[h0, ks, :], wrel[h1, ks, :]], axis=1))
            acc_v = t if acc_v is None else acc_v + t
            yield acc_v

    def do_send(s, val):
        send_pair(U_DO + s // 4, lax.rem(chip + s % 4 + 1, 4), val)

        @pl.when(s + WO_SLOTS < 12)
        def _():
            wo_copy(s + WO_SLOTS).start()

    def relay_kv(i, slot):
        base = HQ + 8 * (i // 4)
        for r in range(0, 768, RB):
            row = pl.multiple_of((i % 4) * 768 + r, RB)
            wrel[pl.ds(base, 8), pl.ds(row, RB), :] = jnp.swapaxes(w_s[slot, pl.ds(r, RB)], 0, 1)
            yield

    def relay_q(j, slot):
        for r in range(0, 256, RB):
            row = pl.multiple_of(j * 256 + r, RB)
            blk = w_s[slot, pl.ds(3 * r, 3 * RB)].reshape(RB, 3, 8, HD)
            for t in range(3):
                wrel[pl.ds(8 * t, 8), pl.ds(row, RB), :] = jnp.swapaxes(blk[:, t], 0, 1)
                yield

    def x_dot(h0, h1):
        w = jnp.concatenate([wrel[h0], wrel[h1]], axis=1)
        return dot(x_v[...], w).astype(BF16)

    with scope('dywait'):
        dy_cp.wait()
    with scope('barrier'):
        pl.semaphore_wait(barrier, N_DEV - 1)

    def step_a(s, _):
        wo_copy(s).wait()
        do_send(s, do_dot(s))
        return 0

    with scope('do'):
        lax.fori_loop(0, 4, step_a, 0)

    def step_b(i, _):
        s = i + 4
        slot = i % W_SLOTS
        wo_copy(s).wait()
        w_copy(wk_hbm, 0, slot).wait()
        for val, _ in zip(do_parts(s), relay_kv(i, slot)):
            pass
        val = val.astype(BF16)
        do_send(s, val)

        @pl.when(i < 4)
        def _():
            w_copy(wv_hbm, i, slot).start()

        @pl.when(i >= 4)
        def _():
            w_copy(wq_hbm, i - 4, slot).start()
        return 0

    with scope('do_relkv'):
        lax.fori_loop(0, 8, step_b, 0)
    x_cp.wait()

    def step_c(j, _):
        slot = j % W_SLOTS
        w_copy(wk_hbm, 0, slot).wait()
        cc = lax.rem(chip + j % 4 + 1, 4)
        h0 = HQ + 8 * (j // 4) + 2 * cc
        for val, _ in zip(x_parts(h0, h0 + 1), relay_q(j, slot)):
            pass
        val = val.astype(BF16)
        send_pair(U_K + j // 4, cc, val)
        w_copy(wq_hbm, j + W_SLOTS, slot).start()
        return 0

    with scope('kv_relq'):
        lax.fori_loop(0, 8, step_c, 0)

    def step_d(j, _):
        slot = j % W_SLOTS
        w_copy(wk_hbm, 0, slot).wait()
        for _ in relay_q(j, slot):
            pass
        return 0

    with scope('relq'):
        lax.fori_loop(8, 12, step_d, 0)

    def q_step(s, _):
        g = s // 2
        ccs = [lax.rem(chip + 2 * (s % 2) + k + 1, 4) for k in range(2)]
        vals = [x_dot(6 * cc + g, 6 * cc + g + 3) for cc in ccs]
        for cc, val in zip(ccs, vals):
            send_pair(U_Q + g, cc, val)
        return 0

    with scope('q'):
        lax.fori_loop(0, 6, q_step, 0)

    def wait_unit(u):
        part = recv.at[u, pl.ds(0, SEQ - TOK)]
        pltpu.make_async_copy(part, part, recv_sem.at[u]).wait()

    with scope('waitkv'):
        wait_unit(U_K)
        wait_unit(U_V)
    kt[...] = recv[U_K].T
    vt[...] = recv[U_V].T

    def send_out(u, head, seg):
        dest, half = (seg, 0) if seg < N_DEV else (2 * N_DEV - 1 - seg, 1)
        rows = pl.ds(seg * SEG, SEG)

        @pl.when(dest != me)
        def _():
            pltpu.make_async_remote_copy(
                src_ref=obuf.at[u, rows], dst_ref=rin.at[head, pl.ds(half * SEG, SEG)],
                send_sem=osend_sem, recv_sem=orecv_sem.at[u],
                device_id=(dp, dest), device_id_type=MESH).start()

        @pl.when(dest == me)
        def _():
            rin[head, half * SEG:(half + 1) * SEG, :] = obuf[u, rows, :]

    def attn_head(g, _):
        with scope('waitq'):
            wait_unit(U_DO + g)
            wait_unit(U_Q + g)
        st = [{} for _ in range(NB)]

        def rows_of(b):
            return slice(b * BQ, (b + 1) * BQ)

        def chunks(b):
            return [slice(k * BQ, (k + 1) * BQ) for k in range(b + 1)]

        def scores(b):
            qb = recv[U_Q + g, rows_of(b), :]
            dob = recv[U_DO + g, rows_of(b), :]
            mx = None
            for kc, ks in enumerate(chunks(b)):
                s = dot_nt(recv[U_K, ks, :], qb)
                if kc == b:
                    key = lax.broadcasted_iota(jnp.int32, (BQ, BQ), 0)
                    qry = lax.broadcasted_iota(jnp.int32, (BQ, BQ), 1)
                    s = jnp.where(key <= qry, s, -jnp.inf)
                s_scr[b][ks, :] = s
                mc = jnp.max(s.reshape(BQ // 8, 8, BQ), axis=0)
                mx = mc if mx is None else jnp.maximum(mx, mc)
            for ks in chunks(b):
                dp_scr[b][ks, :] = dot_nt(recv[U_V, ks, :], dob)
            st[b]['m2'] = jnp.max(mx, axis=0, keepdims=True) * C2

        def probs(b):
            m2 = st[b]['m2']
            ls = None
            for ks in chunks(b):
                e = jnp.exp2(s_scr[b][ks, :] * C2 - m2)
                lc = jnp.sum(e.reshape(BQ // 8, 8, BQ), axis=0)
                ls = lc if ls is None else ls + lc
            lse2 = m2 + jnp.log2(jnp.sum(ls, axis=0, keepdims=True))
            for ks in chunks(b):
                p_scr[b][ks, :] = jnp.exp2(s_scr[b][ks, :] * C2 - lse2).astype(BF16)

        def outs(b):
            n = (b + 1) * BQ
            dob = recv[U_DO + g, rows_of(b), :]
            ot = dot(vt[:, :n], p_scr[b][...]).astype(BF16)
            st[b]['delta'] = jnp.sum(dob.T.astype(F32) * ot.astype(F32), axis=0, keepdims=True)
            for ks in chunks(b):
                dv_acc[ks, :] += dot(p_scr[b][ks, :], dob)

        def dscores(b):
            delta = st[b]['delta']
            for ks in chunks(b):
                ds_scr[b][ks, :] = (p_scr[b][ks, :].astype(F32) * (dp_scr[b][ks, :] - delta)).astype(BF16)

        def grads(b):
            n = (b + 1) * BQ
            qb = recv[U_Q + g, rows_of(b), :]
            for ks in chunks(b):
                dk_acc[ks, :] += dot(ds_scr[b][ks, :], qb)
            dqt = (dot(kt[:, :n], ds_scr[b][...]) * C).astype(BF16)
            obuf[g, rows_of(b), :] = dqt.T

        with scope('attn'):
            scores(3)
            scores(2)
            probs(3)
            outs(3)
            scores(1)
            dscores(3)
            probs(2)
            grads(3)
            outs(2)
            scores(0)
            dscores(2)
            probs(1)
            grads(2)
            outs(1)
            dscores(1)
            probs(0)
            grads(1)
            outs(0)
            dscores(0)
            grads(0)

        with scope('send'):
            for seg in range(2 * N_DEV):
                send_out(g, G * me + g, seg)
        return 0

    lax.fori_loop(0, G, attn_head, 0)
    with scope('senddkv'):
        obuf[3] = (dk_acc[...] * C).astype(BF16)
        for seg in range(2 * N_DEV):
            send_out(3, HQ + me, seg)
        obuf[4] = dv_acc[...].astype(BF16)
        for seg in range(2 * N_DEV):
            send_out(4, HQ + HKV + me, seg)

    ND = 1536
    for u in range(5):
        with scope('waito'):
            part = obuf.at[u, pl.ds(0, SEQ - TOK)]
            pltpu.make_async_copy(part, part, orecv_sem.at[u]).wait()
        heads = [G * j + u for j in range(8)] if u < 3 else [HQ + 8 * (u - 3) + j for j in range(8)]

        def dx_step(i, _, u=u, heads=heads):
            cols = pl.ds(pl.multiple_of(i * ND, ND), ND)
            lhs = jnp.concatenate([rin[h] for h in heads], axis=1)
            rhs = jnp.concatenate([wrel[h, cols, :] for h in heads], axis=1)
            t = dot_nt(lhs, rhs)
            if u > 0:
                t = t + acc[:, cols]
            if u < 4:
                acc[:, cols] = t
            else:
                res[:, cols] = t.astype(BF16)
                pltpu.make_async_copy(res.at[:, cols], out_hbm.at[:, cols], out_sem).start()
            return 0

        with scope('dx'):
            lax.fori_loop(0, D // ND, dx_step, 0)

    with scope('final'):
      part = sbuf.at[pl.ds(0, 7)]
      pltpu.make_async_copy(part, part, send_sem).wait()
      part = obuf.at[:, pl.ds(0, SEQ - TOK)]
      pltpu.make_async_copy(part, part, osend_sem).wait()
      pltpu.make_async_copy(res, out_hbm, out_sem).wait()


def solution(mesh):
    row_spec = P(("dp", "cp"), None)

    def device_fn(x_in, d_y, w_q, w_k, w_v, w_o):
        dma = pltpu.SemaphoreType.DMA
        return pl.pallas_call(
            kernel,
            out_shape=jax.ShapeDtypeStruct((TOK, D), BF16),
            in_specs=[pl.BlockSpec(memory_space=pl.ANY)] * 6,
            out_specs=pl.BlockSpec(memory_space=pl.ANY),
            scratch_shapes=[
                pltpu.VMEM((TOK, D), BF16),
                pltpu.VMEM((TOK, D), BF16),
                pltpu.VMEM((WO_SLOTS, 2, HD, D), BF16),
                pltpu.VMEM((W_SLOTS, 768, 8, HD), BF16),
                pltpu.VMEM((HQ + 2 * HKV, D, HD), BF16),
                pltpu.VMEM((8, N_DEV, TOK, HD), BF16),
                pltpu.VMEM((8, SEQ, HD), BF16),
                pltpu.VMEM((5, SEQ, HD), BF16),
                pltpu.VMEM((HQ + 2 * HKV, TOK, HD), BF16),
                pltpu.VMEM((TOK, D), F32),
                pltpu.VMEM((TOK, D), BF16),
                *[[pltpu.VMEM(((b + 1) * BQ, BQ), t) for b in range(NB)] for t in (F32, F32, BF16, BF16)],
                pltpu.VMEM((HD, SEQ), BF16),
                pltpu.VMEM((HD, SEQ), BF16),
                pltpu.VMEM((SEQ, HD), F32),
                pltpu.VMEM((SEQ, HD), F32),
                dma((2,)), dma((WO_SLOTS,)), dma((W_SLOTS,)),
                dma, dma((8,)), dma, dma((5,)), dma,
            ],
            compiler_params=pltpu.CompilerParams(
                collective_id=0, has_side_effects=True, vmem_limit_bytes=67_043_328),
        )(x_in, d_y, w_q.reshape(12, 768, 8, HD), w_k.reshape(4, 768, 8, HD), w_v.reshape(4, 768, 8, HD),
          w_o.reshape(8, 3, HD, D))

    return jax.shard_map(device_fn, mesh=mesh, in_specs=(row_spec, row_spec, P(), P(), P(), P()),
                         out_specs=row_spec, check_vma=False)
```

```python
import math

import jax
import jax.numpy as jnp
from jax import lax
from jax.experimental import pallas as pl
from jax.experimental.pallas import tpu as pltpu
from jax.sharding import PartitionSpec as P

MESH = pl.DeviceIdType.MESH
BF16, F32 = jnp.bfloat16, jnp.float32
NT = (((1,), (1,)), ((), ()))

N_DEV, N_CHIP, TOK, SEG = 8, 4, 128, 64
ROWS = 2 * TOK
SEQ = N_DEV * TOK
D = 3072
HD = 128
G = 3
BQ = 256
NB = SEQ // BQ
C = HD**-0.5
C2 = C * math.log2(math.e)
U_DO, U_K, U_V, U_Q = 0, 3, 4, 5
SLOTS = 8
RB = 128
ND = 1536
NF = 512

scope = jax.named_scope


def dot_nt(a, b):
    return lax.dot_general(a, b, NT, preferred_element_type=F32)


def dot(a, b):
    return jnp.dot(a, b, preferred_element_type=F32)


def kernel(x_hbm, dy_hbm, wq_hbm, wk_hbm, wv_hbm, wo_hbm, out_hbm,
           x_v, dy_v, wo_s, w_s, wq_r, wk_r, wv_r, sbuf, recv, obuf, rin, acc, pbuf, res,
           s0, s1, s2, s3, d0, d1, d2, d3, p0, p1, p2, p3, e0, e1, e2, e3, kt, vt, dk_acc, dv_acc,
           io_sem, wo_sem, w_sem, xs_sem, xr_sem, send_sem, recv_sem, osend_sem, orecv_sem, ps_sem, pr_sem, out_sem):
    s_scr, dp_scr, p_scr, ds_scr = (s0, s1, s2, s3), (d0, d1, d2, d3), (p0, p1, p2, p3), (e0, e1, e2, e3)
    me = lax.axis_index("cp")
    dp = lax.axis_index("dp")
    chip = me // 2
    q = lax.rem(me, 2)
    partner = (dp, 2 * chip + 1 - q)

    def peer(k):
        return lax.rem(chip + k, N_CHIP)

    def dev_of(cc):
        return (dp, 2 * cc + q)

    barrier = pltpu.get_barrier_semaphore()
    pl.semaphore_signal(barrier, inc=1, device_id=partner, device_id_type=MESH)
    for k in range(1, N_CHIP):
        pl.semaphore_signal(barrier, inc=1, device_id=dev_of(peer(k)), device_id_type=MESH)

    def blk(i):
        return pl.ds(pl.multiple_of(i * SEG, SEG), SEG)

    own = (blk(q), blk(3 - q))
    other = (blk(1 - q), blk(2 + q))

    def io_copies(n):
        src, dst = ((dy_hbm, dy_v), (x_hbm, x_v))[n]
        return [pltpu.make_async_copy(src.at[pl.ds(h * SEG, SEG)], dst.at[own[h]], io_sem.at[n, h]) for h in range(2)]

    def swap_copies(n):
        ref = (dy_v, x_v)[n]
        return [pltpu.make_async_remote_copy(
            src_ref=ref.at[own[h]], dst_ref=ref.at[own[h]], send_sem=xs_sem.at[n, h], recv_sem=xr_sem.at[n, h],
            device_id=partner, device_id_type=MESH) for h in range(2)]

    def wo_copy(g, k):
        return pltpu.make_async_copy(wo_hbm.at[q, peer(k), g], wo_s.at[g, k - 1], wo_sem.at[g, k - 1])

    def wkv_copy(w_hbm, i, slot):
        return pltpu.make_async_copy(w_hbm.at[i, :, q], w_s.at[slot], w_sem.at[slot])

    def wq_copy(i, slot):
        return pltpu.make_async_copy(wq_hbm.at[i, :, pl.ds(3 * q, 3)], w_s.at[slot].reshape(256, 3, 4, HD), w_sem.at[slot])

    def wait_slot(slot):
        wkv_copy(wk_hbm, 0, slot).wait()

    for cp in io_copies(0) + io_copies(1):
        cp.start()
    for i in range(4):
        wkv_copy(wk_hbm, i, i).start()
    for k in range(1, 5):
        wo_copy(0, k).start()
    for i in range(4):
        wkv_copy(wv_hbm, i, 4 + i).start()
    dk_acc[...] = jnp.zeros_like(dk_acc)
    dv_acc[...] = jnp.zeros_like(dv_acc)

    with scope('barrier'):
        pl.semaphore_wait(barrier, N_CHIP)
    with scope('swap'):
        for n in range(2):
            for cp, sw in zip(io_copies(n), swap_copies(n)):
                cp.wait()
                sw.start()

    def relay_kv(dst, i, slot):
        flat = w_s.at[slot].reshape(768 * 4, HD)
        for h in range(4):
            for r in range(0, 768, RB):
                dst[h, pl.ds(i * 768 + r, RB), :] = flat[pl.ds(4 * r + h, RB, stride=4), :]

    def relay_q(i, slot):
        flat = w_s.at[slot].reshape(768 * 4, HD)
        for h in range(12):
            for r in range(0, 256, RB):
                wq_r[h, pl.ds(i * 256 + r, RB), :] = flat[pl.ds(12 * r + h, RB, stride=12), :]

    with scope('relk'):
        for i in range(4):
            wait_slot(i)
            relay_kv(wk_r, i, i)
            wq_copy(i, i).start()

    def send_block(unit, k, val):
        if k == N_CHIP:
            recv[unit, pl.ds(pl.multiple_of(chip * TOK, TOK), TOK), :] = val[:TOK]
            recv[unit, pl.ds(pl.multiple_of(SEQ - TOK - chip * TOK, TOK), TOK), :] = val[TOK:]
            return
        sbuf[unit, k - 1] = val
        for half, row in ((0, chip * TOK), (1, SEQ - TOK - chip * TOK)):
            pltpu.make_async_remote_copy(
                src_ref=sbuf.at[unit, k - 1, pl.ds(half * TOK, TOK)],
                dst_ref=recv.at[unit, pl.ds(pl.multiple_of(row, TOK), TOK)],
                send_sem=send_sem, recv_sem=recv_sem.at[unit],
                device_id=dev_of(peer(k)), device_id_type=MESH).start()

    def do_steps(g):
        for k in (1, 3):
            wo_copy(g, k).wait()
            wo_copy(g, k + 1).wait()
            w = wo_s[g, pl.ds(k - 1, 2)].reshape(2 * HD, D)
            val = dot_nt(dy_v[...], w).astype(BF16)
            send_block(U_DO + g, k, val[:, :HD])
            send_block(U_DO + g, k + 1, val[:, HD:])

    def kv_steps():
        for k in range(1, 5):
            cc = peer(k)
            val = dot(x_v[...], jnp.concatenate([wk_r[cc], wv_r[cc]], axis=1)).astype(BF16)
            send_block(U_K, k, val[:, :HD])
            send_block(U_V, k, val[:, HD:])

    def q_steps(g):
        for k in (1, 3):
            w = jnp.concatenate([wq_r[3 * peer(k) + g], wq_r[3 * peer(k + 1) + g]], axis=1)
            val = dot(x_v[...], w).astype(BF16)
            send_block(U_Q + g, k, val[:, :HD])
            send_block(U_Q + g, k + 1, val[:, HD:])

    with scope('dyswap'):
        for cp in swap_copies(0):
            cp.wait_recv()
    with scope('do0'):
        do_steps(0)
    for g in (1, 2):
        for k in range(1, 5):
            wo_copy(g, k).start()
    with scope('relv'):
        for i in range(4):
            wait_slot(4 + i)
            relay_kv(wv_r, i, 4 + i)
            wq_copy(4 + i, 4 + i).start()
    with scope('xswap'):
        for cp in swap_copies(1):
            cp.wait_recv()
    with scope('kv'):
        kv_steps()

    with scope('relq'):
        for i in range(12):
            slot = i % SLOTS
            wait_slot(slot)
            relay_q(i, slot)
            if i < 4:
                wq_copy(i + SLOTS, slot).start()
    with scope('q0'):
        q_steps(0)
    for g in (1, 2):
        with scope('do12'):
            do_steps(g)
        with scope('q12'):
            q_steps(g)

    def wait_unit(u):
        part = recv.at[u, pl.ds(0, SEQ - ROWS)]
        pltpu.make_async_copy(part, part, recv_sem.at[u]).wait()

    with scope('waitkv'):
        wait_unit(U_K)
        wait_unit(U_V)
    kt[...] = recv[U_K].T
    vt[...] = recv[U_V].T

    def rin_slot(u):
        return G * chip + u if not isinstance(u, int) or u < G else 12 + 4 * (u - G) + chip

    def send_out(u):
        slot = rin_slot(u)
        for k in range(1, N_CHIP):
            cc = peer(k)
            for half, row in ((0, cc * TOK), (1, SEQ - TOK - cc * TOK)):
                pltpu.make_async_remote_copy(
                    src_ref=obuf.at[u, pl.ds(pl.multiple_of(row, TOK), TOK)],
                    dst_ref=rin.at[slot, pl.ds(half * TOK, TOK)],
                    send_sem=osend_sem, recv_sem=orecv_sem.at[u],
                    device_id=dev_of(cc), device_id_type=MESH).start()
        rin[slot, :TOK, :] = obuf[u, pl.ds(pl.multiple_of(chip * TOK, TOK), TOK), :]
        rin[slot, TOK:, :] = obuf[u, pl.ds(pl.multiple_of(SEQ - TOK - chip * TOK, TOK), TOK), :]

    def attn_head(g, _):
        with scope('waitq'):
            wait_unit(U_DO + g)
            wait_unit(U_Q + g)
        st = [{} for _ in range(NB)]

        def rows_of(b):
            return slice(b * BQ, (b + 1) * BQ)

        def chunks(b):
            return [slice(k * BQ, (k + 1) * BQ) for k in range(b + 1)]

        def scores(b):
            qb = recv[U_Q + g, rows_of(b), :]
            dob = recv[U_DO + g, rows_of(b), :]
            mx = None
            for kc, ks in enumerate(chunks(b)):
                s = dot_nt(recv[U_K, ks, :], qb)
                if kc == b:
                    key = lax.broadcasted_iota(jnp.int32, (BQ, BQ), 0)
                    qry = lax.broadcasted_iota(jnp.int32, (BQ, BQ), 1)
                    s = jnp.where(key <= qry, s, -jnp.inf)
                s_scr[b][ks, :] = s
                mc = jnp.max(s.reshape(BQ // 8, 8, BQ), axis=0)
                mx = mc if mx is None else jnp.maximum(mx, mc)
            for ks in chunks(b):
                dp_scr[b][ks, :] = dot_nt(recv[U_V, ks, :], dob)
            st[b]['m2'] = jnp.max(mx, axis=0, keepdims=True) * C2

        def probs(b):
            m2 = st[b]['m2']
            ls = None
            for ks in chunks(b):
                e = jnp.exp2(s_scr[b][ks, :] * C2 - m2)
                lc = jnp.sum(e.reshape(BQ // 8, 8, BQ), axis=0)
                ls = lc if ls is None else ls + lc
            lse2 = m2 + jnp.log2(jnp.sum(ls, axis=0, keepdims=True))
            for ks in chunks(b):
                p_scr[b][ks, :] = jnp.exp2(s_scr[b][ks, :] * C2 - lse2).astype(BF16)

        def outs(b):
            n = (b + 1) * BQ
            dob = recv[U_DO + g, rows_of(b), :]
            ot = dot(vt[:, :n], p_scr[b][...]).astype(BF16)
            st[b]['delta'] = jnp.sum(dob.T.astype(F32) * ot.astype(F32), axis=0, keepdims=True)
            for ks in chunks(b):
                dv_acc[ks, :] += dot(p_scr[b][ks, :], dob)

        def dscores(b):
            delta = st[b]['delta']
            for ks in chunks(b):
                ds_scr[b][ks, :] = (p_scr[b][ks, :].astype(F32) * (dp_scr[b][ks, :] - delta)).astype(BF16)

        def grads(b):
            n = (b + 1) * BQ
            qb = recv[U_Q + g, rows_of(b), :]
            for ks in chunks(b):
                dk_acc[ks, :] += dot(ds_scr[b][ks, :], qb)
            dqt = (dot(kt[:, :n], ds_scr[b][...]) * C).astype(BF16)
            obuf[g, rows_of(b), :] = dqt.T

        with scope('attn'):
            scores(3)
            scores(2)
            probs(3)
            outs(3)
            scores(1)
            dscores(3)
            probs(2)
            grads(3)
            outs(2)
            scores(0)
            dscores(2)
            probs(1)
            grads(2)
            outs(1)
            dscores(1)
            probs(0)
            grads(1)
            outs(0)
            dscores(0)
            grads(0)

        with scope('send'):
            send_out(g)
        return 0

    lax.fori_loop(0, G, attn_head, 0)
    with scope('senddkv'):
        obuf[3] = (dk_acc[...] * C).astype(BF16)
        send_out(3)
        obuf[4] = dv_acc[...].astype(BF16)
        send_out(4)

    def unit_w(u, cols):
        if u < G:
            return [wq_r[G * j + u, cols, :] for j in range(N_CHIP)]
        return [(wk_r, wv_r)[u - G][j, cols, :] for j in range(N_CHIP)]

    def unit_lhs(u):
        return [rin[G * j + u if u < G else 12 + 4 * (u - G) + j] for j in range(N_CHIP)]

    def p_copies(i, cols):
        return [pltpu.make_async_remote_copy(
            src_ref=acc.at[other[h], cols], dst_ref=pbuf.at[pl.ds(h * SEG, SEG), cols],
            send_sem=ps_sem.at[i, h], recv_sem=pr_sem.at[i, h],
            device_id=partner, device_id_type=MESH) for h in range(2)]

    def out_copy(i, cols):
        return pltpu.make_async_copy(res.at[:, cols], out_hbm.at[:, cols], out_sem.at[i])

    for u in range(5):
        with scope('waito'):
            part = obuf.at[u, pl.ds(0, SEQ - ROWS)]
            pltpu.make_async_copy(part, part, orecv_sem.at[u]).wait()
        nd = ND if u < 4 else NF

        def dx_step(i, _, u=u, nd=nd):
            cols = pl.ds(pl.multiple_of(i * nd, nd), nd)
            t = dot_nt(jnp.concatenate(unit_lhs(u), axis=1), jnp.concatenate(unit_w(u, cols), axis=1))
            if u > 0:
                t = t + acc[:, cols]
            acc[:, cols] = t
            if u == 4:
                for cp in p_copies(i, cols):
                    cp.start()
            return 0

        with scope('dx'):
            lax.fori_loop(0, D // nd, dx_step, 0)

    def fin_step(i, _):
        cols = pl.ds(pl.multiple_of(i * NF, NF), NF)
        for h, cp in enumerate(p_copies(i, cols)):
            cp.wait_recv()
            rows = slice(h * SEG, (h + 1) * SEG)
            res[rows, cols] = (acc[own[h], cols] + pbuf[rows, cols]).astype(BF16)
        out_copy(i, cols).start()
        return 0

    with scope('fin'):
        lax.fori_loop(0, D // NF, fin_step, 0)

    with scope('final'):
        for n in range(2):
            for cp in swap_copies(n):
                cp.wait_send()
        part = sbuf
        pltpu.make_async_copy(part, part, send_sem).wait()
        part = obuf.at[:, pl.ds(0, SEQ - ROWS)]
        pltpu.make_async_copy(part, part, osend_sem).wait()

        def drain(i, _):
            cols = pl.ds(pl.multiple_of(i * NF, NF), NF)
            for cp in p_copies(i, cols):
                cp.wait_send()
            out_copy(i, cols).wait()
            return 0

        lax.fori_loop(0, D // NF, drain, 0)


def solution(mesh):
    row_spec = P(("dp", "cp"), None)

    def device_fn(x_in, d_y, w_q, w_k, w_v, w_o):
        dma = pltpu.SemaphoreType.DMA
        return pl.pallas_call(
            kernel,
            out_shape=jax.ShapeDtypeStruct((TOK, D), BF16),
            in_specs=[pl.BlockSpec(memory_space=pl.ANY)] * 6,
            out_specs=pl.BlockSpec(memory_space=pl.ANY),
            scratch_shapes=[
                pltpu.VMEM((ROWS, D), BF16),
                pltpu.VMEM((ROWS, D), BF16),
                pltpu.VMEM((G, N_CHIP, HD, D), BF16),
                pltpu.VMEM((SLOTS, 768, 4, HD), BF16),
                pltpu.VMEM((12, D, HD), BF16),
                pltpu.VMEM((4, D, HD), BF16),
                pltpu.VMEM((4, D, HD), BF16),
                pltpu.VMEM((8, 3, ROWS, HD), BF16),
                pltpu.VMEM((8, SEQ, HD), BF16),
                pltpu.VMEM((5, SEQ, HD), BF16),
                pltpu.VMEM((20, ROWS, HD), BF16),
                pltpu.VMEM((ROWS, D), F32),
                pltpu.VMEM((TOK, D), F32),
                pltpu.VMEM((TOK, D), BF16),
                *[pltpu.VMEM(((b + 1) * BQ, BQ), t) for t in (F32, F32, BF16, BF16) for b in range(NB)],
                pltpu.VMEM((HD, SEQ), BF16),
                pltpu.VMEM((HD, SEQ), BF16),
                pltpu.VMEM((SEQ, HD), F32),
                pltpu.VMEM((SEQ, HD), F32),
                dma((2, 2)), dma((G, N_CHIP)), dma((SLOTS,)), dma((2, 2)), dma((2, 2)),
                dma, dma((8,)), dma, dma((5,)), dma((6, 2)), dma((6, 2)), dma((6,)),
            ],
            compiler_params=pltpu.CompilerParams(
                collective_id=0, has_side_effects=True, vmem_limit_bytes=67_043_328),
        )(x_in, d_y, w_q.reshape(12, 256, 6, 4, HD), w_k.reshape(4, 768, 2, 4, HD), w_v.reshape(4, 768, 2, 4, HD),
          w_o.reshape(2, N_CHIP, G, HD, D))

    return jax.shard_map(device_fn, mesh=mesh, in_specs=(row_spec, row_spec, P(), P(), P(), P()),
                         out_specs=row_spec, check_vma=False)
```

```python
import math

import jax
import jax.numpy as jnp
from jax import lax
from jax.experimental import pallas as pl
from jax.experimental.pallas import tpu as pltpu
from jax.sharding import PartitionSpec as P

MESH = pl.DeviceIdType.MESH
BF16, F32 = jnp.bfloat16, jnp.float32
NT = (((1,), (1,)), ((), ()))

N_DEV, N_CHIP, TOK, SEG = 8, 4, 128, 64
ROWS = 2 * TOK
SEQ = N_DEV * TOK
D = 3072
HD = 128
G = 3
BQ = 256
NB = SEQ // BQ
C = HD**-0.5
C2 = C * math.log2(math.e)
U_DO, U_K, U_V, U_Q = 0, 3, 4, 5
SLOTS = 8
RB = 128
ND = 1536
VLIM = 66_000_000

scope = jax.named_scope


def dot_nt(a, b):
    return lax.dot_general(a, b, NT, preferred_element_type=F32)


def dot(a, b):
    return jnp.dot(a, b, preferred_element_type=F32)


def kernel(x_hbm, dy_hbm, wq_hbm, wk_hbm, wv_hbm, wo_hbm, out_ref,
           x_v, dy_v, wo_s, w_s, wq_r, wk_r, wv_r, sbuf, recv, obuf, rin, rv, acc, pbuf,
           s0, s1, s2, s3, d0, d1, d2, d3, p0, p1, p2, p3, e0, e1, e2, e3, kt, vt, dk_acc, dv_acc,
           io_sem, wo_sem, w_sem, xs_sem, xr_sem, send_sem, recv_sem, osend_sem, orecv_sem, dv_sem, ps_sem, pr_sem):
    s_scr, dp_scr, p_scr, ds_scr = (s0, s1, s2, s3), (d0, d1, d2, d3), (p0, p1, p2, p3), (e0, e1, e2, e3)
    me = lax.axis_index("cp")
    dp = lax.axis_index("dp")
    chip = me // 2
    q = lax.rem(me, 2)
    partner = (dp, 2 * chip + 1 - q)

    def peer(k):
        return lax.rem(chip + k, N_CHIP)

    def dev_of(cc):
        return (dp, 2 * cc + q)

    barrier = pltpu.get_barrier_semaphore()
    pl.semaphore_signal(barrier, inc=1, device_id=partner, device_id_type=MESH)
    for k in range(1, N_CHIP):
        pl.semaphore_signal(barrier, inc=1, device_id=dev_of(peer(k)), device_id_type=MESH)

    def blk(i):
        return pl.ds(pl.multiple_of(i * SEG, SEG), SEG)

    own = (blk(q), blk(3 - q))
    other = (blk(1 - q), blk(2 + q))

    def io_copies(n):
        src, dst = ((dy_hbm, dy_v), (x_hbm, x_v))[n]
        return [pltpu.make_async_copy(src.at[pl.ds(h * SEG, SEG)], dst.at[own[h]], io_sem.at[n, h]) for h in range(2)]

    def swap_copies(n):
        ref = (dy_v, x_v)[n]
        return [pltpu.make_async_remote_copy(
            src_ref=ref.at[own[h]], dst_ref=ref.at[own[h]], send_sem=xs_sem.at[n, h], recv_sem=xr_sem.at[n, h],
            device_id=partner, device_id_type=MESH) for h in range(2)]

    def wo_copy(g, k):
        return pltpu.make_async_copy(wo_hbm.at[q, peer(k), g], wo_s.at[g, k - 1], wo_sem.at[g, k - 1])

    def wkv_copy(w_hbm, i, slot, half=None):
        half = q if half is None else half
        return pltpu.make_async_copy(w_hbm.at[i, :, :, half], w_s.at[slot], w_sem.at[slot])

    def wq_copy(i, slot):
        return pltpu.make_async_copy(wq_hbm.at[i, :, pl.ds(3 * q, 3)], w_s.at[slot], w_sem.at[slot])

    def wait_slot(slot):
        wkv_copy(wk_hbm, 0, slot).wait()

    for cp in io_copies(0):
        cp.start()
    for k in (1, 2):
        wo_copy(0, k).start()
    dk_acc[...] = jnp.zeros_like(dk_acc)
    dv_acc[...] = jnp.zeros_like(dv_acc)
    with scope('barrier'):
        pl.semaphore_wait(barrier, N_CHIP)
    with scope('swapdy'):
        for cp, sw in zip(io_copies(0), swap_copies(0)):
            cp.wait()
            sw.start()
    for cp in io_copies(1):
        cp.start()
    for k in (3, 4):
        wo_copy(0, k).start()
    for i in range(4):
        wkv_copy(wk_hbm, i, i).start()
    for i in range(4):
        wkv_copy(wv_hbm, i, 4 + i).start()

    def relay_kv(dst, base, i, slot):
        flat = w_s.at[slot].reshape(768 * 4, HD)
        for h in range(4):
            for r in range(0, 768, RB):
                dst[base + h, pl.ds(i * 768 + r, RB), :] = flat[pl.ds(4 * r + h, RB, stride=4), :]

    def relay_q(i, slot):
        flat = w_s.at[slot].reshape(768 * 4, HD)
        for h in range(12):
            for r in range(0, 256, RB):
                wq_r[h, pl.ds(i * 256 + r, RB), :] = flat[pl.ds(12 * r + h, RB, stride=12), :]


    def row_of(b):
        return pl.ds(pl.multiple_of(jnp.where(b < 2, chip * TOK, SEQ - 2 * TOK - chip * TOK) + b * SEG, SEG), SEG)

    def send_rows(unit, k, val, blocks):
        for n, b in enumerate(blocks):
            part = val[n * SEG:(n + 1) * SEG]
            if k == N_CHIP:
                recv[unit, row_of(b), :] = part
            else:
                src = sbuf.at[unit, k - 1, blk(b)]
                src[...] = part
                pltpu.make_async_remote_copy(
                    src_ref=src, dst_ref=recv.at[unit, row_of(b)], send_sem=send_sem, recv_sem=recv_sem.at[unit],
                    device_id=dev_of(peer(k)), device_id_type=MESH).start()

    def send_block(unit, k, val):
        if k == N_CHIP:
            recv[unit, pl.ds(pl.multiple_of(chip * TOK, TOK), TOK), :] = val[:TOK]
            recv[unit, pl.ds(pl.multiple_of(SEQ - TOK - chip * TOK, TOK), TOK), :] = val[TOK:]
            return
        sbuf[unit, k - 1] = val
        for half, row in ((0, chip * TOK), (1, SEQ - TOK - chip * TOK)):
            pltpu.make_async_remote_copy(
                src_ref=sbuf.at[unit, k - 1, pl.ds(half * TOK, TOK)],
                dst_ref=recv.at[unit, pl.ds(pl.multiple_of(row, TOK), TOK)],
                send_sem=send_sem, recv_sem=recv_sem.at[unit],
                device_id=dev_of(peer(k)), device_id_type=MESH).start()

    def do0_rows(blocks, ids, ks):
        lhs = jnp.concatenate([dy_v[b, :] for b in blocks], axis=0)
        w = wo_s[0, pl.ds(ks[0] - 1, len(ks))].reshape(len(ks) * HD, D)
        val = dot_nt(lhs, w).astype(BF16)
        for n, k in enumerate(ks):
            send_rows(U_DO, k, val[:, n * HD:(n + 1) * HD], ids)

    def do_steps(g):
        for k in range(1, 5):
            wo_copy(g, k).wait()
        val = dot_nt(dy_v[...], wo_s[g].reshape(4 * HD, D)).astype(BF16)
        for k in range(1, 5):
            send_block(U_DO + g, k, val[:, (k - 1) * HD:k * HD])

    def kv_steps():
        for k in (1, 3):
            c0, c1 = peer(k), peer(k + 1)
            w = jnp.concatenate([wk_r[c0], wv_r[4 * q + c0], wk_r[c1], wv_r[4 * q + c1]], axis=1)
            val = dot(x_v[...], w).astype(BF16)
            for n in range(2):
                send_block(U_K, k + n, val[:, 2 * n * HD:(2 * n + 1) * HD])
                send_block(U_V, k + n, val[:, (2 * n + 1) * HD:(2 * n + 2) * HD])

    def q_steps(g):
        w = jnp.concatenate([wq_r[3 * peer(k) + g] for k in range(1, 5)], axis=1)
        val = dot(x_v[...], w).astype(BF16)
        for k in range(1, 5):
            send_block(U_Q + g, k, val[:, (k - 1) * HD:k * HD])

    own_ids, other_ids = (q, 3 - q), (1 - q, 2 + q)
    with scope('do0a'):
        for k in (1, 2):
            wo_copy(0, k).wait()
        do0_rows(own, own_ids, (1, 2))
    with scope('swapx'):
        for cp, sw in zip(io_copies(1), swap_copies(1)):
            cp.wait()
            sw.start()
    with scope('do0b'):
        for k in (3, 4):
            wo_copy(0, k).wait()
        do0_rows(own, own_ids, (3, 4))
    for g in (1, 2):
        for k in range(1, 5):
            wo_copy(g, k).start()
    with scope('relk'):
        for i in range(4):
            wait_slot(i)
            relay_kv(wk_r, 0, i, i)
            wq_copy(i, i).start()
    with scope('dyswap'):
        for cp in swap_copies(0):
            cp.wait_recv()
    with scope('do0c'):
        do0_rows(other, other_ids, (1, 2, 3, 4))
    with scope('relv'):
        for i in range(4):
            wait_slot(4 + i)
            relay_kv(wv_r, 4 * q, i, 4 + i)
            wq_copy(4 + i, 4 + i).start()
    with scope('xswap'):
        for cp in swap_copies(1):
            cp.wait_recv()
    with scope('kv'):
        kv_steps()
    with scope('relq'):
        for i in range(12):
            slot = i % SLOTS
            wait_slot(slot)
            relay_q(i, slot)
            if i < 4:
                wq_copy(i + SLOTS, slot).start()
            elif i < 8:
                wkv_copy(wv_hbm, i - 4, slot, 1 - q).start()
    with scope('q0'):
        q_steps(0)
    for g in (1, 2):
        with scope('do12'):
            do_steps(g)
        with scope('q12'):
            q_steps(g)
    with scope('relv2'):
        for i in range(4):
            wait_slot(4 + i)
            relay_kv(wv_r, 4 - 4 * q, i, 4 + i)

    def wait_unit(u):
        part = recv.at[u, pl.ds(0, SEQ - ROWS)]
        pltpu.make_async_copy(part, part, recv_sem.at[u]).wait()

    with scope('waitkv'):
        wait_unit(U_K)
        wait_unit(U_V)
    kt[...] = recv[U_K].T
    vt[...] = recv[U_V].T

    def rin_slot(u):
        return G * chip + u if not isinstance(u, int) or u < G else 12 + 4 * (u - G) + chip

    def send_out(u):
        slot = rin_slot(u)
        for k in range(1, N_CHIP):
            cc = peer(k)
            for half, row in ((0, cc * TOK), (1, SEQ - TOK - cc * TOK)):
                pltpu.make_async_remote_copy(
                    src_ref=obuf.at[u, pl.ds(pl.multiple_of(row, TOK), TOK)],
                    dst_ref=rin.at[slot, pl.ds(half * TOK, TOK)],
                    send_sem=osend_sem, recv_sem=orecv_sem.at[u],
                    device_id=dev_of(cc), device_id_type=MESH).start()
        rin[slot, :TOK, :] = obuf[u, pl.ds(pl.multiple_of(chip * TOK, TOK), TOK), :]
        rin[slot, TOK:, :] = obuf[u, pl.ds(pl.multiple_of(SEQ - TOK - chip * TOK, TOK), TOK), :]

    def attn_head(g, _):
        with scope('waitq'):
            wait_unit(U_DO + g)
            wait_unit(U_Q + g)
        st = [{} for _ in range(NB)]

        def rows_of(b):
            return slice(b * BQ, (b + 1) * BQ)

        def chunks(b):
            return [slice(k * BQ, (k + 1) * BQ) for k in range(b + 1)]

        def scores(b):
            qb = recv[U_Q + g, rows_of(b), :]
            dob = recv[U_DO + g, rows_of(b), :]
            mx = None
            for kc, ks in enumerate(chunks(b)):
                s = dot_nt(recv[U_K, ks, :], qb)
                if kc == b:
                    key = lax.broadcasted_iota(jnp.int32, (BQ, BQ), 0)
                    qry = lax.broadcasted_iota(jnp.int32, (BQ, BQ), 1)
                    s = jnp.where(key <= qry, s, -jnp.inf)
                s_scr[b][ks, :] = s
                mc = jnp.max(s.reshape(BQ // 8, 8, BQ), axis=0)
                mx = mc if mx is None else jnp.maximum(mx, mc)
            for ks in chunks(b):
                dp_scr[b][ks, :] = dot_nt(recv[U_V, ks, :], dob)
            st[b]['m2'] = jnp.max(mx, axis=0, keepdims=True) * C2

        def probs(b):
            m2 = st[b]['m2']
            ls = None
            for ks in chunks(b):
                e = jnp.exp2(s_scr[b][ks, :] * C2 - m2)
                lc = jnp.sum(e.reshape(BQ // 8, 8, BQ), axis=0)
                ls = lc if ls is None else ls + lc
            lse2 = m2 + jnp.log2(jnp.sum(ls, axis=0, keepdims=True))
            for ks in chunks(b):
                p_scr[b][ks, :] = jnp.exp2(s_scr[b][ks, :] * C2 - lse2).astype(BF16)

        def outs(b):
            n = (b + 1) * BQ
            dob = recv[U_DO + g, rows_of(b), :]
            ot = dot(vt[:, :n], p_scr[b][...]).astype(BF16)
            st[b]['delta'] = jnp.sum(dob.T.astype(F32) * ot.astype(F32), axis=0, keepdims=True)
            for ks in chunks(b):
                dv_acc[ks, :] += dot(p_scr[b][ks, :], dob)

        def dscores(b):
            delta = st[b]['delta']
            for ks in chunks(b):
                ds_scr[b][ks, :] = (p_scr[b][ks, :].astype(F32) * (dp_scr[b][ks, :] - delta)).astype(BF16)

        def grads(b):
            n = (b + 1) * BQ
            qb = recv[U_Q + g, rows_of(b), :]
            for ks in chunks(b):
                dk_acc[ks, :] += dot(ds_scr[b][ks, :], qb)
            dqt = (dot(kt[:, :n], ds_scr[b][...]) * C).astype(BF16)
            obuf[g, rows_of(b), :] = dqt.T

        with scope('attn'):
            scores(3)
            scores(2)
            probs(3)
            outs(3)
            scores(1)
            dscores(3)
            probs(2)
            grads(3)
            outs(2)
            scores(0)
            dscores(2)
            probs(1)
            grads(2)
            outs(1)
            dscores(1)
            probs(0)
            grads(1)
            outs(0)
            dscores(0)
            grads(0)

        with scope('send'):
            send_out(g)
        return 0

    lax.fori_loop(0, G, attn_head, 0)
    with scope('senddkv'):
        obuf[3] = (dk_acc[...] * C).astype(BF16)
        send_out(3)
        obuf[4] = dv_acc[...].astype(BF16)
        head = 4 * q + chip

        def seg_rows(dev, half):
            seg = dev if half == 0 else 2 * N_DEV - 1 - dev
            return pl.ds(pl.multiple_of(seg * SEG, SEG), SEG)

        def send_dv(dev, n):
            for half in range(2):
                pltpu.make_async_remote_copy(
                    src_ref=obuf.at[4, seg_rows(dev, half)], dst_ref=rv.at[head, pl.ds(half * SEG, SEG)],
                    send_sem=osend_sem, recv_sem=dv_sem.at[n],
                    device_id=(dp, dev), device_id_type=MESH).start()

        send_dv(partner[1], 0)
        for k in range(1, N_CHIP):
            for r in range(2):
                send_dv(2 * peer(k) + r, k // 2)
        for half in range(2):
            rv[head, half * SEG:(half + 1) * SEG, :] = obuf[4, seg_rows(me, half), :]

    def unit_w(u, cols):
        if u < G:
            return [wq_r[G * j + u, cols, :] for j in range(N_CHIP)]
        return [wk_r[j, cols, :] for j in range(N_CHIP)]

    def unit_lhs(u):
        return [rin[G * j + u if u < G else 12 + 4 * (u - G) + j] for j in range(N_CHIP)]

    def p_copies():
        return [pltpu.make_async_remote_copy(
            src_ref=acc.at[other[h]], dst_ref=pbuf.at[pl.ds(h * SEG, SEG)],
            send_sem=ps_sem.at[h], recv_sem=pr_sem.at[h],
            device_id=partner, device_id_type=MESH) for h in range(2)]

    for u in range(4):
        with scope('waito'):
            part = obuf.at[u, pl.ds(0, SEQ - ROWS)]
            pltpu.make_async_copy(part, part, orecv_sem.at[u]).wait()

        def dx_step(i, _, u=u):
            cols = pl.ds(pl.multiple_of(i * ND, ND), ND)
            t = dot_nt(jnp.concatenate(unit_lhs(u), axis=1), jnp.concatenate(unit_w(u, cols), axis=1))
            if u > 0:
                t = t + acc[:, cols]
            acc[:, cols] = t
            return 0

        with scope('dx'):
            lax.fori_loop(0, D // ND, dx_step, 0)
    for cp in p_copies():
        cp.start()

    for n in range(2):
        with scope('waitdv'):
            part = obuf.at[0, pl.ds(0, (3, 4)[n] * TOK)]
            pltpu.make_async_copy(part, part, dv_sem.at[n]).wait()
            if n == 0:
                for cp in p_copies():
                    cp.wait_recv()
        chips = [lax.rem(chip + N_CHIP - k, N_CHIP) for k in ((0, 1), (2, 3))[n]]
        heads = [c + 4 * r for c in chips for r in range(2)]

        def dv_step(i, _, n=n, heads=heads):
            cols = pl.ds(pl.multiple_of(i * ND, ND), ND)
            t = dot_nt(jnp.concatenate([rv[h] for h in heads], axis=1),
                       jnp.concatenate([wv_r[h, cols, :] for h in heads], axis=1))
            if n == 0:
                for h in range(2):
                    rows = slice(h * SEG, (h + 1) * SEG)
                    pbuf[rows, cols] = t[rows] + (acc[own[h], cols] + pbuf[rows, cols])
            else:
                out_ref[:, cols] = (t + pbuf[:, cols]).astype(BF16)
            return 0

        with scope('dxv'):
            lax.fori_loop(0, D // ND, dv_step, 0)

    with scope('final'):
        for n in range(2):
            for cp in swap_copies(n):
                cp.wait_send()
        for cp in p_copies():
            cp.wait_send()
        pltpu.make_async_copy(sbuf, sbuf, send_sem).wait()
        part = obuf.at[pl.ds(0, 4), pl.ds(0, SEQ - ROWS)]
        pltpu.make_async_copy(part, part, osend_sem).wait()
        part = obuf.at[4, pl.ds(0, SEQ - TOK)]
        pltpu.make_async_copy(part, part, osend_sem).wait()


def write_out(src, dst, sem):
    cp = pltpu.make_async_copy(src, dst, sem)
    cp.start()
    cp.wait()


def solution(mesh):
    row_spec = P(("dp", "cp"), None)

    def device_fn(x_in, d_y, w_q, w_k, w_v, w_o):
        dma = pltpu.SemaphoreType.DMA
        res = pl.pallas_call(
            kernel,
            out_shape=pltpu.VMEM((TOK, D), BF16),
            in_specs=[pl.BlockSpec(memory_space=pl.ANY)] * 6,
            out_specs=pl.BlockSpec(memory_space=pltpu.VMEM),
            scratch_shapes=[
                pltpu.VMEM((ROWS, D), BF16),
                pltpu.VMEM((ROWS, D), BF16),
                pltpu.VMEM((G, N_CHIP, HD, D), BF16),
                pltpu.VMEM((SLOTS, 256, 3, 4, HD), BF16),
                pltpu.VMEM((12, D, HD), BF16),
                pltpu.VMEM((4, D, HD), BF16),
                pltpu.VMEM((8, D, HD), BF16),
                pltpu.VMEM((8, 3, ROWS, HD), BF16),
                pltpu.VMEM((8, SEQ, HD), BF16),
                pltpu.VMEM((5, SEQ, HD), BF16),
                pltpu.VMEM((16, ROWS, HD), BF16),
                pltpu.VMEM((8, TOK, HD), BF16),
                pltpu.VMEM((ROWS, D), F32),
                pltpu.VMEM((TOK, D), F32),
                *[pltpu.VMEM(((b + 1) * BQ, BQ), t) for t in (F32, F32, BF16, BF16) for b in range(NB)],
                pltpu.VMEM((HD, SEQ), BF16),
                pltpu.VMEM((HD, SEQ), BF16),
                pltpu.VMEM((SEQ, HD), F32),
                pltpu.VMEM((SEQ, HD), F32),
                dma((2, 2)), dma((G, N_CHIP)), dma((SLOTS,)), dma((2, 2)), dma((2, 2)),
                dma, dma((8,)), dma, dma((4,)), dma((2,)), dma((2,)), dma((2,)),
            ],
            compiler_params=pltpu.CompilerParams(
                collective_id=0, has_side_effects=True, vmem_limit_bytes=VLIM),
        )(x_in, d_y, w_q.reshape(12, 256, 6, 4, HD), w_k.reshape(4, 256, 3, 2, 4, HD), w_v.reshape(4, 256, 3, 2, 4, HD),
          w_o.reshape(2, N_CHIP, G, HD, D))
        return pl.pallas_call(
            write_out,
            out_shape=jax.ShapeDtypeStruct((TOK, D), BF16),
            in_specs=[pl.BlockSpec(memory_space=pltpu.VMEM)],
            out_specs=pl.BlockSpec(memory_space=pl.ANY),
            scratch_shapes=[pltpu.SemaphoreType.DMA],
        )(pltpu.with_memory_space_constraint(res, pltpu.VMEM))

    return jax.shard_map(device_fn, mesh=mesh, in_specs=(row_spec, row_spec, P(), P(), P(), P()),
                         out_specs=row_spec, check_vma=False)
```

```python
import math

import jax
import jax.numpy as jnp
from jax import lax
from jax.experimental import pallas as pl
from jax.experimental.pallas import tpu as pltpu
from jax.sharding import PartitionSpec as P

MESH = pl.DeviceIdType.MESH
BF16, F32 = jnp.bfloat16, jnp.float32
NT = (((1,), (1,)), ((), ()))

N_DEV, N_CHIP, TOK, SEG = 8, 4, 128, 64
ROWS = 2 * TOK
SEQ = N_DEV * TOK
D = 3072
HD = 128
G = 3
BQ = 256
NB = SEQ // BQ
C = HD**-0.5
C2 = C * math.log2(math.e)
U_DO, U_K, U_V, U_Q = 0, 3, 4, 5
SLOTS = 8
RB = 128
ND = 1536
NV = 3072
VLIM = 66_000_000

scope = jax.named_scope


def dot_nt(a, b):
    return lax.dot_general(a, b, NT, preferred_element_type=F32)


def dot(a, b):
    return jnp.dot(a, b, preferred_element_type=F32)


def kernel(x_hbm, dy_hbm, wq_hbm, wk_hbm, wv_hbm, wo_hbm, out_ref,
           x_v, dy_v, wo_s, w_s, wq_r, wk_r, wv_r, sbuf, recv, obuf, rin, fwd, acc, pbuf,
           s0, s1, s2, s3, d0, d1, d2, d3, p0, p1, p2, p3, e0, e1, e2, e3, kt, vt, dk_acc, dv_acc,
           io_sem, wo_sem, w_sem, xs_sem, xr_sem, send_sem, recv_sem, osend_sem, orecv_sem, fs_sem, fr_sem, ps_sem, pr_sem):
    s_scr, dp_scr, p_scr, ds_scr = (s0, s1, s2, s3), (d0, d1, d2, d3), (p0, p1, p2, p3), (e0, e1, e2, e3)
    me = lax.axis_index("cp")
    dp = lax.axis_index("dp")
    chip = me // 2
    q = lax.rem(me, 2)
    partner = (dp, 2 * chip + 1 - q)

    def peer(k):
        return lax.rem(chip + k, N_CHIP)

    def dev_of(cc):
        return (dp, 2 * cc + q)

    barrier = pltpu.get_barrier_semaphore()
    pl.semaphore_signal(barrier, inc=1, device_id=partner, device_id_type=MESH)
    for k in range(1, N_CHIP):
        pl.semaphore_signal(barrier, inc=1, device_id=dev_of(peer(k)), device_id_type=MESH)

    def blk(i):
        return pl.ds(pl.multiple_of(i * SEG, SEG), SEG)

    own = (blk(q), blk(3 - q))
    other = (blk(1 - q), blk(2 + q))

    def io_copies(n):
        src, dst = ((dy_hbm, dy_v), (x_hbm, x_v))[n]
        return [pltpu.make_async_copy(src.at[pl.ds(h * SEG, SEG)], dst.at[own[h]], io_sem.at[n, h]) for h in range(2)]

    def swap_copies(n):
        ref = (dy_v, x_v)[n]
        return [pltpu.make_async_remote_copy(
            src_ref=ref.at[own[h]], dst_ref=ref.at[own[h]], send_sem=xs_sem.at[n, h], recv_sem=xr_sem.at[n, h],
            device_id=partner, device_id_type=MESH) for h in range(2)]

    def wo_copy(g, k):
        return pltpu.make_async_copy(wo_hbm.at[q, peer(k), g], wo_s.at[g, k - 1], wo_sem.at[g, k - 1])

    def wkv_copy(w_hbm, i, slot, half=None):
        half = q if half is None else half
        return pltpu.make_async_copy(w_hbm.at[i, :, :, half], w_s.at[slot], w_sem.at[slot])

    def wq_copy(i, slot):
        return pltpu.make_async_copy(wq_hbm.at[i, :, pl.ds(3 * q, 3)], w_s.at[slot], w_sem.at[slot])

    def wait_slot(slot):
        wkv_copy(wk_hbm, 0, slot).wait()

    for cp in io_copies(0):
        cp.start()
    for k in (1, 2):
        wo_copy(0, k).start()
    dk_acc[...] = jnp.zeros_like(dk_acc)
    dv_acc[...] = jnp.zeros_like(dv_acc)
    with scope('barrier'):
        pl.semaphore_wait(barrier, N_CHIP)
    with scope('swapdy'):
        for cp, sw in zip(io_copies(0), swap_copies(0)):
            cp.wait()
            sw.start()
    for k in (3, 4):
        wo_copy(0, k).start()
    for cp in io_copies(1):
        cp.start()

    def relay_kv(dst, base, i, slot):
        flat = w_s.at[slot].reshape(768 * 4, HD)
        for h in range(4):
            for r in range(0, 768, RB):
                dst[base + h, pl.ds(i * 768 + r, RB), :] = flat[pl.ds(4 * r + h, RB, stride=4), :]

    def relay_q(i, slot):
        flat = w_s.at[slot].reshape(768 * 4, HD)
        for h in range(12):
            for r in range(0, 256, RB):
                wq_r[h, pl.ds(i * 256 + r, RB), :] = flat[pl.ds(12 * r + h, RB, stride=12), :]


    def row_of(b):
        return pl.ds(pl.multiple_of(jnp.where(b < 2, chip * TOK, SEQ - 2 * TOK - chip * TOK) + b * SEG, SEG), SEG)

    def send_rows(unit, k, val, blocks):
        for n, b in enumerate(blocks):
            part = val[n * SEG:(n + 1) * SEG]
            if k == N_CHIP:
                recv[unit, row_of(b), :] = part
            else:
                src = sbuf.at[unit, k - 1, blk(b)]
                src[...] = part
                pltpu.make_async_remote_copy(
                    src_ref=src, dst_ref=recv.at[unit, row_of(b)], send_sem=send_sem, recv_sem=recv_sem.at[unit],
                    device_id=dev_of(peer(k)), device_id_type=MESH).start()

    def send_block(unit, k, val):
        if k == N_CHIP:
            recv[unit, pl.ds(pl.multiple_of(chip * TOK, TOK), TOK), :] = val[:TOK]
            recv[unit, pl.ds(pl.multiple_of(SEQ - TOK - chip * TOK, TOK), TOK), :] = val[TOK:]
            return
        sbuf[unit, k - 1] = val
        for half, row in ((0, chip * TOK), (1, SEQ - TOK - chip * TOK)):
            pltpu.make_async_remote_copy(
                src_ref=sbuf.at[unit, k - 1, pl.ds(half * TOK, TOK)],
                dst_ref=recv.at[unit, pl.ds(pl.multiple_of(row, TOK), TOK)],
                send_sem=send_sem, recv_sem=recv_sem.at[unit],
                device_id=dev_of(peer(k)), device_id_type=MESH).start()

    def do0_rows(blocks, ids, ks):
        lhs = jnp.concatenate([dy_v[b, :] for b in blocks], axis=0)
        w = wo_s[0, pl.ds(ks[0] - 1, len(ks))].reshape(len(ks) * HD, D)
        val = dot_nt(lhs, w).astype(BF16)
        for n, k in enumerate(ks):
            send_rows(U_DO, k, val[:, n * HD:(n + 1) * HD], ids)

    def do_steps(g):
        for k in range(1, 5):
            wo_copy(g, k).wait()
        val = dot_nt(dy_v[...], wo_s[g].reshape(4 * HD, D)).astype(BF16)
        for k in range(1, 5):
            send_block(U_DO + g, k, val[:, (k - 1) * HD:k * HD])

    def kv_steps():
        for k in (1, 3):
            c0, c1 = peer(k), peer(k + 1)
            w = jnp.concatenate([wk_r[c0], wv_r[4 * q + c0], wk_r[c1], wv_r[4 * q + c1]], axis=1)
            val = dot(x_v[...], w).astype(BF16)
            for n in range(2):
                send_block(U_K, k + n, val[:, 2 * n * HD:(2 * n + 1) * HD])
                send_block(U_V, k + n, val[:, (2 * n + 1) * HD:(2 * n + 2) * HD])

    def q_steps(g):
        w = jnp.concatenate([wq_r[3 * peer(k) + g] for k in range(1, 5)], axis=1)
        val = dot(x_v[...], w).astype(BF16)
        for k in range(1, 5):
            send_block(U_Q + g, k, val[:, (k - 1) * HD:k * HD])

    own_ids, other_ids = (q, 3 - q), (1 - q, 2 + q)
    with scope('do0a'):
        for k in (1, 2):
            wo_copy(0, k).wait()
        do0_rows(own, own_ids, (1, 2))
    for i in range(4):
        wkv_copy(wk_hbm, i, i).start()
    with scope('do0b'):
        for k in (3, 4):
            wo_copy(0, k).wait()
        do0_rows(own, own_ids, (3, 4))
    for i in range(4):
        wkv_copy(wv_hbm, i, 4 + i).start()
    with scope('swapx'):
        for cp, sw in zip(io_copies(1), swap_copies(1)):
            cp.wait()
            sw.start()
    with scope('dyswap'):
        for cp in swap_copies(0):
            cp.wait_recv()
    with scope('do0c'):
        do0_rows(other, other_ids, (1, 2, 3, 4))
    for k in range(1, 5):
        wo_copy(1, k).start()
    with scope('relk'):
        for i in range(4):
            wait_slot(i)
            relay_kv(wk_r, 0, i, i)
            wq_copy(i, i).start()
    with scope('relv'):
        for i in range(4):
            wait_slot(4 + i)
            relay_kv(wv_r, 4 * q, i, 4 + i)
            wq_copy(4 + i, 4 + i).start()
    for k in range(1, 5):
        wo_copy(2, k).start()
    with scope('xswap'):
        for cp in swap_copies(1):
            cp.wait_recv()
    with scope('kv'):
        kv_steps()
    with scope('relq'):
        for i in range(12):
            slot = i % SLOTS
            wait_slot(slot)
            relay_q(i, slot)
            if i < 4:
                wq_copy(i + SLOTS, slot).start()
            elif i < 8:
                wkv_copy(wv_hbm, i - 4, slot, 1 - q).start()
    with scope('q0'):
        q_steps(0)
    for g in (1, 2):
        with scope('do12'):
            do_steps(g)
        with scope('q12'):
            q_steps(g)
    with scope('relv2'):
        for i in range(4):
            wait_slot(4 + i)
            relay_kv(wv_r, 4 - 4 * q, i, 4 + i)

    def wait_unit(u):
        part = recv.at[u, pl.ds(0, SEQ - ROWS)]
        pltpu.make_async_copy(part, part, recv_sem.at[u]).wait()

    with scope('waitkv'):
        wait_unit(U_K)
        wait_unit(U_V)
    kt[...] = recv[U_K].T
    vt[...] = recv[U_V].T

    def rin_slot(u):
        return G * chip + u if not isinstance(u, int) or u < G else 12 + 4 * (u - G) + chip

    def send_out(u):
        slot = rin_slot(u)
        for k in range(1, N_CHIP):
            cc = peer(k)
            for half, row in ((0, cc * TOK), (1, SEQ - TOK - cc * TOK)):
                pltpu.make_async_remote_copy(
                    src_ref=obuf.at[u, pl.ds(pl.multiple_of(row, TOK), TOK)],
                    dst_ref=rin.at[slot, pl.ds(half * TOK, TOK)],
                    send_sem=osend_sem, recv_sem=orecv_sem.at[u],
                    device_id=dev_of(cc), device_id_type=MESH).start()
        rin[slot, :TOK, :] = obuf[u, pl.ds(pl.multiple_of(chip * TOK, TOK), TOK), :]
        rin[slot, TOK:, :] = obuf[u, pl.ds(pl.multiple_of(SEQ - TOK - chip * TOK, TOK), TOK), :]

    def attn_head(g, _):
        with scope('waitq'):
            wait_unit(U_DO + g)
            wait_unit(U_Q + g)
        st = [{} for _ in range(NB)]

        def rows_of(b):
            return slice(b * BQ, (b + 1) * BQ)

        def chunks(b):
            return [slice(k * BQ, (k + 1) * BQ) for k in range(b + 1)]

        def scores(b):
            qb = recv[U_Q + g, rows_of(b), :]
            dob = recv[U_DO + g, rows_of(b), :]
            mx = None
            for kc, ks in enumerate(chunks(b)):
                s = dot_nt(recv[U_K, ks, :], qb)
                if kc == b:
                    key = lax.broadcasted_iota(jnp.int32, (BQ, BQ), 0)
                    qry = lax.broadcasted_iota(jnp.int32, (BQ, BQ), 1)
                    s = jnp.where(key <= qry, s, -jnp.inf)
                s_scr[b][ks, :] = s
                mc = jnp.max(s.reshape(BQ // 8, 8, BQ), axis=0)
                mx = mc if mx is None else jnp.maximum(mx, mc)
            for ks in chunks(b):
                dp_scr[b][ks, :] = dot_nt(recv[U_V, ks, :], dob)
            st[b]['m2'] = jnp.max(mx, axis=0, keepdims=True) * C2

        def probs(b):
            m2 = st[b]['m2']
            ls = None
            for ks in chunks(b):
                e = jnp.exp2(s_scr[b][ks, :] * C2 - m2)
                lc = jnp.sum(e.reshape(BQ // 8, 8, BQ), axis=0)
                ls = lc if ls is None else ls + lc
            lse2 = m2 + jnp.log2(jnp.sum(ls, axis=0, keepdims=True))
            for ks in chunks(b):
                p_scr[b][ks, :] = jnp.exp2(s_scr[b][ks, :] * C2 - lse2).astype(BF16)

        def outs(b):
            n = (b + 1) * BQ
            dob = recv[U_DO + g, rows_of(b), :]
            ot = dot(vt[:, :n], p_scr[b][...]).astype(BF16)
            st[b]['delta'] = jnp.sum(dob.T.astype(F32) * ot.astype(F32), axis=0, keepdims=True)
            for ks in chunks(b):
                dv_acc[ks, :] += dot(p_scr[b][ks, :], dob)

        def dscores(b):
            delta = st[b]['delta']
            for ks in chunks(b):
                ds_scr[b][ks, :] = (p_scr[b][ks, :].astype(F32) * (dp_scr[b][ks, :] - delta)).astype(BF16)

        def grads(b):
            n = (b + 1) * BQ
            qb = recv[U_Q + g, rows_of(b), :]
            for ks in chunks(b):
                dk_acc[ks, :] += dot(ds_scr[b][ks, :], qb)
            dqt = (dot(kt[:, :n], ds_scr[b][...]) * C).astype(BF16)
            obuf[g, rows_of(b), :] = dqt.T

        with scope('attn'):
            scores(3)
            scores(2)
            probs(3)
            outs(3)
            scores(1)
            dscores(3)
            probs(2)
            grads(3)
            outs(2)
            scores(0)
            dscores(2)
            probs(1)
            grads(2)
            outs(1)
            dscores(1)
            probs(0)
            grads(1)
            outs(0)
            dscores(0)
            grads(0)

        with scope('send'):
            send_out(g)
        return 0

    lax.fori_loop(0, G, attn_head, 0)
    with scope('senddkv'):
        obuf[3] = (dk_acc[...] * C).astype(BF16)
        send_out(3)
        obuf[4] = dv_acc[...].astype(BF16)
        send_out(4)

    def unit_w(u, cols):
        if u < G:
            return [wq_r[G * j + u, cols, :] for j in range(N_CHIP)]
        return [wk_r[j, cols, :] for j in range(N_CHIP)]

    def unit_lhs(u):
        return [rin[G * j + u if u < G else 12 + 4 * (u - G) + j] for j in range(N_CHIP)]

    def p_copies():
        return [pltpu.make_async_remote_copy(
            src_ref=acc.at[other[h]], dst_ref=pbuf.at[pl.ds(h * SEG, SEG)],
            send_sem=ps_sem.at[h], recv_sem=pr_sem.at[h],
            device_id=partner, device_id_type=MESH) for h in range(2)]

    for u in range(4):
        with scope('waito'):
            part = obuf.at[u, pl.ds(0, SEQ - ROWS)]
            pltpu.make_async_copy(part, part, orecv_sem.at[u]).wait()

        def dx_step(i, _, u=u):
            cols = pl.ds(pl.multiple_of(i * ND, ND), ND)
            t = dot_nt(jnp.concatenate(unit_lhs(u), axis=1), jnp.concatenate(unit_w(u, cols), axis=1))
            if u > 0:
                t = t + acc[:, cols]
            acc[:, cols] = t
            return 0

        with scope('dx'):
            lax.fori_loop(0, D // ND, dx_step, 0)
    for cp in p_copies():
        cp.start()

    def f_copies():
        return [pltpu.make_async_remote_copy(
            src_ref=rin.at[pl.ds(16, 4), other[h]], dst_ref=fwd.at[:, pl.ds(h * SEG, SEG)],
            send_sem=fs_sem.at[h], recv_sem=fr_sem.at[h],
            device_id=partner, device_id_type=MESH) for h in range(2)]

    with scope('waitdv'):
        part = obuf.at[4, pl.ds(0, SEQ - ROWS)]
        pltpu.make_async_copy(part, part, orecv_sem.at[4]).wait()
    for cp in f_copies():
        cp.start()
    with scope('waitp'):
        for cp in p_copies():
            cp.wait_recv()

    def dv_own(i, _):
        cols = pl.ds(pl.multiple_of(i * NV, NV), NV)
        lhs = jnp.concatenate([rin[pl.ds(16, 4), o, :] for o in own], axis=1)
        lhs = jnp.concatenate([lhs[j] for j in range(N_CHIP)], axis=1)
        t = dot_nt(lhs, jnp.concatenate([wv_r[4 * q + j, cols, :] for j in range(N_CHIP)], axis=1))
        for h in range(2):
            rows = slice(h * SEG, (h + 1) * SEG)
            pbuf[rows, cols] = t[rows] + (acc[own[h], cols] + pbuf[rows, cols])
        return 0

    def dv_other(i, _):
        cols = pl.ds(pl.multiple_of(i * NV, NV), NV)
        t = dot_nt(jnp.concatenate([fwd[j] for j in range(N_CHIP)], axis=1),
                   jnp.concatenate([wv_r[4 - 4 * q + j, cols, :] for j in range(N_CHIP)], axis=1))
        out_ref[:, cols] = (t + pbuf[:, cols]).astype(BF16)
        return 0

    with scope('dv_own'):
        lax.fori_loop(0, D // NV, dv_own, 0)
    with scope('waitf'):
        for cp in f_copies():
            cp.wait_recv()
    with scope('dv_other'):
        lax.fori_loop(0, D // NV, dv_other, 0)

    with scope('final'):
        for n in range(2):
            for cp in swap_copies(n):
                cp.wait_send()
        for cp in p_copies():
            cp.wait_send()
        pltpu.make_async_copy(sbuf, sbuf, send_sem).wait()
        for cp in f_copies():
            cp.wait_send()
        part = obuf.at[:, pl.ds(0, SEQ - ROWS)]
        pltpu.make_async_copy(part, part, osend_sem).wait()


def write_out(src, dst, sem):
    cp = pltpu.make_async_copy(src, dst, sem)
    cp.start()
    cp.wait()


def solution(mesh):
    row_spec = P(("dp", "cp"), None)

    def device_fn(x_in, d_y, w_q, w_k, w_v, w_o):
        dma = pltpu.SemaphoreType.DMA
        res = pl.pallas_call(
            kernel,
            out_shape=pltpu.VMEM((TOK, D), BF16),
            in_specs=[pl.BlockSpec(memory_space=pl.ANY)] * 6,
            out_specs=pl.BlockSpec(memory_space=pltpu.VMEM),
            scratch_shapes=[
                pltpu.VMEM((ROWS, D), BF16),
                pltpu.VMEM((ROWS, D), BF16),
                pltpu.VMEM((G, N_CHIP, HD, D), BF16),
                pltpu.VMEM((SLOTS, 256, 3, 4, HD), BF16),
                pltpu.VMEM((12, D, HD), BF16),
                pltpu.VMEM((4, D, HD), BF16),
                pltpu.VMEM((8, D, HD), BF16),
                pltpu.VMEM((8, 3, ROWS, HD), BF16),
                pltpu.VMEM((8, SEQ, HD), BF16),
                pltpu.VMEM((5, SEQ, HD), BF16),
                pltpu.VMEM((20, ROWS, HD), BF16),
                pltpu.VMEM((4, TOK, HD), BF16),
                pltpu.VMEM((ROWS, D), F32),
                pltpu.VMEM((TOK, D), F32),
                *[pltpu.VMEM(((b + 1) * BQ, BQ), t) for t in (F32, F32, BF16, BF16) for b in range(NB)],
                pltpu.VMEM((HD, SEQ), BF16),
                pltpu.VMEM((HD, SEQ), BF16),
                pltpu.VMEM((SEQ, HD), F32),
                pltpu.VMEM((SEQ, HD), F32),
                dma((2, 2)), dma((G, N_CHIP)), dma((SLOTS,)), dma((2, 2)), dma((2, 2)),
                dma, dma((8,)), dma, dma((5,)), dma((2,)), dma((2,)), dma((2,)), dma((2,)),
            ],
            compiler_params=pltpu.CompilerParams(
                collective_id=0, has_side_effects=True, vmem_limit_bytes=VLIM),
        )(x_in, d_y, w_q.reshape(12, 256, 6, 4, HD), w_k.reshape(4, 256, 3, 2, 4, HD), w_v.reshape(4, 256, 3, 2, 4, HD),
          w_o.reshape(2, N_CHIP, G, HD, D))
        return pl.pallas_call(
            write_out,
            out_shape=jax.ShapeDtypeStruct((TOK, D), BF16),
            in_specs=[pl.BlockSpec(memory_space=pltpu.VMEM)],
            out_specs=pl.BlockSpec(memory_space=pl.ANY),
            scratch_shapes=[pltpu.SemaphoreType.DMA],
        )(pltpu.with_memory_space_constraint(res, pltpu.VMEM))

    return jax.shard_map(device_fn, mesh=mesh, in_specs=(row_spec, row_spec, P(), P(), P(), P()),
                         out_specs=row_spec, check_vma=False)
```

```python
import math

import jax
import jax.numpy as jnp
from jax import lax
from jax.experimental import pallas as pl
from jax.experimental.pallas import tpu as pltpu
from jax.sharding import PartitionSpec as P

MESH = pl.DeviceIdType.MESH
BF16, F32 = jnp.bfloat16, jnp.float32
NT = (((1,), (1,)), ((), ()))

N_DEV, N_CHIP, TOK, SEG = 8, 4, 128, 64
ROWS = 2 * TOK
SEQ = N_DEV * TOK
D = 3072
HD = 128
G = 3
BQ = 256
NB = SEQ // BQ
C = HD**-0.5
C2 = C * math.log2(math.e)
U_DO, U_K, U_V, U_Q = 0, 3, 4, 5
SLOTS = 8
RB = 128
ND = 1536
NV = 3072
VLIM = 66_000_000

scope = jax.named_scope


def dot_nt(a, b):
    return lax.dot_general(a, b, NT, preferred_element_type=F32)


def dot(a, b):
    return jnp.dot(a, b, preferred_element_type=F32)


def kernel(x_hbm, dy_hbm, wq_hbm, wk_hbm, wv_hbm, wo_hbm, out_ref,
           x_v, dy_v, wo_s, w_s, wq_r, wk_r, wv_r, sbuf, recv, obuf, rin, rkv, acc, pbuf,
           s0, s1, s2, s3, d0, d1, d2, d3, p0, p1, p2, p3, e0, e1, e2, e3, kt, vt, dk_acc, dv_acc,
           io_sem, wo_sem, w_sem, xs_sem, xr_sem, send_sem, recv_sem, osend_sem, orecv_sem, kv_sem, ps_sem, pr_sem):
    s_scr, dp_scr, p_scr, ds_scr = (s0, s1, s2, s3), (d0, d1, d2, d3), (p0, p1, p2, p3), (e0, e1, e2, e3)
    me = lax.axis_index("cp")
    dp = lax.axis_index("dp")
    chip = me // 2
    q = lax.rem(me, 2)
    partner = (dp, 2 * chip + 1 - q)

    def peer(k):
        return lax.rem(chip + k, N_CHIP)

    def dev_of(cc):
        return (dp, 2 * cc + q)

    barrier = pltpu.get_barrier_semaphore()
    pl.semaphore_signal(barrier, inc=1, device_id=partner, device_id_type=MESH)
    for k in range(1, N_CHIP):
        pl.semaphore_signal(barrier, inc=1, device_id=dev_of(peer(k)), device_id_type=MESH)

    def blk(i):
        return pl.ds(pl.multiple_of(i * SEG, SEG), SEG)

    own = (blk(q), blk(3 - q))
    other = (blk(1 - q), blk(2 + q))

    def io_copies(n):
        src, dst = ((dy_hbm, dy_v), (x_hbm, x_v))[n]
        return [pltpu.make_async_copy(src.at[pl.ds(h * SEG, SEG)], dst.at[own[h]], io_sem.at[n, h]) for h in range(2)]

    def swap_copies(n):
        ref = (dy_v, x_v)[n]
        return [pltpu.make_async_remote_copy(
            src_ref=ref.at[own[h]], dst_ref=ref.at[own[h]], send_sem=xs_sem.at[n, h], recv_sem=xr_sem.at[n, h],
            device_id=partner, device_id_type=MESH) for h in range(2)]

    def wo_copy(g, k):
        return pltpu.make_async_copy(wo_hbm.at[q, peer(k), g], wo_s.at[g, k - 1], wo_sem.at[g, k - 1])

    def wkv_copy(w_hbm, i, slot, half=None):
        half = q if half is None else half
        return pltpu.make_async_copy(w_hbm.at[i, :, :, half], w_s.at[slot], w_sem.at[slot])

    def wq_copy(i, slot):
        return pltpu.make_async_copy(wq_hbm.at[i, :, pl.ds(3 * q, 3)], w_s.at[slot], w_sem.at[slot])

    def wait_slot(slot):
        wkv_copy(wk_hbm, 0, slot).wait()

    for cp in io_copies(0):
        cp.start()
    for k in (1, 2):
        wo_copy(0, k).start()
    dk_acc[...] = jnp.zeros_like(dk_acc)
    dv_acc[...] = jnp.zeros_like(dv_acc)
    with scope('barrier'):
        pl.semaphore_wait(barrier, N_CHIP)
    for cp in io_copies(1):
        cp.start()
    for k in (3, 4):
        wo_copy(0, k).start()
    with scope('swapdy'):
        for cp, sw in zip(io_copies(0), swap_copies(0)):
            cp.wait()
            sw.start()
    for i in range(4):
        wkv_copy(wk_hbm, i, i).start()

    def relay_kv(dst, base, i, slot):
        flat = w_s.at[slot].reshape(768 * 4, HD)
        for h in range(4):
            for r in range(0, 768, RB):
                dst[base + h, pl.ds(i * 768 + r, RB), :] = flat[pl.ds(4 * r + h, RB, stride=4), :]

    def relay_q(i, slot):
        flat = w_s.at[slot].reshape(768 * 4, HD)
        for h in range(12):
            for r in range(0, 256, RB):
                wq_r[h, pl.ds(i * 256 + r, RB), :] = flat[pl.ds(12 * r + h, RB, stride=12), :]


    def row_of(b):
        return pl.ds(pl.multiple_of(jnp.where(b < 2, chip * TOK, SEQ - 2 * TOK - chip * TOK) + b * SEG, SEG), SEG)

    def send_rows(unit, k, val, blocks):
        for n, b in enumerate(blocks):
            part = val[n * SEG:(n + 1) * SEG]
            if k == N_CHIP:
                recv[unit, row_of(b), :] = part
            else:
                src = sbuf.at[unit, k - 1, blk(b)]
                src[...] = part
                pltpu.make_async_remote_copy(
                    src_ref=src, dst_ref=recv.at[unit, row_of(b)], send_sem=send_sem, recv_sem=recv_sem.at[unit],
                    device_id=dev_of(peer(k)), device_id_type=MESH).start()

    def send_block(unit, k, val):
        if k == N_CHIP:
            recv[unit, pl.ds(pl.multiple_of(chip * TOK, TOK), TOK), :] = val[:TOK]
            recv[unit, pl.ds(pl.multiple_of(SEQ - TOK - chip * TOK, TOK), TOK), :] = val[TOK:]
            return
        sbuf[unit, k - 1] = val
        for half, row in ((0, chip * TOK), (1, SEQ - TOK - chip * TOK)):
            pltpu.make_async_remote_copy(
                src_ref=sbuf.at[unit, k - 1, pl.ds(half * TOK, TOK)],
                dst_ref=recv.at[unit, pl.ds(pl.multiple_of(row, TOK), TOK)],
                send_sem=send_sem, recv_sem=recv_sem.at[unit],
                device_id=dev_of(peer(k)), device_id_type=MESH).start()

    def do0_rows(blocks, ids, ks):
        lhs = jnp.concatenate([dy_v[b, :] for b in blocks], axis=0)
        w = wo_s[0, pl.ds(ks[0] - 1, len(ks))].reshape(len(ks) * HD, D)
        val = dot_nt(lhs, w).astype(BF16)
        for n, k in enumerate(ks):
            send_rows(U_DO, k, val[:, n * HD:(n + 1) * HD], ids)

    def do_steps(g):
        for k in range(1, 5):
            wo_copy(g, k).wait()
        val = dot_nt(dy_v[...], wo_s[g].reshape(4 * HD, D)).astype(BF16)
        for k in range(1, 5):
            send_block(U_DO + g, k, val[:, (k - 1) * HD:k * HD])

    def kv_steps(w_r, unit):
        w = jnp.concatenate([w_r[4 * q + peer(k)] for k in range(1, 5)], axis=1)
        val = dot(x_v[...], w).astype(BF16)
        for k in range(1, 5):
            send_block(unit, k, val[:, (k - 1) * HD:k * HD])

    def q_steps(g):
        w = jnp.concatenate([wq_r[3 * peer(k) + g] for k in range(1, 5)], axis=1)
        val = dot(x_v[...], w).astype(BF16)
        for k in range(1, 5):
            send_block(U_Q + g, k, val[:, (k - 1) * HD:k * HD])

    own_ids, other_ids = (q, 3 - q), (1 - q, 2 + q)
    with scope('do0a'):
        for k in (1, 2):
            wo_copy(0, k).wait()
        do0_rows(own, own_ids, (1, 2))
    for i in range(4):
        wkv_copy(wv_hbm, i, 4 + i).start()
    with scope('swapx'):
        for cp, sw in zip(io_copies(1), swap_copies(1)):
            cp.wait()
            sw.start()
    with scope('do0b'):
        for k in (3, 4):
            wo_copy(0, k).wait()
        do0_rows(own, own_ids, (3, 4))
    for k in range(1, 5):
        wo_copy(1, k).start()
    with scope('relk'):
        for i in range(4):
            wait_slot(i)
            relay_kv(wk_r, 4 * q, i, i)
            wq_copy(i, i).start()
    with scope('dyswap'):
        for cp in swap_copies(0):
            cp.wait_recv()
    with scope('do0c'):
        do0_rows(other, other_ids, (1, 2, 3, 4))
    with scope('xswap'):
        for cp in swap_copies(1):
            cp.wait_recv()
    with scope('k'):
        kv_steps(wk_r, U_K)
    with scope('relv'):
        for i in range(4):
            wait_slot(4 + i)
            relay_kv(wv_r, 4 * q, i, 4 + i)
            wq_copy(4 + i, 4 + i).start()
    for k in range(1, 5):
        wo_copy(2, k).start()
    with scope('v'):
        kv_steps(wv_r, U_V)
    with scope('relq'):
        for i in range(12):
            slot = i % SLOTS
            wait_slot(slot)
            relay_q(i, slot)
            if i < 4:
                wq_copy(i + SLOTS, slot).start()
            elif i < 8:
                wkv_copy(wk_hbm, i - 4, slot, 1 - q).start()
            else:
                wkv_copy(wv_hbm, i - 8, slot, 1 - q).start()
    with scope('q0'):
        q_steps(0)
    for g in (1, 2):
        with scope('do12'):
            do_steps(g)
        with scope('q12'):
            q_steps(g)
    with scope('relkv2'):
        for i in range(4):
            wait_slot(4 + i)
            relay_kv(wk_r, 4 - 4 * q, i, 4 + i)
            wait_slot(i)
            relay_kv(wv_r, 4 - 4 * q, i, i)

    def wait_unit(u):
        part = recv.at[u, pl.ds(0, SEQ - ROWS)]
        pltpu.make_async_copy(part, part, recv_sem.at[u]).wait()

    with scope('waitkv'):
        wait_unit(U_K)
        wait_unit(U_V)
    kt[...] = recv[U_K].T
    vt[...] = recv[U_V].T

    def send_out(u):
        slot = G * chip + u
        for k in range(1, N_CHIP):
            cc = peer(k)
            for half, row in ((0, cc * TOK), (1, SEQ - TOK - cc * TOK)):
                pltpu.make_async_remote_copy(
                    src_ref=obuf.at[u, pl.ds(pl.multiple_of(row, TOK), TOK)],
                    dst_ref=rin.at[slot, pl.ds(half * TOK, TOK)],
                    send_sem=osend_sem, recv_sem=orecv_sem.at[u],
                    device_id=dev_of(cc), device_id_type=MESH).start()
        rin[slot, :TOK, :] = obuf[u, pl.ds(pl.multiple_of(chip * TOK, TOK), TOK), :]
        rin[slot, TOK:, :] = obuf[u, pl.ds(pl.multiple_of(SEQ - TOK - chip * TOK, TOK), TOK), :]

    def attn_head(g, _):
        with scope('waitq'):
            wait_unit(U_DO + g)
            wait_unit(U_Q + g)
        st = [{} for _ in range(NB)]

        def rows_of(b):
            return slice(b * BQ, (b + 1) * BQ)

        def chunks(b):
            return [slice(k * BQ, (k + 1) * BQ) for k in range(b + 1)]

        def scores(b):
            qb = recv[U_Q + g, rows_of(b), :]
            dob = recv[U_DO + g, rows_of(b), :]
            mx = None
            for kc, ks in enumerate(chunks(b)):
                s = dot_nt(recv[U_K, ks, :], qb)
                if kc == b:
                    key = lax.broadcasted_iota(jnp.int32, (BQ, BQ), 0)
                    qry = lax.broadcasted_iota(jnp.int32, (BQ, BQ), 1)
                    s = jnp.where(key <= qry, s, -jnp.inf)
                s_scr[b][ks, :] = s
                mc = jnp.max(s.reshape(BQ // 8, 8, BQ), axis=0)
                mx = mc if mx is None else jnp.maximum(mx, mc)
            for ks in chunks(b):
                dp_scr[b][ks, :] = dot_nt(recv[U_V, ks, :], dob)
            st[b]['m2'] = jnp.max(mx, axis=0, keepdims=True) * C2

        def probs(b):
            m2 = st[b]['m2']
            ls = None
            for ks in chunks(b):
                e = jnp.exp2(s_scr[b][ks, :] * C2 - m2)
                lc = jnp.sum(e.reshape(BQ // 8, 8, BQ), axis=0)
                ls = lc if ls is None else ls + lc
            lse2 = m2 + jnp.log2(jnp.sum(ls, axis=0, keepdims=True))
            for ks in chunks(b):
                p_scr[b][ks, :] = jnp.exp2(s_scr[b][ks, :] * C2 - lse2).astype(BF16)

        def outs(b):
            n = (b + 1) * BQ
            dob = recv[U_DO + g, rows_of(b), :]
            ot = dot(vt[:, :n], p_scr[b][...]).astype(BF16)
            st[b]['delta'] = jnp.sum(dob.T.astype(F32) * ot.astype(F32), axis=0, keepdims=True)
            for ks in chunks(b):
                dv_acc[ks, :] += dot(p_scr[b][ks, :], dob)

        def dscores(b):
            delta = st[b]['delta']
            for ks in chunks(b):
                ds_scr[b][ks, :] = (p_scr[b][ks, :].astype(F32) * (dp_scr[b][ks, :] - delta)).astype(BF16)

        def grads(b):
            n = (b + 1) * BQ
            qb = recv[U_Q + g, rows_of(b), :]
            for ks in chunks(b):
                dk_acc[ks, :] += dot(ds_scr[b][ks, :], qb)
            dqt = (dot(kt[:, :n], ds_scr[b][...]) * C).astype(BF16)
            obuf[g, rows_of(b), :] = dqt.T

        with scope('attn'):
            scores(3)
            scores(2)
            probs(3)
            outs(3)
            scores(1)
            dscores(3)
            probs(2)
            grads(3)
            outs(2)
            scores(0)
            dscores(2)
            probs(1)
            grads(2)
            outs(1)
            dscores(1)
            probs(0)
            grads(1)
            outs(0)
            dscores(0)
            grads(0)

        with scope('send'):
            send_out(g)
        return 0

    lax.fori_loop(0, G, attn_head, 0)
    def seg_rows(dev, half):
        seg = dev if half == 0 else 2 * N_DEV - 1 - dev
        return pl.ds(pl.multiple_of(seg * SEG, SEG), SEG)

    def send_owners(n):
        slot = 8 * n + 4 * q + chip

        def send_dev(dev, part):
            for half in range(2):
                pltpu.make_async_remote_copy(
                    src_ref=obuf.at[G + n, seg_rows(dev, half)], dst_ref=rkv.at[slot, pl.ds(half * SEG, SEG)],
                    send_sem=osend_sem, recv_sem=kv_sem.at[n, part],
                    device_id=(dp, dev), device_id_type=MESH).start()

        send_dev(partner[1], 0)
        for k in range(1, N_CHIP):
            for r in range(2):
                send_dev(2 * peer(k) + r, k // 2)
        for half in range(2):
            rkv[slot, half * SEG:(half + 1) * SEG, :] = obuf[G + n, seg_rows(me, half), :]

    with scope('senddkv'):
        obuf[3] = (dk_acc[...] * C).astype(BF16)
        send_owners(0)
        obuf[4] = dv_acc[...].astype(BF16)
        send_owners(1)

    def p_copies():
        return [pltpu.make_async_remote_copy(
            src_ref=acc.at[other[h]], dst_ref=pbuf.at[pl.ds(h * SEG, SEG)],
            send_sem=ps_sem.at[h], recv_sem=pr_sem.at[h],
            device_id=partner, device_id_type=MESH) for h in range(2)]

    for u in range(G):
        with scope('waito'):
            part = obuf.at[u, pl.ds(0, SEQ - ROWS)]
            pltpu.make_async_copy(part, part, orecv_sem.at[u]).wait()

        def dx_step(i, _, u=u):
            cols = pl.ds(pl.multiple_of(i * ND, ND), ND)
            t = dot_nt(jnp.concatenate([rin[G * j + u] for j in range(N_CHIP)], axis=1),
                       jnp.concatenate([wq_r[G * j + u, cols, :] for j in range(N_CHIP)], axis=1))
            if u > 0:
                t = t + acc[:, cols]
            acc[:, cols] = t
            return 0

        with scope('dx'):
            lax.fori_loop(0, D // ND, dx_step, 0)
    for cp in p_copies():
        cp.start()

    for n in range(2):
        for part in range(2):
            last = n == 1 and part == 1
            with scope('waitkv%d%d' % (n, part)):
                ref = obuf.at[0, pl.ds(0, (3, 4)[part] * TOK)]
                pltpu.make_async_copy(ref, ref, kv_sem.at[n, part]).wait()
            if last:
                with scope('waitp'):
                    for cp in p_copies():
                        cp.wait_recv()
            chips = [lax.rem(chip + N_CHIP - k, N_CHIP) for k in ((0, 1), (2, 3))[part]]
            heads = [c + 4 * r for c in chips for r in range(2)]

            def kv_dx(i, _, n=n, last=last, heads=heads):
                cols = pl.ds(pl.multiple_of(i * NV, NV), NV)
                t = dot_nt(jnp.concatenate([rkv[8 * n + h] for h in heads], axis=1),
                           jnp.concatenate([(wk_r, wv_r)[n][h, cols, :] for h in heads], axis=1))
                for h in range(2):
                    rows = slice(h * SEG, (h + 1) * SEG)
                    part_t = t[rows] + acc[own[h], cols]
                    if last:
                        out_ref[rows, cols] = (part_t + pbuf[rows, cols]).astype(BF16)
                    else:
                        acc[own[h], cols] = part_t
                return 0

            with scope('kvdx'):
                lax.fori_loop(0, D // NV, kv_dx, 0)

    with scope('final'):
        for n in range(2):
            for cp in swap_copies(n):
                cp.wait_send()
        for cp in p_copies():
            cp.wait_send()
        pltpu.make_async_copy(sbuf, sbuf, send_sem).wait()
        part = obuf.at[pl.ds(0, G), pl.ds(0, SEQ - ROWS)]
        pltpu.make_async_copy(part, part, osend_sem).wait()
        part = obuf.at[pl.ds(0, 2), pl.ds(0, SEQ - TOK)]
        pltpu.make_async_copy(part, part, osend_sem).wait()


def write_out(src, dst, sem):
    cp = pltpu.make_async_copy(src, dst, sem)
    cp.start()
    cp.wait()


def solution(mesh):
    row_spec = P(("dp", "cp"), None)

    def device_fn(x_in, d_y, w_q, w_k, w_v, w_o):
        dma = pltpu.SemaphoreType.DMA
        res = pl.pallas_call(
            kernel,
            out_shape=pltpu.VMEM((TOK, D), BF16),
            in_specs=[pl.BlockSpec(memory_space=pl.ANY)] * 6,
            out_specs=pl.BlockSpec(memory_space=pltpu.VMEM),
            scratch_shapes=[
                pltpu.VMEM((ROWS, D), BF16),
                pltpu.VMEM((ROWS, D), BF16),
                pltpu.VMEM((G, N_CHIP, HD, D), BF16),
                pltpu.VMEM((SLOTS, 256, 3, 4, HD), BF16),
                pltpu.VMEM((12, D, HD), BF16),
                pltpu.VMEM((8, D, HD), BF16),
                pltpu.VMEM((8, D, HD), BF16),
                pltpu.VMEM((8, 3, ROWS, HD), BF16),
                pltpu.VMEM((8, SEQ, HD), BF16),
                pltpu.VMEM((5, SEQ, HD), BF16),
                pltpu.VMEM((12, ROWS, HD), BF16),
                pltpu.VMEM((16, TOK, HD), BF16),
                pltpu.VMEM((ROWS, D), F32),
                pltpu.VMEM((TOK, D), F32),
                *[pltpu.VMEM(((b + 1) * BQ, BQ), t) for t in (F32, F32, BF16, BF16) for b in range(NB)],
                pltpu.VMEM((HD, SEQ), BF16),
                pltpu.VMEM((HD, SEQ), BF16),
                pltpu.VMEM((SEQ, HD), F32),
                pltpu.VMEM((SEQ, HD), F32),
                dma((2, 2)), dma((G, N_CHIP)), dma((SLOTS,)), dma((2, 2)), dma((2, 2)),
                dma, dma((8,)), dma, dma((G,)), dma((2, 2)), dma((2,)), dma((2,)),
            ],
            compiler_params=pltpu.CompilerParams(
                collective_id=0, has_side_effects=True, vmem_limit_bytes=VLIM),
        )(x_in, d_y, w_q.reshape(12, 256, 6, 4, HD), w_k.reshape(4, 256, 3, 2, 4, HD), w_v.reshape(4, 256, 3, 2, 4, HD),
          w_o.reshape(2, N_CHIP, G, HD, D))
        return pl.pallas_call(
            write_out,
            out_shape=jax.ShapeDtypeStruct((TOK, D), BF16),
            in_specs=[pl.BlockSpec(memory_space=pltpu.VMEM)],
            out_specs=pl.BlockSpec(memory_space=pl.ANY),
            scratch_shapes=[pltpu.SemaphoreType.DMA],
        )(pltpu.with_memory_space_constraint(res, pltpu.VMEM))

    return jax.shard_map(device_fn, mesh=mesh, in_specs=(row_spec, row_spec, P(), P(), P(), P()),
                         out_specs=row_spec, check_vma=False)
```

```python
import math

import jax
import jax.numpy as jnp
from jax import lax
from jax.experimental import pallas as pl
from jax.experimental.pallas import tpu as pltpu
from jax.sharding import PartitionSpec as P

MESH = pl.DeviceIdType.MESH
BF16, F32 = jnp.bfloat16, jnp.float32
NT = (((1,), (1,)), ((), ()))

N_DEV, N_CHIP, TOK, SEG = 8, 4, 128, 64
ROWS = 2 * TOK
SEQ = N_DEV * TOK
D = 3072
HD = 128
G = 3
BQ = 256
NB = SEQ // BQ
C = HD**-0.5
C2 = C * math.log2(math.e)
U_DO, U_K, U_V, U_Q = 0, 3, 4, 5
SLOTS = 8
RB = 128
ND = 3072
NV = 3072
VLIM = 66_000_000

scope = jax.named_scope


def dot_nt(a, b):
    return lax.dot_general(a, b, NT, preferred_element_type=F32)


def dot(a, b):
    return jnp.dot(a, b, preferred_element_type=F32)


def kernel(x_hbm, dy_hbm, wq_hbm, wk_hbm, wv_hbm, wo_hbm, out_ref,
           x_v, dy_v, wo_s, w_s, wq_r, wk_r, wv_r, sbuf, recv, obuf, rin, rkv, acc, pbuf,
           s0, s1, s2, s3, d0, d1, d2, d3, p0, p1, p2, p3, e0, e1, e2, e3, kt, vt, dk_acc, dv_acc,
           io_sem, wo_sem, w_sem, xs_sem, xr_sem, send_sem, recv_sem, osend_sem, orecv_sem, kv_sem, ps_sem, pr_sem):
    s_scr, dp_scr, p_scr, ds_scr = (s0, s1, s2, s3), (d0, d1, d2, d3), (p0, p1, p2, p3), (e0, e1, e2, e3)
    me = lax.axis_index("cp")
    dp = lax.axis_index("dp")
    chip = me // 2
    q = lax.rem(me, 2)
    partner = (dp, 2 * chip + 1 - q)

    def peer(k):
        return lax.rem(chip + k, N_CHIP)

    def dev_of(cc):
        return (dp, 2 * cc + q)

    barrier = pltpu.get_barrier_semaphore()
    pl.semaphore_signal(barrier, inc=1, device_id=partner, device_id_type=MESH)
    for k in range(1, N_CHIP):
        pl.semaphore_signal(barrier, inc=1, device_id=dev_of(peer(k)), device_id_type=MESH)

    def blk(i):
        return pl.ds(pl.multiple_of(i * SEG, SEG), SEG)

    own = (blk(q), blk(3 - q))
    other = (blk(1 - q), blk(2 + q))

    def io_copies(n):
        src, dst = ((dy_hbm, dy_v), (x_hbm, x_v))[n]
        return [pltpu.make_async_copy(src.at[pl.ds(h * SEG, SEG)], dst.at[own[h]], io_sem.at[n, h]) for h in range(2)]

    def swap_copies(n):
        ref = (dy_v, x_v)[n]
        return [pltpu.make_async_remote_copy(
            src_ref=ref.at[own[h]], dst_ref=ref.at[own[h]], send_sem=xs_sem.at[n, h], recv_sem=xr_sem.at[n, h],
            device_id=partner, device_id_type=MESH) for h in range(2)]

    def wo_copy(g, k):
        return pltpu.make_async_copy(wo_hbm.at[q, peer(k), g], wo_s.at[g, k - 1], wo_sem.at[g, k - 1])

    def wkv_copy(w_hbm, i, slot, half=None):
        half = q if half is None else half
        return pltpu.make_async_copy(w_hbm.at[i, :, :, half], w_s.at[slot], w_sem.at[slot])

    def wq_copy(i, slot):
        return pltpu.make_async_copy(wq_hbm.at[i, :, pl.ds(3 * q, 3)], w_s.at[slot], w_sem.at[slot])

    def wait_slot(slot):
        wkv_copy(wk_hbm, 0, slot).wait()

    for cp in io_copies(0):
        cp.start()
    for k in (1, 2):
        wo_copy(0, k).start()
    dk_acc[...] = jnp.zeros_like(dk_acc)
    dv_acc[...] = jnp.zeros_like(dv_acc)
    with scope('barrier'):
        pl.semaphore_wait(barrier, N_CHIP)
    for cp in io_copies(1):
        cp.start()
    with scope('swapdy'):
        for cp, sw in zip(io_copies(0), swap_copies(0)):
            cp.wait()
            sw.start()
    for i in range(4):
        wkv_copy(wk_hbm, i, i).start()

    def relay_kv(dst, base, i, slot):
        flat = w_s.at[slot].reshape(768 * 4, HD)
        for h in range(4):
            for r in range(0, 768, RB):
                dst[base + h, pl.ds(i * 768 + r, RB), :] = flat[pl.ds(4 * r + h, RB, stride=4), :]

    def relay_q(i, slot):
        flat = w_s.at[slot].reshape(768 * 4, HD)
        for h in range(12):
            for r in range(0, 256, RB):
                wq_r[h, pl.ds(i * 256 + r, RB), :] = flat[pl.ds(12 * r + h, RB, stride=12), :]


    def row_of(b):
        return pl.ds(pl.multiple_of(jnp.where(b < 2, chip * TOK, SEQ - 2 * TOK - chip * TOK) + b * SEG, SEG), SEG)

    def send_rows(unit, k, val, blocks):
        for n, b in enumerate(blocks):
            part = val[n * SEG:(n + 1) * SEG]
            if k == N_CHIP:
                recv[unit, row_of(b), :] = part
            else:
                src = sbuf.at[unit, k - 1, blk(b)]
                src[...] = part
                pltpu.make_async_remote_copy(
                    src_ref=src, dst_ref=recv.at[unit, row_of(b)], send_sem=send_sem, recv_sem=recv_sem.at[unit],
                    device_id=dev_of(peer(k)), device_id_type=MESH).start()

    def send_block(unit, k, val):
        if k == N_CHIP:
            recv[unit, pl.ds(pl.multiple_of(chip * TOK, TOK), TOK), :] = val[:TOK]
            recv[unit, pl.ds(pl.multiple_of(SEQ - TOK - chip * TOK, TOK), TOK), :] = val[TOK:]
            return
        sbuf[unit, k - 1] = val
        for half, row in ((0, chip * TOK), (1, SEQ - TOK - chip * TOK)):
            pltpu.make_async_remote_copy(
                src_ref=sbuf.at[unit, k - 1, pl.ds(half * TOK, TOK)],
                dst_ref=recv.at[unit, pl.ds(pl.multiple_of(row, TOK), TOK)],
                send_sem=send_sem, recv_sem=recv_sem.at[unit],
                device_id=dev_of(peer(k)), device_id_type=MESH).start()

    def do0_rows(blocks, ids, ks):
        lhs = jnp.concatenate([dy_v[b, :] for b in blocks], axis=0)
        w = wo_s[0, pl.ds(ks[0] - 1, len(ks))].reshape(len(ks) * HD, D)
        val = dot_nt(lhs, w).astype(BF16)
        for n, k in enumerate(ks):
            send_rows(U_DO, k, val[:, n * HD:(n + 1) * HD], ids)

    def do_steps(g):
        for k in range(1, 5):
            wo_copy(g, k).wait()
        val = dot_nt(dy_v[...], wo_s[g].reshape(4 * HD, D)).astype(BF16)
        for k in range(1, 5):
            send_block(U_DO + g, k, val[:, (k - 1) * HD:k * HD])

    def k_rows(blocks, ids):
        lhs = jnp.concatenate([x_v[b, :] for b in blocks], axis=0)
        w = jnp.concatenate([wk_r[4 * q + peer(k)] for k in range(1, 5)], axis=1)
        val = dot(lhs, w).astype(BF16)
        for k in range(1, 5):
            send_rows(U_K, k, val[:, (k - 1) * HD:k * HD], ids)

    def v_steps():
        w = jnp.concatenate([wv_r[4 * q + peer(k)] for k in range(1, 5)], axis=1)
        val = dot(x_v[...], w).astype(BF16)
        for k in range(1, 5):
            send_block(U_V, k, val[:, (k - 1) * HD:k * HD])

    def q_steps(g):
        w = jnp.concatenate([wq_r[3 * peer(k) + g] for k in range(1, 5)], axis=1)
        val = dot(x_v[...], w).astype(BF16)
        for k in range(1, 5):
            send_block(U_Q + g, k, val[:, (k - 1) * HD:k * HD])

    own_ids, other_ids = (q, 3 - q), (1 - q, 2 + q)
    with scope('do0a'):
        for k in (1, 2):
            wo_copy(0, k).wait()
        do0_rows(own, own_ids, (1, 2))
    for i in range(4):
        wkv_copy(wv_hbm, i, 4 + i).start()
    for k in (3, 4):
        wo_copy(0, k).start()
    with scope('swapx'):
        for cp, sw in zip(io_copies(1), swap_copies(1)):
            cp.wait()
            sw.start()
    with scope('relk'):
        for i in range(4):
            wait_slot(i)
            relay_kv(wk_r, 4 * q, i, i)
            wq_copy(i, i).start()
    with scope('k_own'):
        k_rows(own, own_ids)
    with scope('xswap'):
        for cp in swap_copies(1):
            cp.wait_recv()
    with scope('k_other'):
        k_rows(other, other_ids)
    with scope('relv'):
        for i in range(4):
            wait_slot(4 + i)
            relay_kv(wv_r, 4 * q, i, 4 + i)
            wq_copy(4 + i, 4 + i).start()
    for k in range(1, 5):
        wo_copy(1, k).start()
    with scope('v'):
        v_steps()
    with scope('do0b'):
        for k in (3, 4):
            wo_copy(0, k).wait()
        do0_rows(own, own_ids, (3, 4))
    with scope('dyswap'):
        for cp in swap_copies(0):
            cp.wait_recv()
    with scope('do0c'):
        do0_rows(other, other_ids, (1, 2, 3, 4))
    for k in range(1, 5):
        wo_copy(2, k).start()
    with scope('relq'):
        for i in range(12):
            slot = i % SLOTS
            wait_slot(slot)
            relay_q(i, slot)
            if i < 4:
                wq_copy(i + SLOTS, slot).start()
            elif i < 8:
                wkv_copy(wk_hbm, i - 4, slot, 1 - q).start()
            else:
                wkv_copy(wv_hbm, i - 8, slot, 1 - q).start()
    with scope('q0'):
        q_steps(0)
    for g in (1, 2):
        with scope('do12'):
            do_steps(g)
        with scope('q12'):
            q_steps(g)
    with scope('relkv2'):
        for i in range(4):
            wait_slot(4 + i)
            relay_kv(wk_r, 4 - 4 * q, i, 4 + i)
            wait_slot(i)
            relay_kv(wv_r, 4 - 4 * q, i, i)

    def wait_unit(u):
        part = recv.at[u, pl.ds(0, SEQ - ROWS)]
        pltpu.make_async_copy(part, part, recv_sem.at[u]).wait()

    with scope('waitkv'):
        wait_unit(U_K)
        wait_unit(U_V)
    kt[...] = recv[U_K].T
    vt[...] = recv[U_V].T

    def send_out(u):
        slot = G * chip + u
        for k in range(1, N_CHIP):
            cc = peer(k)
            for half, row in ((0, cc * TOK), (1, SEQ - TOK - cc * TOK)):
                pltpu.make_async_remote_copy(
                    src_ref=obuf.at[u, pl.ds(pl.multiple_of(row, TOK), TOK)],
                    dst_ref=rin.at[slot, pl.ds(half * TOK, TOK)],
                    send_sem=osend_sem, recv_sem=orecv_sem.at[u],
                    device_id=dev_of(cc), device_id_type=MESH).start()
        rin[slot, :TOK, :] = obuf[u, pl.ds(pl.multiple_of(chip * TOK, TOK), TOK), :]
        rin[slot, TOK:, :] = obuf[u, pl.ds(pl.multiple_of(SEQ - TOK - chip * TOK, TOK), TOK), :]

    def attn_head(g, _):
        with scope('waitq'):
            wait_unit(U_DO + g)
            wait_unit(U_Q + g)
        st = [{} for _ in range(NB)]

        def rows_of(b):
            return slice(b * BQ, (b + 1) * BQ)

        def chunks(b):
            return [slice(k * BQ, (k + 1) * BQ) for k in range(b + 1)]

        def scores(b):
            qb = recv[U_Q + g, rows_of(b), :]
            dob = recv[U_DO + g, rows_of(b), :]
            mx = None
            for kc, ks in enumerate(chunks(b)):
                s = dot_nt(recv[U_K, ks, :], qb)
                if kc == b:
                    key = lax.broadcasted_iota(jnp.int32, (BQ, BQ), 0)
                    qry = lax.broadcasted_iota(jnp.int32, (BQ, BQ), 1)
                    s = jnp.where(key <= qry, s, -jnp.inf)
                s_scr[b][ks, :] = s
                mc = jnp.max(s.reshape(BQ // 8, 8, BQ), axis=0)
                mx = mc if mx is None else jnp.maximum(mx, mc)
            for ks in chunks(b):
                dp_scr[b][ks, :] = dot_nt(recv[U_V, ks, :], dob)
            st[b]['m2'] = jnp.max(mx, axis=0, keepdims=True) * C2

        def probs(b):
            m2 = st[b]['m2']
            ls = None
            for ks in chunks(b):
                e = jnp.exp2(s_scr[b][ks, :] * C2 - m2)
                lc = jnp.sum(e.reshape(BQ // 8, 8, BQ), axis=0)
                ls = lc if ls is None else ls + lc
            lse2 = m2 + jnp.log2(jnp.sum(ls, axis=0, keepdims=True))
            for ks in chunks(b):
                p_scr[b][ks, :] = jnp.exp2(s_scr[b][ks, :] * C2 - lse2).astype(BF16)

        def outs(b):
            n = (b + 1) * BQ
            dob = recv[U_DO + g, rows_of(b), :]
            ot = dot(vt[:, :n], p_scr[b][...]).astype(BF16)
            st[b]['delta'] = jnp.sum(dob.T.astype(F32) * ot.astype(F32), axis=0, keepdims=True)
            for ks in chunks(b):
                dv_acc[ks, :] += dot(p_scr[b][ks, :], dob)

        def dscores(b):
            delta = st[b]['delta']
            for ks in chunks(b):
                ds_scr[b][ks, :] = (p_scr[b][ks, :].astype(F32) * (dp_scr[b][ks, :] - delta)).astype(BF16)

        def grads(b):
            n = (b + 1) * BQ
            qb = recv[U_Q + g, rows_of(b), :]
            for ks in chunks(b):
                dk_acc[ks, :] += dot(ds_scr[b][ks, :], qb)
            dqt = (dot(kt[:, :n], ds_scr[b][...]) * C).astype(BF16)
            obuf[g, rows_of(b), :] = dqt.T

        with scope('attn'):
            scores(3)
            scores(2)
            probs(3)
            outs(3)
            scores(1)
            dscores(3)
            probs(2)
            grads(3)
            outs(2)
            scores(0)
            dscores(2)
            probs(1)
            grads(2)
            outs(1)
            dscores(1)
            probs(0)
            grads(1)
            outs(0)
            dscores(0)
            grads(0)

        with scope('send'):
            send_out(g)
        return 0

    lax.fori_loop(0, G, attn_head, 0)
    def seg_rows(dev, half):
        seg = dev if half == 0 else 2 * N_DEV - 1 - dev
        return pl.ds(pl.multiple_of(seg * SEG, SEG), SEG)

    def send_owners(n):
        slot = 8 * n + 4 * q + chip

        def send_dev(dev, part):
            for half in range(2):
                pltpu.make_async_remote_copy(
                    src_ref=obuf.at[G + n, seg_rows(dev, half)], dst_ref=rkv.at[slot, pl.ds(half * SEG, SEG)],
                    send_sem=osend_sem, recv_sem=kv_sem.at[n, part],
                    device_id=(dp, dev), device_id_type=MESH).start()

        send_dev(partner[1], 0)
        for k in range(1, N_CHIP):
            for r in range(2):
                send_dev(2 * peer(k) + r, k // 2)
        for half in range(2):
            rkv[slot, half * SEG:(half + 1) * SEG, :] = obuf[G + n, seg_rows(me, half), :]

    with scope('senddkv'):
        obuf[3] = (dk_acc[...] * C).astype(BF16)
        send_owners(0)
        obuf[4] = dv_acc[...].astype(BF16)
        send_owners(1)

    def p_copies():
        return [pltpu.make_async_remote_copy(
            src_ref=acc.at[other[h]], dst_ref=pbuf.at[pl.ds(h * SEG, SEG)],
            send_sem=ps_sem.at[h], recv_sem=pr_sem.at[h],
            device_id=partner, device_id_type=MESH) for h in range(2)]

    for u in range(G):
        with scope('waito'):
            part = obuf.at[u, pl.ds(0, SEQ - ROWS)]
            pltpu.make_async_copy(part, part, orecv_sem.at[u]).wait()

        def dx_step(i, _, u=u):
            cols = pl.ds(pl.multiple_of(i * ND, ND), ND)
            t = dot_nt(jnp.concatenate([rin[G * j + u] for j in range(N_CHIP)], axis=1),
                       jnp.concatenate([wq_r[G * j + u, cols, :] for j in range(N_CHIP)], axis=1))
            if u > 0:
                t = t + acc[:, cols]
            acc[:, cols] = t
            return 0

        with scope('dx'):
            lax.fori_loop(0, D // ND, dx_step, 0)
    for cp in p_copies():
        cp.start()

    for n, parts in ((0, (0, 1)), (1, (0,)), (1, (1,))):
            last = n == 1 and 1 in parts
            with scope('waitkv%d%d' % (n, parts[0])):
                for part in parts:
                    ref = obuf.at[0, pl.ds(0, (3, 4)[part] * TOK)]
                    pltpu.make_async_copy(ref, ref, kv_sem.at[n, part]).wait()
            if last:
                with scope('waitp'):
                    for cp in p_copies():
                        cp.wait_recv()
            chips = [lax.rem(chip + N_CHIP - k, N_CHIP) for part in parts for k in ((0, 1), (2, 3))[part]]
            heads = [c + 4 * r for c in chips for r in range(2)]

            def kv_dx(i, _, n=n, last=last, heads=heads):
                cols = pl.ds(pl.multiple_of(i * NV, NV), NV)
                t = dot_nt(jnp.concatenate([rkv[8 * n + h] for h in heads], axis=1),
                           jnp.concatenate([(wk_r, wv_r)[n][h, cols, :] for h in heads], axis=1))
                for h in range(2):
                    rows = slice(h * SEG, (h + 1) * SEG)
                    part_t = t[rows] + acc[own[h], cols]
                    if last:
                        out_ref[rows, cols] = (part_t + pbuf[rows, cols]).astype(BF16)
                    else:
                        acc[own[h], cols] = part_t
                return 0

            with scope('kvdx'):
                lax.fori_loop(0, D // NV, kv_dx, 0)

    with scope('final'):
        for n in range(2):
            for cp in swap_copies(n):
                cp.wait_send()
        for cp in p_copies():
            cp.wait_send()
        pltpu.make_async_copy(sbuf, sbuf, send_sem).wait()
        part = obuf.at[pl.ds(0, G), pl.ds(0, SEQ - ROWS)]
        pltpu.make_async_copy(part, part, osend_sem).wait()
        part = obuf.at[pl.ds(0, 2), pl.ds(0, SEQ - TOK)]
        pltpu.make_async_copy(part, part, osend_sem).wait()


def write_out(src, dst, sem):
    cp = pltpu.make_async_copy(src, dst, sem)
    cp.start()
    cp.wait()


def solution(mesh):
    row_spec = P(("dp", "cp"), None)

    def device_fn(x_in, d_y, w_q, w_k, w_v, w_o):
        dma = pltpu.SemaphoreType.DMA
        res = pl.pallas_call(
            kernel,
            out_shape=pltpu.VMEM((TOK, D), BF16),
            in_specs=[pl.BlockSpec(memory_space=pl.ANY)] * 6,
            out_specs=pl.BlockSpec(memory_space=pltpu.VMEM),
            scratch_shapes=[
                pltpu.VMEM((ROWS, D), BF16),
                pltpu.VMEM((ROWS, D), BF16),
                pltpu.VMEM((G, N_CHIP, HD, D), BF16),
                pltpu.VMEM((SLOTS, 256, 3, 4, HD), BF16),
                pltpu.VMEM((12, D, HD), BF16),
                pltpu.VMEM((8, D, HD), BF16),
                pltpu.VMEM((8, D, HD), BF16),
                pltpu.VMEM((8, 3, ROWS, HD), BF16),
                pltpu.VMEM((8, SEQ, HD), BF16),
                pltpu.VMEM((5, SEQ, HD), BF16),
                pltpu.VMEM((12, ROWS, HD), BF16),
                pltpu.VMEM((16, TOK, HD), BF16),
                pltpu.VMEM((ROWS, D), F32),
                pltpu.VMEM((TOK, D), F32),
                *[pltpu.VMEM(((b + 1) * BQ, BQ), t) for t in (F32, F32, BF16, BF16) for b in range(NB)],
                pltpu.VMEM((HD, SEQ), BF16),
                pltpu.VMEM((HD, SEQ), BF16),
                pltpu.VMEM((SEQ, HD), F32),
                pltpu.VMEM((SEQ, HD), F32),
                dma((2, 2)), dma((G, N_CHIP)), dma((SLOTS,)), dma((2, 2)), dma((2, 2)),
                dma, dma((8,)), dma, dma((G,)), dma((2, 2)), dma((2,)), dma((2,)),
            ],
            compiler_params=pltpu.CompilerParams(
                collective_id=0, has_side_effects=True, vmem_limit_bytes=VLIM),
        )(x_in, d_y, w_q.reshape(12, 256, 6, 4, HD), w_k.reshape(4, 256, 3, 2, 4, HD), w_v.reshape(4, 256, 3, 2, 4, HD),
          w_o.reshape(2, N_CHIP, G, HD, D))
        return pl.pallas_call(
            write_out,
            out_shape=jax.ShapeDtypeStruct((TOK, D), BF16),
            in_specs=[pl.BlockSpec(memory_space=pltpu.VMEM)],
            out_specs=pl.BlockSpec(memory_space=pl.ANY),
            scratch_shapes=[pltpu.SemaphoreType.DMA],
        )(pltpu.with_memory_space_constraint(res, pltpu.VMEM))

    return jax.shard_map(device_fn, mesh=mesh, in_specs=(row_spec, row_spec, P(), P(), P(), P()),
                         out_specs=row_spec, check_vma=False)
```

```python
import math

import jax
import jax.numpy as jnp
from jax import lax
from jax.experimental import pallas as pl
from jax.experimental.pallas import tpu as pltpu
from jax.sharding import PartitionSpec as P

MESH = pl.DeviceIdType.MESH
BF16, F32 = jnp.bfloat16, jnp.float32
NT = (((1,), (1,)), ((), ()))

N_DEV, N_CHIP, TOK, SEG = 8, 4, 128, 64
ROWS = 2 * TOK
SEQ = N_DEV * TOK
D = 3072
HD = 128
G = 3
BQ = 256
NB = SEQ // BQ
C = HD**-0.5
C2 = C * math.log2(math.e)
U_DO, U_K, U_V, U_Q = 0, 3, 4, 5
SLOTS = 12
RB = 128
ND = 3072
NV = 3072
VLIM = 66_000_000

scope = jax.named_scope


def dot_nt(a, b):
    return lax.dot_general(a, b, NT, preferred_element_type=F32)


def dot(a, b):
    return jnp.dot(a, b, preferred_element_type=F32)


def kernel(x_hbm, dy_hbm, wq_hbm, wk_hbm, wv_hbm, wo_hbm, out_ref,
           x_v, dy_v, wo_s, w_s, wq_r, wk_r, wv_r, sbuf, recv, obuf, rin, rkv, acc, pbuf,
           s0, s1, s2, s3, d0, d1, d2, d3, p0, p1, p2, p3, e0, e1, e2, e3, kt, vt, dk_acc, dv_acc,
           io_sem, wo_sem, w_sem, xs_sem, xr_sem, send_sem, recv_sem, osend_sem, orecv_sem, kv_sem, ps_sem, pr_sem):
    s_scr, dp_scr, p_scr, ds_scr = (s0, s1, s2, s3), (d0, d1, d2, d3), (p0, p1, p2, p3), (e0, e1, e2, e3)
    me = lax.axis_index("cp")
    dp = lax.axis_index("dp")
    chip = me // 2
    q = lax.rem(me, 2)
    partner = (dp, 2 * chip + 1 - q)

    def peer(k):
        return lax.rem(chip + k, N_CHIP)

    def dev_of(cc):
        return (dp, 2 * cc + q)

    barrier = pltpu.get_barrier_semaphore()
    pl.semaphore_signal(barrier, inc=1, device_id=partner, device_id_type=MESH)
    for k in range(1, N_CHIP):
        pl.semaphore_signal(barrier, inc=1, device_id=dev_of(peer(k)), device_id_type=MESH)

    def blk(i):
        return pl.ds(pl.multiple_of(i * SEG, SEG), SEG)

    own = (blk(q), blk(3 - q))
    other = (blk(1 - q), blk(2 + q))

    def io_copies(n):
        src, dst = ((dy_hbm, dy_v), (x_hbm, x_v))[n]
        return [pltpu.make_async_copy(src.at[pl.ds(h * SEG, SEG)], dst.at[own[h]], io_sem.at[n, h]) for h in range(2)]

    def swap_copies(n):
        ref = (dy_v, x_v)[n]
        return [pltpu.make_async_remote_copy(
            src_ref=ref.at[own[h]], dst_ref=ref.at[own[h]], send_sem=xs_sem.at[n, h], recv_sem=xr_sem.at[n, h],
            device_id=partner, device_id_type=MESH) for h in range(2)]

    def wo_copy(g, k):
        return pltpu.make_async_copy(wo_hbm.at[q, peer(k), g], wo_s.at[g % 2, k - 1], wo_sem.at[g % 2, k - 1])

    def wkv_copy(w_hbm, i, slot, half=None):
        half = q if half is None else half
        return pltpu.make_async_copy(w_hbm.at[i, :, :, half], w_s.at[slot], w_sem.at[slot])

    def wq_copy(i, slot):
        return pltpu.make_async_copy(wq_hbm.at[i, :, pl.ds(3 * q, 3)], w_s.at[slot], w_sem.at[slot])

    def wait_slot(slot):
        wkv_copy(wk_hbm, 0, slot).wait()

    for cp in io_copies(0):
        cp.start()
    for k in (1, 2):
        wo_copy(0, k).start()
    dk_acc[...] = jnp.zeros_like(dk_acc)
    dv_acc[...] = jnp.zeros_like(dv_acc)
    with scope('barrier'):
        pl.semaphore_wait(barrier, N_CHIP)
    for cp in io_copies(1):
        cp.start()
    for i in range(4):
        wkv_copy(wk_hbm, i, i).start()
    with scope('swapdy'):
        for cp, sw in zip(io_copies(0), swap_copies(0)):
            cp.wait()
            sw.start()

    def relay_kv(dst, base, i, slot):
        flat = w_s.at[slot].reshape(768 * 4, HD)
        for h in range(4):
            for r in range(0, 768, RB):
                dst[base + h, pl.ds(i * 768 + r, RB), :] = flat[pl.ds(4 * r + h, RB, stride=4), :]

    def relay_q(i, slot):
        flat = w_s.at[slot].reshape(768 * 4, HD)
        for h in range(12):
            for r in range(0, 256, RB):
                wq_r[h, pl.ds(i * 256 + r, RB), :] = flat[pl.ds(12 * r + h, RB, stride=12), :]


    def row_of(b):
        return pl.ds(pl.multiple_of(jnp.where(b < 2, chip * TOK, SEQ - 2 * TOK - chip * TOK) + b * SEG, SEG), SEG)

    def send_rows(unit, k, val, blocks):
        for n, b in enumerate(blocks):
            part = val[n * SEG:(n + 1) * SEG]
            if k == N_CHIP:
                recv[unit, row_of(b), :] = part
            else:
                src = sbuf.at[unit, k - 1, blk(b)]
                src[...] = part
                pltpu.make_async_remote_copy(
                    src_ref=src, dst_ref=recv.at[unit, row_of(b)], send_sem=send_sem, recv_sem=recv_sem.at[unit],
                    device_id=dev_of(peer(k)), device_id_type=MESH).start()

    def send_block(unit, k, val):
        if k == N_CHIP:
            recv[unit, pl.ds(pl.multiple_of(chip * TOK, TOK), TOK), :] = val[:TOK]
            recv[unit, pl.ds(pl.multiple_of(SEQ - TOK - chip * TOK, TOK), TOK), :] = val[TOK:]
            return
        sbuf[unit, k - 1] = val
        for half, row in ((0, chip * TOK), (1, SEQ - TOK - chip * TOK)):
            pltpu.make_async_remote_copy(
                src_ref=sbuf.at[unit, k - 1, pl.ds(half * TOK, TOK)],
                dst_ref=recv.at[unit, pl.ds(pl.multiple_of(row, TOK), TOK)],
                send_sem=send_sem, recv_sem=recv_sem.at[unit],
                device_id=dev_of(peer(k)), device_id_type=MESH).start()

    def do0_rows(blocks, ids, ks):
        lhs = jnp.concatenate([dy_v[b, :] for b in blocks], axis=0)
        w = wo_s[0, pl.ds(ks[0] - 1, len(ks))].reshape(len(ks) * HD, D)
        val = dot_nt(lhs, w).astype(BF16)
        for n, k in enumerate(ks):
            send_rows(U_DO, k, val[:, n * HD:(n + 1) * HD], ids)

    def do_steps(g):
        for k in range(1, 5):
            wo_copy(g, k).wait()
        val = dot_nt(dy_v[...], wo_s[g % 2].reshape(4 * HD, D)).astype(BF16)
        for k in range(1, 5):
            send_block(U_DO + g, k, val[:, (k - 1) * HD:k * HD])

    def k_rows(blocks, ids):
        lhs = jnp.concatenate([x_v[b, :] for b in blocks], axis=0)
        w = jnp.concatenate([wk_r[4 * q + peer(k)] for k in range(1, 5)], axis=1)
        val = dot(lhs, w).astype(BF16)
        for k in range(1, 5):
            send_rows(U_K, k, val[:, (k - 1) * HD:k * HD], ids)

    def v_steps():
        w = jnp.concatenate([wv_r[4 * q + peer(k)] for k in range(1, 5)], axis=1)
        val = dot(x_v[...], w).astype(BF16)
        for k in range(1, 5):
            send_block(U_V, k, val[:, (k - 1) * HD:k * HD])

    def q_steps(g):
        w = jnp.concatenate([wq_r[3 * peer(k) + g] for k in range(1, 5)], axis=1)
        val = dot(x_v[...], w).astype(BF16)
        for k in range(1, 5):
            send_block(U_Q + g, k, val[:, (k - 1) * HD:k * HD])

    own_ids, other_ids = (q, 3 - q), (1 - q, 2 + q)
    with scope('do0a'):
        for k in (1, 2):
            wo_copy(0, k).wait()
        do0_rows(own, own_ids, (1, 2))
    for i in range(4):
        wkv_copy(wv_hbm, i, 4 + i).start()
    with scope('swapx'):
        for cp, sw in zip(io_copies(1), swap_copies(1)):
            cp.wait()
            sw.start()
    with scope('relk'):
        for i in range(4):
            wait_slot(i)
            relay_kv(wk_r, 4 * q, i, i)
    for k in (3, 4):
        wo_copy(0, k).start()
    for i in range(4):
        wq_copy(i, 8 + i).start()
    with scope('k_own'):
        k_rows(own, own_ids)
    with scope('xswap'):
        for cp in swap_copies(1):
            cp.wait_recv()
    with scope('k_other'):
        k_rows(other, other_ids)
    for i in range(4):
        wq_copy(4 + i, i).start()
    with scope('relv'):
        for i in range(4):
            wait_slot(4 + i)
            relay_kv(wv_r, 4 * q, i, 4 + i)
            wq_copy(8 + i, 4 + i).start()
    for k in range(1, 5):
        wo_copy(1, k).start()
    with scope('v'):
        v_steps()
    with scope('do0b'):
        for k in (3, 4):
            wo_copy(0, k).wait()
        do0_rows(own, own_ids, (3, 4))
    with scope('dyswap'):
        for cp in swap_copies(0):
            cp.wait_recv()
    with scope('do0c'):
        do0_rows(other, other_ids, (1, 2, 3, 4))
    for k in range(1, 5):
        wo_copy(2, k).start()
    with scope('relq'):
        for i in range(12):
            slot = (8 + i) % SLOTS
            wait_slot(slot)
            relay_q(i, slot)
            if i < 8:
                wkv_copy((wk_hbm, wv_hbm)[i // 4], i % 4, slot, 1 - q).start()
    with scope('q0'):
        q_steps(0)
    for g in (1, 2):
        with scope('do12'):
            do_steps(g)
        with scope('q12'):
            q_steps(g)
    with scope('relkv2'):
        for i in range(4):
            wait_slot(8 + i)
            relay_kv(wk_r, 4 - 4 * q, i, 8 + i)
            wait_slot(i)
            relay_kv(wv_r, 4 - 4 * q, i, i)

    def wait_unit(u):
        part = recv.at[u, pl.ds(0, SEQ - ROWS)]
        pltpu.make_async_copy(part, part, recv_sem.at[u]).wait()

    with scope('waitkv'):
        wait_unit(U_K)
        wait_unit(U_V)
    kt[...] = recv[U_K].T
    vt[...] = recv[U_V].T

    def send_out(u):
        slot = G * chip + u
        for k in range(1, N_CHIP):
            cc = peer(k)
            for half, row in ((0, cc * TOK), (1, SEQ - TOK - cc * TOK)):
                pltpu.make_async_remote_copy(
                    src_ref=obuf.at[u, pl.ds(pl.multiple_of(row, TOK), TOK)],
                    dst_ref=rin.at[slot, pl.ds(half * TOK, TOK)],
                    send_sem=osend_sem, recv_sem=orecv_sem.at[u],
                    device_id=dev_of(cc), device_id_type=MESH).start()
        rin[slot, :TOK, :] = obuf[u, pl.ds(pl.multiple_of(chip * TOK, TOK), TOK), :]
        rin[slot, TOK:, :] = obuf[u, pl.ds(pl.multiple_of(SEQ - TOK - chip * TOK, TOK), TOK), :]

    def attn_head(g, _):
        with scope('waitq'):
            wait_unit(U_DO + g)
            wait_unit(U_Q + g)
        st = [{} for _ in range(NB)]

        def rows_of(b):
            return slice(b * BQ, (b + 1) * BQ)

        def chunks(b):
            return [slice(k * BQ, (k + 1) * BQ) for k in range(b + 1)]

        def scores(b):
            qb = recv[U_Q + g, rows_of(b), :]
            dob = recv[U_DO + g, rows_of(b), :]
            mx = None
            for kc, ks in enumerate(chunks(b)):
                s = dot_nt(recv[U_K, ks, :], qb)
                if kc == b:
                    key = lax.broadcasted_iota(jnp.int32, (BQ, BQ), 0)
                    qry = lax.broadcasted_iota(jnp.int32, (BQ, BQ), 1)
                    s = jnp.where(key <= qry, s, -jnp.inf)
                s_scr[b][ks, :] = s
                mc = jnp.max(s.reshape(BQ // 8, 8, BQ), axis=0)
                mx = mc if mx is None else jnp.maximum(mx, mc)
            for ks in chunks(b):
                dp_scr[b][ks, :] = dot_nt(recv[U_V, ks, :], dob)
            st[b]['m2'] = jnp.max(mx, axis=0, keepdims=True) * C2

        def probs(b):
            m2 = st[b]['m2']
            ls = None
            for ks in chunks(b):
                e = jnp.exp2(s_scr[b][ks, :] * C2 - m2)
                lc = jnp.sum(e.reshape(BQ // 8, 8, BQ), axis=0)
                ls = lc if ls is None else ls + lc
            lse2 = m2 + jnp.log2(jnp.sum(ls, axis=0, keepdims=True))
            for ks in chunks(b):
                p_scr[b][ks, :] = jnp.exp2(s_scr[b][ks, :] * C2 - lse2).astype(BF16)

        def outs(b):
            n = (b + 1) * BQ
            dob = recv[U_DO + g, rows_of(b), :]
            ot = dot(vt[:, :n], p_scr[b][...]).astype(BF16)
            st[b]['delta'] = jnp.sum(dob.T.astype(F32) * ot.astype(F32), axis=0, keepdims=True)
            for ks in chunks(b):
                dv_acc[ks, :] += dot(p_scr[b][ks, :], dob)

        def dscores(b):
            delta = st[b]['delta']
            for ks in chunks(b):
                ds_scr[b][ks, :] = (p_scr[b][ks, :].astype(F32) * (dp_scr[b][ks, :] - delta)).astype(BF16)

        def grads(b):
            n = (b + 1) * BQ
            qb = recv[U_Q + g, rows_of(b), :]
            for ks in chunks(b):
                dk_acc[ks, :] += dot(ds_scr[b][ks, :], qb)
            dqt = (dot(kt[:, :n], ds_scr[b][...]) * C).astype(BF16)
            obuf[g, rows_of(b), :] = dqt.T

        with scope('attn'):
            scores(3)
            scores(2)
            probs(3)
            outs(3)
            scores(1)
            dscores(3)
            probs(2)
            grads(3)
            outs(2)
            scores(0)
            dscores(2)
            probs(1)
            grads(2)
            outs(1)
            dscores(1)
            probs(0)
            grads(1)
            outs(0)
            dscores(0)
            grads(0)

        with scope('send'):
            send_out(g)
        return 0

    lax.fori_loop(0, G, attn_head, 0)
    def seg_rows(dev, half):
        seg = dev if half == 0 else 2 * N_DEV - 1 - dev
        return pl.ds(pl.multiple_of(seg * SEG, SEG), SEG)

    def send_owners(n):
        slot = 8 * n + 4 * q + chip

        def send_dev(dev, part):
            for half in range(2):
                pltpu.make_async_remote_copy(
                    src_ref=obuf.at[G + n, seg_rows(dev, half)], dst_ref=rkv.at[slot, pl.ds(half * SEG, SEG)],
                    send_sem=osend_sem, recv_sem=kv_sem.at[n, part],
                    device_id=(dp, dev), device_id_type=MESH).start()

        send_dev(partner[1], 0)
        for k in range(1, N_CHIP):
            for r in range(2):
                send_dev(2 * peer(k) + r, k // 2)
        for half in range(2):
            rkv[slot, half * SEG:(half + 1) * SEG, :] = obuf[G + n, seg_rows(me, half), :]

    with scope('senddkv'):
        obuf[3] = (dk_acc[...] * C).astype(BF16)
        send_owners(0)
        obuf[4] = dv_acc[...].astype(BF16)
        send_owners(1)

    def p_copies():
        return [pltpu.make_async_remote_copy(
            src_ref=acc.at[other[h]], dst_ref=pbuf.at[pl.ds(h * SEG, SEG)],
            send_sem=ps_sem.at[h], recv_sem=pr_sem.at[h],
            device_id=partner, device_id_type=MESH) for h in range(2)]

    for u in range(G):
        with scope('waito'):
            part = obuf.at[u, pl.ds(0, SEQ - ROWS)]
            pltpu.make_async_copy(part, part, orecv_sem.at[u]).wait()

        def dx_step(i, _, u=u):
            cols = pl.ds(pl.multiple_of(i * ND, ND), ND)
            t = dot_nt(jnp.concatenate([rin[G * j + u] for j in range(N_CHIP)], axis=1),
                       jnp.concatenate([wq_r[G * j + u, cols, :] for j in range(N_CHIP)], axis=1))
            if u > 0:
                t = t + acc[:, cols]
            acc[:, cols] = t
            return 0

        with scope('dx'):
            lax.fori_loop(0, D // ND, dx_step, 0)
    for cp in p_copies():
        cp.start()

    for n, parts in ((0, (0,)), (0, (1,)), (1, (0,)), (1, (1,))):
            last = n == 1 and 1 in parts
            with scope('waitkv%d%d' % (n, parts[0])):
                for part in parts:
                    ref = obuf.at[0, pl.ds(0, (3, 4)[part] * TOK)]
                    pltpu.make_async_copy(ref, ref, kv_sem.at[n, part]).wait()
            if last:
                with scope('waitp'):
                    for cp in p_copies():
                        cp.wait_recv()
            chips = [lax.rem(chip + N_CHIP - k, N_CHIP) for part in parts for k in ((0, 1), (2, 3))[part]]
            heads = [c + 4 * r for c in chips for r in range(2)]

            def kv_dx(i, _, n=n, last=last, heads=heads):
                cols = pl.ds(pl.multiple_of(i * NV, NV), NV)
                t = dot_nt(jnp.concatenate([rkv[8 * n + h] for h in heads], axis=1),
                           jnp.concatenate([(wk_r, wv_r)[n][h, cols, :] for h in heads], axis=1))
                for h in range(2):
                    rows = slice(h * SEG, (h + 1) * SEG)
                    part_t = t[rows] + acc[own[h], cols]
                    if last:
                        out_ref[rows, cols] = (part_t + pbuf[rows, cols]).astype(BF16)
                    else:
                        acc[own[h], cols] = part_t
                return 0

            with scope('kvdx'):
                lax.fori_loop(0, D // NV, kv_dx, 0)

    with scope('final'):
        for n in range(2):
            for cp in swap_copies(n):
                cp.wait_send()
        for cp in p_copies():
            cp.wait_send()
        pltpu.make_async_copy(sbuf, sbuf, send_sem).wait()
        part = obuf.at[pl.ds(0, G), pl.ds(0, SEQ - ROWS)]
        pltpu.make_async_copy(part, part, osend_sem).wait()
        part = obuf.at[pl.ds(0, 2), pl.ds(0, SEQ - TOK)]
        pltpu.make_async_copy(part, part, osend_sem).wait()


def write_out(src, dst, sem):
    cp = pltpu.make_async_copy(src, dst, sem)
    cp.start()
    cp.wait()


def solution(mesh):
    row_spec = P(("dp", "cp"), None)

    def device_fn(x_in, d_y, w_q, w_k, w_v, w_o):
        dma = pltpu.SemaphoreType.DMA
        res = pl.pallas_call(
            kernel,
            out_shape=pltpu.VMEM((TOK, D), BF16),
            in_specs=[pl.BlockSpec(memory_space=pl.ANY)] * 6,
            out_specs=pl.BlockSpec(memory_space=pltpu.VMEM),
            scratch_shapes=[
                pltpu.VMEM((ROWS, D), BF16),
                pltpu.VMEM((ROWS, D), BF16),
                pltpu.VMEM((2, N_CHIP, HD, D), BF16),
                pltpu.VMEM((SLOTS, 256, 3, 4, HD), BF16),
                pltpu.VMEM((12, D, HD), BF16),
                pltpu.VMEM((8, D, HD), BF16),
                pltpu.VMEM((8, D, HD), BF16),
                pltpu.VMEM((8, 3, ROWS, HD), BF16),
                pltpu.VMEM((8, SEQ, HD), BF16),
                pltpu.VMEM((5, SEQ, HD), BF16),
                pltpu.VMEM((12, ROWS, HD), BF16),
                pltpu.VMEM((16, TOK, HD), BF16),
                pltpu.VMEM((ROWS, D), F32),
                pltpu.VMEM((TOK, D), F32),
                *[pltpu.VMEM(((b + 1) * BQ, BQ), t) for t in (F32, F32, BF16, BF16) for b in range(NB)],
                pltpu.VMEM((HD, SEQ), BF16),
                pltpu.VMEM((HD, SEQ), BF16),
                pltpu.VMEM((SEQ, HD), F32),
                pltpu.VMEM((SEQ, HD), F32),
                dma((2, 2)), dma((2, N_CHIP)), dma((SLOTS,)), dma((2, 2)), dma((2, 2)),
                dma, dma((8,)), dma, dma((G,)), dma((2, 2)), dma((2,)), dma((2,)),
            ],
            compiler_params=pltpu.CompilerParams(
                collective_id=0, has_side_effects=True, vmem_limit_bytes=VLIM),
        )(x_in, d_y, w_q.reshape(12, 256, 6, 4, HD), w_k.reshape(4, 256, 3, 2, 4, HD), w_v.reshape(4, 256, 3, 2, 4, HD),
          w_o.reshape(2, N_CHIP, G, HD, D))
        return pl.pallas_call(
            write_out,
            out_shape=jax.ShapeDtypeStruct((TOK, D), BF16),
            in_specs=[pl.BlockSpec(memory_space=pltpu.VMEM)],
            out_specs=pl.BlockSpec(memory_space=pl.ANY),
            scratch_shapes=[pltpu.SemaphoreType.DMA],
        )(pltpu.with_memory_space_constraint(res, pltpu.VMEM))

    return jax.shard_map(device_fn, mesh=mesh, in_specs=(row_spec, row_spec, P(), P(), P(), P()),
                         out_specs=row_spec, check_vma=False)
```

```python
import math

import jax
import jax.numpy as jnp
from jax import lax
from jax.experimental import pallas as pl
from jax.experimental.pallas import tpu as pltpu
from jax.sharding import PartitionSpec as P

MESH = pl.DeviceIdType.MESH
BF16, F32 = jnp.bfloat16, jnp.float32
NT = (((1,), (1,)), ((), ()))

N_DEV, N_CHIP, TOK, SEG = 8, 4, 128, 64
ROWS = 2 * TOK
SEQ = N_DEV * TOK
D = 3072
HD = 128
G = 3
BQ = 256
NB = SEQ // BQ
C = HD**-0.5
C2 = C * math.log2(math.e)
U_DO, U_K, U_V, U_Q = 0, 3, 4, 5
SLOTS = 12
RB = 128
ND = 3072
NV = 3072
VLIM = 66_000_000

scope = jax.named_scope


def dot_nt(a, b):
    return lax.dot_general(a, b, NT, preferred_element_type=F32)


def dot(a, b):
    return jnp.dot(a, b, preferred_element_type=F32)


def kernel(x_hbm, dy_hbm, wq_hbm, wk_hbm, wv_hbm, wo_hbm, out_ref,
           x_v, dy_v, wo_s, w_s, wq_r, wk_r, wv_r, sbuf, recv, obuf, rin, rkv, acc, pbuf,
           s0, s1, s2, s3, d0, d1, d2, d3, p0, p1, p2, p3, e0, e1, e2, e3, kt, vt, dk_acc, dv_acc,
           io_sem, wo_sem, w_sem, xs_sem, xr_sem, send_sem, recv_sem, osend_sem, orecv_sem, kv_sem, ps_sem, pr_sem):
    s_scr, dp_scr, p_scr, ds_scr = (s0, s1, s2, s3), (d0, d1, d2, d3), (p0, p1, p2, p3), (e0, e1, e2, e3)
    me = lax.axis_index("cp")
    dp = lax.axis_index("dp")
    chip = me // 2
    q = lax.rem(me, 2)
    partner = (dp, 2 * chip + 1 - q)

    def peer(k):
        return lax.rem(chip + k, N_CHIP)

    def dev_of(cc):
        return (dp, 2 * cc + q)

    barrier = pltpu.get_barrier_semaphore()
    pl.semaphore_signal(barrier, inc=1, device_id=partner, device_id_type=MESH)
    for k in range(1, N_CHIP):
        pl.semaphore_signal(barrier, inc=1, device_id=dev_of(peer(k)), device_id_type=MESH)

    def tok_rows(i):
        return pl.ds(pl.multiple_of(i * TOK, TOK), TOK)

    def chip_rows(i):
        return pl.ds(pl.multiple_of(i * ROWS, ROWS), ROWS)

    own, other = tok_rows(q), tok_rows(1 - q)

    def io_copy(n):
        src, dst = ((dy_hbm, dy_v), (x_hbm, x_v))[n]
        return pltpu.make_async_copy(src, dst.at[own], io_sem.at[n])

    def swap_copy(n):
        ref = (dy_v, x_v)[n]
        return pltpu.make_async_remote_copy(
            src_ref=ref.at[own], dst_ref=ref.at[own], send_sem=xs_sem.at[n], recv_sem=xr_sem.at[n],
            device_id=partner, device_id_type=MESH)

    def wo_copy(g, k):
        return pltpu.make_async_copy(wo_hbm.at[q, peer(k), g], wo_s.at[g % 2, k - 1], wo_sem.at[g % 2, k - 1])

    def wkv_copy(w_hbm, i, slot, half=None):
        half = q if half is None else half
        return pltpu.make_async_copy(w_hbm.at[i, :, :, half], w_s.at[slot], w_sem.at[slot])

    def wq_copy(i, slot):
        return pltpu.make_async_copy(wq_hbm.at[i, :, pl.ds(3 * q, 3)], w_s.at[slot], w_sem.at[slot])

    def wait_slot(slot):
        wkv_copy(wk_hbm, 0, slot).wait()

    io_copy(0).start()
    for k in (1, 2):
        wo_copy(0, k).start()
    dk_acc[...] = jnp.zeros_like(dk_acc)
    dv_acc[...] = jnp.zeros_like(dv_acc)
    with scope('barrier'):
        pl.semaphore_wait(barrier, N_CHIP)
    io_copy(1).start()
    for i in range(4):
        wkv_copy(wk_hbm, i, i).start()
    with scope('swapdy'):
        io_copy(0).wait()
        swap_copy(0).start()

    def relay_kv(dst, base, i, slot):
        flat = w_s.at[slot].reshape(768 * 4, HD)
        for h in range(4):
            for r in range(0, 768, RB):
                dst[base + h, pl.ds(i * 768 + r, RB), :] = flat[pl.ds(4 * r + h, RB, stride=4), :]

    def relay_q(i, slot):
        flat = w_s.at[slot].reshape(768 * 4, HD)
        for h in range(12):
            for r in range(0, 256, RB):
                wq_r[h, pl.ds(i * 256 + r, RB), :] = flat[pl.ds(12 * r + h, RB, stride=12), :]


    def send_part(unit, k, val, rows, dst_rows):
        if k == N_CHIP:
            recv[unit, dst_rows, :] = val
            return
        sbuf[unit, k - 1, rows, :] = val
        pltpu.make_async_remote_copy(
            src_ref=sbuf.at[unit, k - 1, rows], dst_ref=recv.at[unit, dst_rows],
            send_sem=send_sem, recv_sem=recv_sem.at[unit],
            device_id=dev_of(peer(k)), device_id_type=MESH).start()

    def send_rows(unit, k, val, r):
        send_part(unit, k, val, tok_rows(r), tok_rows(2 * chip + r))

    def send_block(unit, k, val):
        send_part(unit, k, val, pl.ds(0, ROWS), chip_rows(chip))

    def do0_rows(r, ks):
        w = wo_s[0, pl.ds(ks[0] - 1, len(ks))].reshape(len(ks) * HD, D)
        val = dot_nt(dy_v[tok_rows(r), :], w).astype(BF16)
        for n, k in enumerate(ks):
            send_rows(U_DO, k, val[:, n * HD:(n + 1) * HD], r)

    def do_steps(g):
        for k in range(1, 5):
            wo_copy(g, k).wait()
        val = dot_nt(dy_v[...], wo_s[g % 2].reshape(4 * HD, D)).astype(BF16)
        for k in range(1, 5):
            send_block(U_DO + g, k, val[:, (k - 1) * HD:k * HD])

    def k_rows(r):
        w = jnp.concatenate([wk_r[4 * q + peer(k)] for k in range(1, 5)], axis=1)
        val = dot(x_v[tok_rows(r), :], w).astype(BF16)
        for k in range(1, 5):
            send_rows(U_K, k, val[:, (k - 1) * HD:k * HD], r)

    def v_steps():
        w = jnp.concatenate([wv_r[4 * q + peer(k)] for k in range(1, 5)], axis=1)
        val = dot(x_v[...], w).astype(BF16)
        for k in range(1, 5):
            send_block(U_V, k, val[:, (k - 1) * HD:k * HD])

    def q_steps(g):
        w = jnp.concatenate([wq_r[3 * peer(k) + g] for k in range(1, 5)], axis=1)
        val = dot(x_v[...], w).astype(BF16)
        for k in range(1, 5):
            send_block(U_Q + g, k, val[:, (k - 1) * HD:k * HD])

    with scope('do0a'):
        for k in (1, 2):
            wo_copy(0, k).wait()
        do0_rows(q, (1, 2))
    for i in range(4):
        wkv_copy(wv_hbm, i, 4 + i).start()
    with scope('swapx'):
        io_copy(1).wait()
        swap_copy(1).start()
    with scope('relk'):
        for i in range(4):
            wait_slot(i)
            relay_kv(wk_r, 4 * q, i, i)
    for k in (3, 4):
        wo_copy(0, k).start()
    for i in range(4):
        wq_copy(i, 8 + i).start()
    with scope('k_own'):
        k_rows(q)
    with scope('xswap'):
        swap_copy(1).wait_recv()
    with scope('k_other'):
        k_rows(1 - q)
    for i in range(4):
        wq_copy(4 + i, i).start()
    with scope('relv'):
        for i in range(4):
            wait_slot(4 + i)
            relay_kv(wv_r, 4 * q, i, 4 + i)
            wq_copy(8 + i, 4 + i).start()
    for k in range(1, 5):
        wo_copy(1, k).start()
    with scope('v'):
        v_steps()
    with scope('do0b'):
        for k in (3, 4):
            wo_copy(0, k).wait()
        do0_rows(q, (3, 4))
    with scope('dyswap'):
        swap_copy(0).wait_recv()
    with scope('do0c'):
        do0_rows(1 - q, (1, 2, 3, 4))
    for k in range(1, 5):
        wo_copy(2, k).start()
    with scope('relq'):
        for i in range(12):
            slot = (8 + i) % SLOTS
            wait_slot(slot)
            relay_q(i, slot)
            if i < 8:
                wkv_copy((wk_hbm, wv_hbm)[i // 4], i % 4, slot, 1 - q).start()
    with scope('q0'):
        q_steps(0)
    for g in (1, 2):
        with scope('do12'):
            do_steps(g)
        with scope('q12'):
            q_steps(g)
    with scope('relkv2'):
        for i in range(4):
            wait_slot(8 + i)
            relay_kv(wk_r, 4 - 4 * q, i, 8 + i)
            wait_slot(i)
            relay_kv(wv_r, 4 - 4 * q, i, i)

    def wait_unit(u):
        part = recv.at[u, pl.ds(0, SEQ - ROWS)]
        pltpu.make_async_copy(part, part, recv_sem.at[u]).wait()

    with scope('waitkv'):
        wait_unit(U_K)
        wait_unit(U_V)
    def segs(b):
        out = []
        for seg in range(4 * b, 4 * b + 4):
            row = seg * TOK if seg < N_DEV else (2 * N_DEV - 1 - seg) * TOK + SEG
            out.append(slice(row, row + SEG))
        return out

    def pos_block(u, b):
        return jnp.concatenate([recv[u, r, :] for r in segs(b)], axis=0)

    def put_block(u, b, val):
        for n, r in enumerate(segs(b)):
            obuf[u, r, :] = val[n * SEG:(n + 1) * SEG]

    for b in range(NB):
        kt[:, b * BQ:(b + 1) * BQ] = pos_block(U_K, b).T
        vt[:, b * BQ:(b + 1) * BQ] = pos_block(U_V, b).T

    def send_out(u):
        slot = G * chip + u
        for k in range(1, N_CHIP):
            pltpu.make_async_remote_copy(
                src_ref=obuf.at[u, chip_rows(peer(k))], dst_ref=rin.at[slot],
                send_sem=osend_sem, recv_sem=orecv_sem.at[u],
                device_id=dev_of(peer(k)), device_id_type=MESH).start()
        rin[slot] = obuf[u, chip_rows(chip), :]

    def attn_head(g, _):
        with scope('waitq'):
            wait_unit(U_DO + g)
            wait_unit(U_Q + g)
        st = [{} for _ in range(NB)]

        def chunks(b):
            return [slice(k * BQ, (k + 1) * BQ) for k in range(b + 1)]

        def scores(b):
            qb = pos_block(U_Q + g, b)
            dob = pos_block(U_DO + g, b)
            mx = None
            for kc, ks in enumerate(chunks(b)):
                s = dot_nt(pos_block(U_K, kc), qb)
                if kc == b:
                    key = lax.broadcasted_iota(jnp.int32, (BQ, BQ), 0)
                    qry = lax.broadcasted_iota(jnp.int32, (BQ, BQ), 1)
                    s = jnp.where(key <= qry, s, -jnp.inf)
                s_scr[b][ks, :] = s
                mc = jnp.max(s.reshape(BQ // 8, 8, BQ), axis=0)
                mx = mc if mx is None else jnp.maximum(mx, mc)
            for kc, ks in enumerate(chunks(b)):
                dp_scr[b][ks, :] = dot_nt(pos_block(U_V, kc), dob)
            st[b]['m2'] = jnp.max(mx, axis=0, keepdims=True) * C2

        def probs(b):
            m2 = st[b]['m2']
            ls = None
            for ks in chunks(b):
                e = jnp.exp2(s_scr[b][ks, :] * C2 - m2)
                lc = jnp.sum(e.reshape(BQ // 8, 8, BQ), axis=0)
                ls = lc if ls is None else ls + lc
            lse2 = m2 + jnp.log2(jnp.sum(ls, axis=0, keepdims=True))
            for ks in chunks(b):
                p_scr[b][ks, :] = jnp.exp2(s_scr[b][ks, :] * C2 - lse2).astype(BF16)

        def outs(b):
            n = (b + 1) * BQ
            dob = pos_block(U_DO + g, b)
            ot = dot(vt[:, :n], p_scr[b][...]).astype(BF16)
            st[b]['delta'] = jnp.sum(dob.T.astype(F32) * ot.astype(F32), axis=0, keepdims=True)
            for ks in chunks(b):
                dv_acc[ks, :] += dot(p_scr[b][ks, :], dob)

        def dscores(b):
            delta = st[b]['delta']
            for ks in chunks(b):
                ds_scr[b][ks, :] = (p_scr[b][ks, :].astype(F32) * (dp_scr[b][ks, :] - delta)).astype(BF16)

        def grads(b):
            n = (b + 1) * BQ
            qb = pos_block(U_Q + g, b)
            for ks in chunks(b):
                dk_acc[ks, :] += dot(ds_scr[b][ks, :], qb)
            dqt = (dot(kt[:, :n], ds_scr[b][...]) * C).astype(BF16)
            put_block(g, b, dqt.T)

        with scope('attn'):
            scores(3)
            scores(2)
            probs(3)
            outs(3)
            scores(1)
            dscores(3)
            probs(2)
            grads(3)
            outs(2)
            scores(0)
            dscores(2)
            probs(1)
            grads(2)
            outs(1)
            dscores(1)
            probs(0)
            grads(1)
            outs(0)
            dscores(0)
            grads(0)

        with scope('send'):
            send_out(g)
        return 0

    lax.fori_loop(0, G, attn_head, 0)
    def send_owners(n):
        slot = 8 * n + 4 * q + chip

        def send_dev(dev, part):
            pltpu.make_async_remote_copy(
                src_ref=obuf.at[G + n, tok_rows(dev)], dst_ref=rkv.at[slot],
                send_sem=osend_sem, recv_sem=kv_sem.at[n, part],
                device_id=(dp, dev), device_id_type=MESH).start()

        send_dev(partner[1], 0)
        for k in range(1, N_CHIP):
            for r in range(2):
                send_dev(2 * peer(k) + r, k // 2)
        rkv[slot] = obuf[G + n, tok_rows(me), :]

    with scope('senddkv'):
        for b in range(NB):
            put_block(3, b, (dk_acc[b * BQ:(b + 1) * BQ, :] * C).astype(BF16))
        send_owners(0)
        for b in range(NB):
            put_block(4, b, dv_acc[b * BQ:(b + 1) * BQ, :].astype(BF16))
        send_owners(1)

    def p_copy():
        return pltpu.make_async_remote_copy(
            src_ref=acc.at[other], dst_ref=pbuf, send_sem=ps_sem, recv_sem=pr_sem,
            device_id=partner, device_id_type=MESH)

    for u in range(G):
        with scope('waito'):
            part = obuf.at[u, pl.ds(0, SEQ - ROWS)]
            pltpu.make_async_copy(part, part, orecv_sem.at[u]).wait()

        def dx_step(i, _, u=u):
            cols = pl.ds(pl.multiple_of(i * ND, ND), ND)
            t = dot_nt(jnp.concatenate([rin[G * j + u] for j in range(N_CHIP)], axis=1),
                       jnp.concatenate([wq_r[G * j + u, cols, :] for j in range(N_CHIP)], axis=1))
            if u > 0:
                t = t + acc[:, cols]
            acc[:, cols] = t
            return 0

        with scope('dx'):
            lax.fori_loop(0, D // ND, dx_step, 0)
    p_copy().start()

    for n, parts in ((0, (0,)), (0, (1,)), (1, (0,)), (1, (1,))):
            last = n == 1 and 1 in parts
            with scope('waitkv%d%d' % (n, parts[0])):
                for part in parts:
                    ref = obuf.at[0, pl.ds(0, (3, 4)[part] * TOK)]
                    pltpu.make_async_copy(ref, ref, kv_sem.at[n, part]).wait()
            if last:
                with scope('waitp'):
                    p_copy().wait_recv()
            chips = [lax.rem(chip + N_CHIP - k, N_CHIP) for part in parts for k in ((0, 1), (2, 3))[part]]
            heads = [c + 4 * r for c in chips for r in range(2)]

            def kv_dx(i, _, n=n, last=last, heads=heads):
                cols = pl.ds(pl.multiple_of(i * NV, NV), NV)
                t = dot_nt(jnp.concatenate([rkv[8 * n + h] for h in heads], axis=1),
                           jnp.concatenate([(wk_r, wv_r)[n][h, cols, :] for h in heads], axis=1))
                t = t + acc[own, cols]
                if last:
                    out_ref[:, cols] = (t + pbuf[:, cols]).astype(BF16)
                else:
                    acc[own, cols] = t
                return 0

            with scope('kvdx'):
                lax.fori_loop(0, D // NV, kv_dx, 0)

    with scope('final'):
        for n in range(2):
            swap_copy(n).wait_send()
        p_copy().wait_send()
        pltpu.make_async_copy(sbuf, sbuf, send_sem).wait()
        part = obuf.at[pl.ds(0, G), pl.ds(0, SEQ - ROWS)]
        pltpu.make_async_copy(part, part, osend_sem).wait()
        part = obuf.at[pl.ds(0, 2), pl.ds(0, SEQ - TOK)]
        pltpu.make_async_copy(part, part, osend_sem).wait()


def write_out(src, dst, sem):
    cp = pltpu.make_async_copy(src, dst, sem)
    cp.start()
    cp.wait()


def solution(mesh):
    row_spec = P(("dp", "cp"), None)

    def device_fn(x_in, d_y, w_q, w_k, w_v, w_o):
        dma = pltpu.SemaphoreType.DMA
        res = pl.pallas_call(
            kernel,
            out_shape=pltpu.VMEM((TOK, D), BF16),
            in_specs=[pl.BlockSpec(memory_space=pl.ANY)] * 6,
            out_specs=pl.BlockSpec(memory_space=pltpu.VMEM),
            scratch_shapes=[
                pltpu.VMEM((ROWS, D), BF16),
                pltpu.VMEM((ROWS, D), BF16),
                pltpu.VMEM((2, N_CHIP, HD, D), BF16),
                pltpu.VMEM((SLOTS, 256, 3, 4, HD), BF16),
                pltpu.VMEM((12, D, HD), BF16),
                pltpu.VMEM((8, D, HD), BF16),
                pltpu.VMEM((8, D, HD), BF16),
                pltpu.VMEM((8, 3, ROWS, HD), BF16),
                pltpu.VMEM((8, SEQ, HD), BF16),
                pltpu.VMEM((5, SEQ, HD), BF16),
                pltpu.VMEM((12, ROWS, HD), BF16),
                pltpu.VMEM((16, TOK, HD), BF16),
                pltpu.VMEM((ROWS, D), F32),
                pltpu.VMEM((TOK, D), F32),
                *[pltpu.VMEM(((b + 1) * BQ, BQ), t) for t in (F32, F32, BF16, BF16) for b in range(NB)],
                pltpu.VMEM((HD, SEQ), BF16),
                pltpu.VMEM((HD, SEQ), BF16),
                pltpu.VMEM((SEQ, HD), F32),
                pltpu.VMEM((SEQ, HD), F32),
                dma((2,)), dma((2, N_CHIP)), dma((SLOTS,)), dma((2,)), dma((2,)),
                dma, dma((8,)), dma, dma((G,)), dma((2, 2)), dma, dma,
            ],
            compiler_params=pltpu.CompilerParams(
                collective_id=0, has_side_effects=True, vmem_limit_bytes=VLIM),
        )(x_in, d_y, w_q.reshape(12, 256, 6, 4, HD), w_k.reshape(4, 256, 3, 2, 4, HD), w_v.reshape(4, 256, 3, 2, 4, HD),
          w_o.reshape(2, N_CHIP, G, HD, D))
        return pl.pallas_call(
            write_out,
            out_shape=jax.ShapeDtypeStruct((TOK, D), BF16),
            in_specs=[pl.BlockSpec(memory_space=pltpu.VMEM)],
            out_specs=pl.BlockSpec(memory_space=pl.ANY),
            scratch_shapes=[pltpu.SemaphoreType.DMA],
        )(pltpu.with_memory_space_constraint(res, pltpu.VMEM))

    return jax.shard_map(device_fn, mesh=mesh, in_specs=(row_spec, row_spec, P(), P(), P(), P()),
                         out_specs=row_spec, check_vma=False)
```

```python
import math

import jax
import jax.numpy as jnp
from jax import lax
from jax.experimental import pallas as pl
from jax.experimental.pallas import tpu as pltpu
from jax.sharding import PartitionSpec as P

MESH = pl.DeviceIdType.MESH
BF16, F32 = jnp.bfloat16, jnp.float32
NT = (((1,), (1,)), ((), ()))

N_DEV, N_CHIP, TOK, SEG = 8, 4, 128, 64
ROWS = 2 * TOK
SEQ = N_DEV * TOK
D = 3072
HD = 128
G = 3
BQ = 256
NB = SEQ // BQ
C = HD**-0.5
C2 = C * math.log2(math.e)
U_DO, U_K, U_V, U_Q = 0, 3, 4, 5
SLOTS = 12
RB = 128
ND = 3072
NV = 3072
VLIM = 66_000_000

scope = jax.named_scope


def dot_nt(a, b):
    return lax.dot_general(a, b, NT, preferred_element_type=F32)


def dot(a, b):
    return jnp.dot(a, b, preferred_element_type=F32)


def kernel(x_hbm, dy_hbm, wq_hbm, wk_hbm, wv_hbm, wo_hbm, out_ref,
           x_v, dy_v, wo_s, w_s, wq_r, wk_r, wv_r, sbuf, recv, obuf, rin, rkv, acc, pbuf,
           s0, s1, s2, s3, d0, d1, d2, d3, p0, p1, p2, p3, e0, e1, e2, e3, kt, vt, dk_acc, dv_acc,
           io_sem, wo_sem, w_sem, xs_sem, xr_sem, send_sem, recv_sem, osend_sem, orecv_sem, kv_sem, ps_sem, pr_sem):
    s_scr, dp_scr, p_scr, ds_scr = (s0, s1, s2, s3), (d0, d1, d2, d3), (p0, p1, p2, p3), (e0, e1, e2, e3)
    me = lax.axis_index("cp")
    dp = lax.axis_index("dp")
    chip = me // 2
    q = lax.rem(me, 2)
    partner = (dp, 2 * chip + 1 - q)

    def peer(k):
        return lax.rem(chip + k, N_CHIP)

    def dev_of(cc):
        return (dp, 2 * cc + q)

    barrier = pltpu.get_barrier_semaphore()
    pl.semaphore_signal(barrier, inc=1, device_id=partner, device_id_type=MESH)
    for k in range(1, N_CHIP):
        pl.semaphore_signal(barrier, inc=1, device_id=dev_of(peer(k)), device_id_type=MESH)

    def tok_rows(i):
        return pl.ds(pl.multiple_of(i * TOK, TOK), TOK)

    def chip_rows(i):
        return pl.ds(pl.multiple_of(i * ROWS, ROWS), ROWS)

    own, other = tok_rows(q), tok_rows(1 - q)

    def io_copy(n):
        src, dst = ((dy_hbm, dy_v), (x_hbm, x_v))[n]
        return pltpu.make_async_copy(src, dst.at[own], io_sem.at[n])

    def swap_copy(n):
        ref = (dy_v, x_v)[n]
        return pltpu.make_async_remote_copy(
            src_ref=ref.at[own], dst_ref=ref.at[own], send_sem=xs_sem.at[n], recv_sem=xr_sem.at[n],
            device_id=partner, device_id_type=MESH)

    def wo_copy(g, k):
        return pltpu.make_async_copy(wo_hbm.at[q, peer(k), g], wo_s.at[g % 2, k - 1], wo_sem.at[g % 2, k - 1])

    def wkv_copy(w_hbm, i, slot, half=None):
        half = q if half is None else half
        return pltpu.make_async_copy(w_hbm.at[i, :, :, half], w_s.at[slot], w_sem.at[slot])

    def wq_copy(i, slot):
        return pltpu.make_async_copy(wq_hbm.at[i, :, pl.ds(3 * q, 3)], w_s.at[slot], w_sem.at[slot])

    def wait_slot(slot):
        wkv_copy(wk_hbm, 0, slot).wait()

    io_copy(0).start()
    for k in (1, 2):
        wo_copy(0, k).start()
    dk_acc[...] = jnp.zeros_like(dk_acc)
    dv_acc[...] = jnp.zeros_like(dv_acc)
    with scope('barrier'):
        pl.semaphore_wait(barrier, N_CHIP)
    io_copy(1).start()
    for i in range(4):
        wkv_copy(wk_hbm, i, i).start()
    with scope('swapdy'):
        io_copy(0).wait()
        swap_copy(0).start()

    def relay_kv(dst, base, i, slot):
        flat = w_s.at[slot].reshape(768 * 4, HD)
        for h in range(4):
            for r in range(0, 768, RB):
                dst[base + h, pl.ds(i * 768 + r, RB), :] = flat[pl.ds(4 * r + h, RB, stride=4), :]

    def relay_q(i, slot):
        flat = w_s.at[slot].reshape(768 * 4, HD)
        for h in range(12):
            for r in range(0, 256, RB):
                wq_r[h, pl.ds(i * 256 + r, RB), :] = flat[pl.ds(12 * r + h, RB, stride=12), :]


    def send_part(unit, k, val, rows, dst_rows):
        if k == N_CHIP:
            recv[unit, dst_rows, :] = val
            return
        sbuf[unit, k - 1, rows, :] = val
        pltpu.make_async_remote_copy(
            src_ref=sbuf.at[unit, k - 1, rows], dst_ref=recv.at[unit, dst_rows],
            send_sem=send_sem, recv_sem=recv_sem.at[unit],
            device_id=dev_of(peer(k)), device_id_type=MESH).start()

    def send_rows(unit, k, val, r):
        send_part(unit, k, val, tok_rows(r), tok_rows(2 * chip + r))

    def send_block(unit, k, val):
        send_part(unit, k, val, pl.ds(0, ROWS), chip_rows(chip))

    def do0_rows(r, ks):
        w = wo_s[0, pl.ds(ks[0] - 1, len(ks))].reshape(len(ks) * HD, D)
        val = dot_nt(dy_v[tok_rows(r), :], w).astype(BF16)
        for n, k in enumerate(ks):
            send_rows(U_DO, k, val[:, n * HD:(n + 1) * HD], r)

    def do_steps(g):
        for k in range(1, 5):
            wo_copy(g, k).wait()
        val = dot_nt(dy_v[...], wo_s[g % 2].reshape(4 * HD, D)).astype(BF16)
        for k in range(1, 5):
            send_block(U_DO + g, k, val[:, (k - 1) * HD:k * HD])

    def k_rows(r):
        w = jnp.concatenate([wk_r[4 * q + peer(k)] for k in range(1, 5)], axis=1)
        val = dot(x_v[tok_rows(r), :], w).astype(BF16)
        for k in range(1, 5):
            send_rows(U_K, k, val[:, (k - 1) * HD:k * HD], r)

    def v_steps():
        w = jnp.concatenate([wv_r[4 * q + peer(k)] for k in range(1, 5)], axis=1)
        val = dot(x_v[...], w).astype(BF16)
        for k in range(1, 5):
            send_block(U_V, k, val[:, (k - 1) * HD:k * HD])

    def q_steps(g):
        w = jnp.concatenate([wq_r[3 * peer(k) + g] for k in range(1, 5)], axis=1)
        val = dot(x_v[...], w).astype(BF16)
        for k in range(1, 5):
            send_block(U_Q + g, k, val[:, (k - 1) * HD:k * HD])

    with scope('do0a'):
        for k in (1, 2):
            wo_copy(0, k).wait()
        do0_rows(q, (1, 2))
    for i in range(4):
        wkv_copy(wv_hbm, i, 4 + i).start()
    with scope('swapx'):
        io_copy(1).wait()
        swap_copy(1).start()
    with scope('relk'):
        for i in range(4):
            wait_slot(i)
            relay_kv(wk_r, 4 * q, i, i)
    for k in (3, 4):
        wo_copy(0, k).start()
    with scope('k_own'):
        k_rows(q)
    with scope('xswap'):
        swap_copy(1).wait_recv()
    with scope('k_other'):
        k_rows(1 - q)
    with scope('relv'):
        for i in range(4):
            wait_slot(4 + i)
            relay_kv(wv_r, 4 * q, i, 4 + i)
    for i in range(4):
        wq_copy(i, 8 + i).start()
    with scope('v'):
        v_steps()
    for i in range(4):
        wq_copy(4 + i, i).start()
    with scope('do0b'):
        for k in (3, 4):
            wo_copy(0, k).wait()
        do0_rows(q, (3, 4))
    for i in range(4):
        wq_copy(8 + i, 4 + i).start()
    with scope('dyswap'):
        swap_copy(0).wait_recv()
    with scope('do0c'):
        do0_rows(1 - q, (1, 2, 3, 4))
    for k in range(1, 5):
        wo_copy(1, k).start()
    with scope('relq'):
        for i in range(12):
            slot = (8 + i) % SLOTS
            wait_slot(slot)
            relay_q(i, slot)
    for k in range(1, 5):
        wo_copy(2, k).start()
    with scope('q0'):
        q_steps(0)
    for i in range(8):
        wkv_copy((wk_hbm, wv_hbm)[i // 4], i % 4, (8 + i) % SLOTS, 1 - q).start()
    for g in (1, 2):
        with scope('do12'):
            do_steps(g)
        with scope('q12'):
            q_steps(g)
    with scope('relkv2'):
        for i in range(4):
            wait_slot(8 + i)
            relay_kv(wk_r, 4 - 4 * q, i, 8 + i)
            wait_slot(i)
            relay_kv(wv_r, 4 - 4 * q, i, i)

    def wait_unit(u):
        part = recv.at[u, pl.ds(0, SEQ - ROWS)]
        pltpu.make_async_copy(part, part, recv_sem.at[u]).wait()

    with scope('waitkv'):
        wait_unit(U_K)
        wait_unit(U_V)
    def segs(b):
        out = []
        for seg in range(4 * b, 4 * b + 4):
            row = seg * TOK if seg < N_DEV else (2 * N_DEV - 1 - seg) * TOK + SEG
            out.append(slice(row, row + SEG))
        return out

    def pos_block(u, b):
        return jnp.concatenate([recv[u, r, :] for r in segs(b)], axis=0)

    def put_block(u, b, val):
        for n, r in enumerate(segs(b)):
            obuf[u, r, :] = val[n * SEG:(n + 1) * SEG]

    for b in range(NB):
        kt[:, b * BQ:(b + 1) * BQ] = pos_block(U_K, b).T
        vt[:, b * BQ:(b + 1) * BQ] = pos_block(U_V, b).T

    def send_out(u):
        slot = G * chip + u
        for k in range(1, N_CHIP):
            pltpu.make_async_remote_copy(
                src_ref=obuf.at[u, chip_rows(peer(k))], dst_ref=rin.at[slot],
                send_sem=osend_sem, recv_sem=orecv_sem.at[u],
                device_id=dev_of(peer(k)), device_id_type=MESH).start()
        rin[slot] = obuf[u, chip_rows(chip), :]

    def attn_head(g, _):
        with scope('waitq'):
            wait_unit(U_DO + g)
            wait_unit(U_Q + g)
        st = [{} for _ in range(NB)]

        def chunks(b):
            return [slice(k * BQ, (k + 1) * BQ) for k in range(b + 1)]

        def scores(b):
            qb = pos_block(U_Q + g, b)
            dob = pos_block(U_DO + g, b)
            mx = None
            for kc, ks in enumerate(chunks(b)):
                s = dot_nt(pos_block(U_K, kc), qb)
                if kc == b:
                    key = lax.broadcasted_iota(jnp.int32, (BQ, BQ), 0)
                    qry = lax.broadcasted_iota(jnp.int32, (BQ, BQ), 1)
                    s = jnp.where(key <= qry, s, -jnp.inf)
                s_scr[b][ks, :] = s
                mc = jnp.max(s.reshape(BQ // 8, 8, BQ), axis=0)
                mx = mc if mx is None else jnp.maximum(mx, mc)
            for kc, ks in enumerate(chunks(b)):
                dp_scr[b][ks, :] = dot_nt(pos_block(U_V, kc), dob)
            st[b]['m2'] = jnp.max(mx, axis=0, keepdims=True) * C2

        def probs(b):
            m2 = st[b]['m2']
            ls = None
            for ks in chunks(b):
                e = jnp.exp2(s_scr[b][ks, :] * C2 - m2)
                lc = jnp.sum(e.reshape(BQ // 8, 8, BQ), axis=0)
                ls = lc if ls is None else ls + lc
            lse2 = m2 + jnp.log2(jnp.sum(ls, axis=0, keepdims=True))
            for ks in chunks(b):
                p_scr[b][ks, :] = jnp.exp2(s_scr[b][ks, :] * C2 - lse2).astype(BF16)

        def outs(b):
            n = (b + 1) * BQ
            dob = pos_block(U_DO + g, b)
            ot = dot(vt[:, :n], p_scr[b][...]).astype(BF16)
            st[b]['delta'] = jnp.sum(dob.T.astype(F32) * ot.astype(F32), axis=0, keepdims=True)
            for ks in chunks(b):
                dv_acc[ks, :] += dot(p_scr[b][ks, :], dob)

        def dscores(b):
            delta = st[b]['delta']
            for ks in chunks(b):
                ds_scr[b][ks, :] = (p_scr[b][ks, :].astype(F32) * (dp_scr[b][ks, :] - delta)).astype(BF16)

        def grads(b):
            n = (b + 1) * BQ
            qb = pos_block(U_Q + g, b)
            for ks in chunks(b):
                dk_acc[ks, :] += dot(ds_scr[b][ks, :], qb)
            dqt = (dot(kt[:, :n], ds_scr[b][...]) * C).astype(BF16)
            put_block(g, b, dqt.T)

        with scope('attn'):
            scores(3)
            scores(2)
            probs(3)
            outs(3)
            scores(1)
            dscores(3)
            probs(2)
            grads(3)
            outs(2)
            scores(0)
            dscores(2)
            probs(1)
            grads(2)
            outs(1)
            dscores(1)
            probs(0)
            grads(1)
            outs(0)
            dscores(0)
            grads(0)

        with scope('send'):
            send_out(g)
        return 0

    lax.fori_loop(0, G, attn_head, 0)
    def send_owners(n):
        slot = 8 * n + 4 * q + chip

        def send_dev(dev, part):
            pltpu.make_async_remote_copy(
                src_ref=obuf.at[G + n, tok_rows(dev)], dst_ref=rkv.at[slot],
                send_sem=osend_sem, recv_sem=kv_sem.at[n, part],
                device_id=(dp, dev), device_id_type=MESH).start()

        send_dev(partner[1], 0)
        for k in range(1, N_CHIP):
            for r in range(2):
                send_dev(2 * peer(k) + r, k // 2)
        rkv[slot] = obuf[G + n, tok_rows(me), :]

    with scope('senddkv'):
        for b in range(NB):
            put_block(3, b, (dk_acc[b * BQ:(b + 1) * BQ, :] * C).astype(BF16))
        send_owners(0)
        for b in range(NB):
            put_block(4, b, dv_acc[b * BQ:(b + 1) * BQ, :].astype(BF16))
        send_owners(1)

    def p_copy():
        return pltpu.make_async_remote_copy(
            src_ref=acc.at[other], dst_ref=pbuf, send_sem=ps_sem, recv_sem=pr_sem,
            device_id=partner, device_id_type=MESH)

    for u in range(G):
        with scope('waito'):
            part = obuf.at[u, pl.ds(0, SEQ - ROWS)]
            pltpu.make_async_copy(part, part, orecv_sem.at[u]).wait()

        def dx_step(i, _, u=u):
            cols = pl.ds(pl.multiple_of(i * ND, ND), ND)
            t = dot_nt(jnp.concatenate([rin[G * j + u] for j in range(N_CHIP)], axis=1),
                       jnp.concatenate([wq_r[G * j + u, cols, :] for j in range(N_CHIP)], axis=1))
            if u > 0:
                t = t + acc[:, cols]
            acc[:, cols] = t
            return 0

        with scope('dx'):
            lax.fori_loop(0, D // ND, dx_step, 0)
    p_copy().start()

    for n, parts in ((0, (0,)), (0, (1,)), (1, (0,)), (1, (1,))):
            last = n == 1 and 1 in parts
            with scope('waitkv%d%d' % (n, parts[0])):
                for part in parts:
                    ref = obuf.at[0, pl.ds(0, (3, 4)[part] * TOK)]
                    pltpu.make_async_copy(ref, ref, kv_sem.at[n, part]).wait()
            if last:
                with scope('waitp'):
                    p_copy().wait_recv()
            chips = [lax.rem(chip + N_CHIP - k, N_CHIP) for part in parts for k in ((0, 1), (2, 3))[part]]
            heads = [c + 4 * r for c in chips for r in range(2)]

            def kv_dx(i, _, n=n, last=last, heads=heads):
                cols = pl.ds(pl.multiple_of(i * NV, NV), NV)
                t = dot_nt(jnp.concatenate([rkv[8 * n + h] for h in heads], axis=1),
                           jnp.concatenate([(wk_r, wv_r)[n][h, cols, :] for h in heads], axis=1))
                t = t + acc[own, cols]
                if last:
                    out_ref[:, cols] = (t + pbuf[:, cols]).astype(BF16)
                else:
                    acc[own, cols] = t
                return 0

            with scope('kvdx'):
                lax.fori_loop(0, D // NV, kv_dx, 0)

    with scope('final'):
        for n in range(2):
            swap_copy(n).wait_send()
        p_copy().wait_send()
        pltpu.make_async_copy(sbuf, sbuf, send_sem).wait()
        part = obuf.at[pl.ds(0, G), pl.ds(0, SEQ - ROWS)]
        pltpu.make_async_copy(part, part, osend_sem).wait()
        part = obuf.at[pl.ds(0, 2), pl.ds(0, SEQ - TOK)]
        pltpu.make_async_copy(part, part, osend_sem).wait()


def write_out(src, dst, sem):
    cp = pltpu.make_async_copy(src, dst, sem)
    cp.start()
    cp.wait()


def solution(mesh):
    row_spec = P(("dp", "cp"), None)

    def device_fn(x_in, d_y, w_q, w_k, w_v, w_o):
        dma = pltpu.SemaphoreType.DMA
        res = pl.pallas_call(
            kernel,
            out_shape=pltpu.VMEM((TOK, D), BF16),
            in_specs=[pl.BlockSpec(memory_space=pl.ANY)] * 6,
            out_specs=pl.BlockSpec(memory_space=pltpu.VMEM),
            scratch_shapes=[
                pltpu.VMEM((ROWS, D), BF16),
                pltpu.VMEM((ROWS, D), BF16),
                pltpu.VMEM((2, N_CHIP, HD, D), BF16),
                pltpu.VMEM((SLOTS, 256, 3, 4, HD), BF16),
                pltpu.VMEM((12, D, HD), BF16),
                pltpu.VMEM((8, D, HD), BF16),
                pltpu.VMEM((8, D, HD), BF16),
                pltpu.VMEM((8, 3, ROWS, HD), BF16),
                pltpu.VMEM((8, SEQ, HD), BF16),
                pltpu.VMEM((5, SEQ, HD), BF16),
                pltpu.VMEM((12, ROWS, HD), BF16),
                pltpu.VMEM((16, TOK, HD), BF16),
                pltpu.VMEM((ROWS, D), F32),
                pltpu.VMEM((TOK, D), F32),
                *[pltpu.VMEM(((b + 1) * BQ, BQ), t) for t in (F32, F32, BF16, BF16) for b in range(NB)],
                pltpu.VMEM((HD, SEQ), BF16),
                pltpu.VMEM((HD, SEQ), BF16),
                pltpu.VMEM((SEQ, HD), F32),
                pltpu.VMEM((SEQ, HD), F32),
                dma((2,)), dma((2, N_CHIP)), dma((SLOTS,)), dma((2,)), dma((2,)),
                dma, dma((8,)), dma, dma((G,)), dma((2, 2)), dma, dma,
            ],
            compiler_params=pltpu.CompilerParams(
                collective_id=0, has_side_effects=True, vmem_limit_bytes=VLIM),
        )(x_in, d_y, w_q.reshape(12, 256, 6, 4, HD), w_k.reshape(4, 256, 3, 2, 4, HD), w_v.reshape(4, 256, 3, 2, 4, HD),
          w_o.reshape(2, N_CHIP, G, HD, D))
        return pl.pallas_call(
            write_out,
            out_shape=jax.ShapeDtypeStruct((TOK, D), BF16),
            in_specs=[pl.BlockSpec(memory_space=pltpu.VMEM)],
            out_specs=pl.BlockSpec(memory_space=pl.ANY),
            scratch_shapes=[pltpu.SemaphoreType.DMA],
        )(pltpu.with_memory_space_constraint(res, pltpu.VMEM))

    return jax.shard_map(device_fn, mesh=mesh, in_specs=(row_spec, row_spec, P(), P(), P(), P()),
                         out_specs=row_spec, check_vma=False)
```

```python
import math

import jax
import jax.numpy as jnp
from jax import lax
from jax.experimental import pallas as pl
from jax.experimental.pallas import tpu as pltpu
from jax.sharding import PartitionSpec as P

MESH = pl.DeviceIdType.MESH
BF16, F32 = jnp.bfloat16, jnp.float32
NT = (((1,), (1,)), ((), ()))

N_DEV, N_CHIP, TOK, SEG = 8, 4, 128, 64
ROWS = 2 * TOK
SEQ = N_DEV * TOK
D = 3072
HD = 128
G = 3
BQ = 256
NB = SEQ // BQ
C = HD**-0.5
C2 = C * math.log2(math.e)
U_DO, U_K, U_V, U_Q = 0, 3, 4, 5
SLOTS = 12
RB = 128
ND = 3072
NV = 3072
VLIM = 66_000_000

scope = jax.named_scope


def dot_nt(a, b):
    return lax.dot_general(a, b, NT, preferred_element_type=F32)


def dot(a, b):
    return jnp.dot(a, b, preferred_element_type=F32)


def kernel(x_hbm, dy_hbm, wq_hbm, wk_hbm, wv_hbm, wo_hbm, out_ref,
           x_v, dy_v, wo_s, w_s, wq_r, wk_r, wv_r, sbuf, recv, obuf, rin, rkv, acc, pbuf,
           s0, s1, s2, s3, d0, d1, d2, d3, p0, p1, p2, p3, e0, e1, e2, e3, kt, vt, dk_acc, dv_acc,
           io_sem, wo_sem, w_sem, xs_sem, xr_sem, send_sem, recv_sem, osend_sem, orecv_sem, kv_sem, ps_sem, pr_sem):
    s_scr, dp_scr, p_scr, ds_scr = (s0, s1, s2, s3), (d0, d1, d2, d3), (p0, p1, p2, p3), (e0, e1, e2, e3)
    me = lax.axis_index("cp")
    dp = lax.axis_index("dp")
    chip = me // 2
    q = lax.rem(me, 2)
    partner = (dp, 2 * chip + 1 - q)

    def peer(k):
        return lax.rem(chip + k, N_CHIP)

    def dev_of(cc):
        return (dp, 2 * cc + q)

    barrier = pltpu.get_barrier_semaphore()
    pl.semaphore_signal(barrier, inc=1, device_id=partner, device_id_type=MESH)
    for k in range(1, N_CHIP):
        pl.semaphore_signal(barrier, inc=1, device_id=dev_of(peer(k)), device_id_type=MESH)

    def tok_rows(i):
        return pl.ds(pl.multiple_of(i * TOK, TOK), TOK)

    def chip_rows(i):
        return pl.ds(pl.multiple_of(i * ROWS, ROWS), ROWS)

    own, other = tok_rows(q), tok_rows(1 - q)

    def io_copy(n):
        src, dst = ((dy_hbm, dy_v), (x_hbm, x_v))[n]
        return pltpu.make_async_copy(src, dst.at[own], io_sem.at[n])

    def swap_copy(n):
        ref = (dy_v, x_v)[n]
        return pltpu.make_async_remote_copy(
            src_ref=ref.at[own], dst_ref=ref.at[own], send_sem=xs_sem.at[n], recv_sem=xr_sem.at[n],
            device_id=partner, device_id_type=MESH)

    def wo_copy(g, k):
        return pltpu.make_async_copy(wo_hbm.at[q, peer(k), g], wo_s.at[g % 2, k - 1], wo_sem.at[g % 2, k - 1])

    def wkv_copy(w_hbm, i, slot, half=None):
        half = q if half is None else half
        return pltpu.make_async_copy(w_hbm.at[i, :, :, half], w_s.at[slot], w_sem.at[slot])

    def wq_copy(i, slot):
        return pltpu.make_async_copy(wq_hbm.at[i, :, pl.ds(3 * q, 3)], w_s.at[slot], w_sem.at[slot])

    def wait_slot(slot):
        wkv_copy(wk_hbm, 0, slot).wait()

    io_copy(0).start()
    for k in (1, 2):
        wo_copy(0, k).start()
    dk_acc[...] = jnp.zeros_like(dk_acc)
    dv_acc[...] = jnp.zeros_like(dv_acc)
    with scope('barrier'):
        pl.semaphore_wait(barrier, N_CHIP)
    io_copy(1).start()
    for i in range(4):
        wkv_copy(wk_hbm, i, i).start()
    with scope('swapdy'):
        io_copy(0).wait()
        swap_copy(0).start()

    def relay_kv(dst, base, i, slot):
        flat = w_s.at[slot].reshape(768 * 4, HD)
        for h in range(4):
            for r in range(0, 768, RB):
                dst[base + h, pl.ds(i * 768 + r, RB), :] = flat[pl.ds(4 * r + h, RB, stride=4), :]

    def relay_q(i, slot):
        flat = w_s.at[slot].reshape(768 * 4, HD)
        for h in range(12):
            for r in range(0, 256, RB):
                wq_r[h, pl.ds(i * 256 + r, RB), :] = flat[pl.ds(12 * r + h, RB, stride=12), :]


    def send_part(unit, k, val, rows, dst_rows):
        if k == N_CHIP:
            recv[unit, dst_rows, :] = val
            return
        sbuf[unit, k - 1, rows, :] = val
        pltpu.make_async_remote_copy(
            src_ref=sbuf.at[unit, k - 1, rows], dst_ref=recv.at[unit, dst_rows],
            send_sem=send_sem, recv_sem=recv_sem.at[unit],
            device_id=dev_of(peer(k)), device_id_type=MESH).start()

    def send_rows(unit, k, val, r):
        send_part(unit, k, val, tok_rows(r), tok_rows(2 * chip + r))

    def send_block(unit, k, val):
        send_part(unit, k, val, pl.ds(0, ROWS), chip_rows(chip))

    def do0_rows(r, ks):
        w = wo_s[0, pl.ds(ks[0] - 1, len(ks))].reshape(len(ks) * HD, D)
        val = dot_nt(dy_v[tok_rows(r), :], w).astype(BF16)
        for n, k in enumerate(ks):
            send_rows(U_DO, k, val[:, n * HD:(n + 1) * HD], r)

    def do_steps(g):
        for k in range(1, 5):
            wo_copy(g, k).wait()
        val = dot_nt(dy_v[...], wo_s[g % 2].reshape(4 * HD, D)).astype(BF16)
        for k in range(1, 5):
            send_block(U_DO + g, k, val[:, (k - 1) * HD:k * HD])

    def k_rows(r):
        w = jnp.concatenate([wk_r[4 * q + peer(k)] for k in range(1, 5)], axis=1)
        val = dot(x_v[tok_rows(r), :], w).astype(BF16)
        for k in range(1, 5):
            send_rows(U_K, k, val[:, (k - 1) * HD:k * HD], r)

    def v_steps():
        w = jnp.concatenate([wv_r[4 * q + peer(k)] for k in range(1, 5)], axis=1)
        val = dot(x_v[...], w).astype(BF16)
        for k in range(1, 5):
            send_block(U_V, k, val[:, (k - 1) * HD:k * HD])

    def q_steps(g):
        w = jnp.concatenate([wq_r[3 * peer(k) + g] for k in range(1, 5)], axis=1)
        val = dot(x_v[...], w).astype(BF16)
        for k in range(1, 5):
            send_block(U_Q + g, k, val[:, (k - 1) * HD:k * HD])

    with scope('do0a'):
        for k in (1, 2):
            wo_copy(0, k).wait()
        do0_rows(q, (1, 2))
    for i in range(4):
        wkv_copy(wv_hbm, i, 4 + i).start()
    with scope('swapx'):
        io_copy(1).wait()
        swap_copy(1).start()
    with scope('relk'):
        for i in range(4):
            wait_slot(i)
            relay_kv(wk_r, 4 * q, i, i)
    for k in (3, 4):
        wo_copy(0, k).start()
    with scope('k_own'):
        k_rows(q)
    with scope('xswap'):
        swap_copy(1).wait_recv()
    with scope('k_other'):
        k_rows(1 - q)
    with scope('relv'):
        for i in range(4):
            wait_slot(4 + i)
            relay_kv(wv_r, 4 * q, i, 4 + i)
    for i in range(4):
        wq_copy(i, 8 + i).start()
    with scope('v'):
        v_steps()
    for i in range(4):
        wq_copy(4 + i, i).start()
    with scope('do0b'):
        for k in (3, 4):
            wo_copy(0, k).wait()
        do0_rows(q, (3, 4))
    for i in range(4):
        wq_copy(8 + i, 4 + i).start()
    with scope('dyswap'):
        swap_copy(0).wait_recv()
    with scope('do0c'):
        do0_rows(1 - q, (1, 2, 3, 4))
    for k in range(1, 5):
        wo_copy(1, k).start()
    with scope('relq'):
        for i in range(12):
            slot = (8 + i) % SLOTS
            wait_slot(slot)
            relay_q(i, slot)
    for k in range(1, 5):
        wo_copy(2, k).start()
    with scope('q0'):
        q_steps(0)
    for i in range(8):
        wkv_copy((wk_hbm, wv_hbm)[i // 4], i % 4, (8 + i) % SLOTS, 1 - q).start()
    for g in (1, 2):
        with scope('do12'):
            do_steps(g)
        with scope('q12'):
            q_steps(g)
    with scope('relkv2'):
        for i in range(4):
            wait_slot(8 + i)
            relay_kv(wk_r, 4 - 4 * q, i, 8 + i)
            wait_slot(i)
            relay_kv(wv_r, 4 - 4 * q, i, i)

    def wait_unit(u):
        part = recv.at[u, pl.ds(0, SEQ - ROWS)]
        pltpu.make_async_copy(part, part, recv_sem.at[u]).wait()

    with scope('waitkv'):
        wait_unit(U_K)
        wait_unit(U_V)
    def segs(b):
        out = []
        for seg in range(4 * b, 4 * b + 4):
            row = seg * TOK if seg < N_DEV else (2 * N_DEV - 1 - seg) * TOK + SEG
            out.append(slice(row, row + SEG))
        return out

    def pos_block(u, b):
        return jnp.concatenate([recv[u, r, :] for r in segs(b)], axis=0)

    def put_block(u, b, val):
        for n, r in enumerate(segs(b)):
            obuf[u, r, :] = val[n * SEG:(n + 1) * SEG]

    for b in range(NB):
        kt[:, b * BQ:(b + 1) * BQ] = pos_block(U_K, b).T
        vt[:, b * BQ:(b + 1) * BQ] = pos_block(U_V, b).T

    def send_out(u):
        slot = G * chip + u
        for k in range(1, N_CHIP):
            pltpu.make_async_remote_copy(
                src_ref=obuf.at[u, chip_rows(peer(k))], dst_ref=rin.at[slot],
                send_sem=osend_sem, recv_sem=orecv_sem.at[u],
                device_id=dev_of(peer(k)), device_id_type=MESH).start()
        rin[slot] = obuf[u, chip_rows(chip), :]

    def attn_head(g, _):
        with scope('waitq'):
            wait_unit(U_DO + g)
            wait_unit(U_Q + g)
        st = [{} for _ in range(NB)]

        def chunks(b):
            return [slice(k * BQ, (k + 1) * BQ) for k in range(b + 1)]

        def scores(b):
            qb = pos_block(U_Q + g, b)
            dob = pos_block(U_DO + g, b)
            mx = None
            for kc, ks in enumerate(chunks(b)):
                s = dot_nt(pos_block(U_K, kc), qb)
                if kc == b:
                    key = lax.broadcasted_iota(jnp.int32, (BQ, BQ), 0)
                    qry = lax.broadcasted_iota(jnp.int32, (BQ, BQ), 1)
                    s = jnp.where(key <= qry, s, -jnp.inf)
                s_scr[b][ks, :] = s
                mc = jnp.max(s.reshape(BQ // 8, 8, BQ), axis=0)
                mx = mc if mx is None else jnp.maximum(mx, mc)
            for kc, ks in enumerate(chunks(b)):
                dp_scr[b][ks, :] = dot_nt(pos_block(U_V, kc), dob)
            st[b]['m2'] = jnp.max(mx, axis=0, keepdims=True) * C2

        def probs(b):
            m2 = st[b]['m2']
            ls = None
            for ks in chunks(b):
                e = jnp.exp2(s_scr[b][ks, :] * C2 - m2)
                lc = jnp.sum(e.reshape(BQ // 8, 8, BQ), axis=0)
                ls = lc if ls is None else ls + lc
            lse2 = m2 + jnp.log2(jnp.sum(ls, axis=0, keepdims=True))
            for ks in chunks(b):
                p_scr[b][ks, :] = jnp.exp2(s_scr[b][ks, :] * C2 - lse2).astype(BF16)

        def outs(b):
            n = (b + 1) * BQ
            dob = pos_block(U_DO + g, b)
            ot = dot(vt[:, :n], p_scr[b][...]).astype(BF16)
            st[b]['delta'] = jnp.sum(dob.T.astype(F32) * ot.astype(F32), axis=0, keepdims=True)
            for ks in chunks(b):
                dv_acc[ks, :] += dot(p_scr[b][ks, :], dob)

        def dscores(b):
            delta = st[b]['delta']
            for ks in chunks(b):
                ds_scr[b][ks, :] = (p_scr[b][ks, :].astype(F32) * (dp_scr[b][ks, :] - delta)).astype(BF16)

        def grads(b):
            n = (b + 1) * BQ
            qb = pos_block(U_Q + g, b)
            for ks in chunks(b):
                dk_acc[ks, :] += dot(ds_scr[b][ks, :], qb)
            dqt = (dot(kt[:, :n], ds_scr[b][...]) * C).astype(BF16)
            put_block(g, b, dqt.T)

        with scope('attn'):
            scores(3)
            scores(2)
            probs(3)
            outs(3)
            scores(1)
            dscores(3)
            probs(2)
            grads(3)
            outs(2)
            scores(0)
            dscores(2)
            probs(1)
            grads(2)
            outs(1)
            dscores(1)
            probs(0)
            grads(1)
            outs(0)
            dscores(0)
            grads(0)

        with scope('send'):
            send_out(g)
        return 0

    lax.fori_loop(0, G, attn_head, 0)
    def send_owners(n):
        slot = 8 * n + 4 * q + chip

        def send_dev(dev, part):
            pltpu.make_async_remote_copy(
                src_ref=obuf.at[G + n, tok_rows(dev)], dst_ref=rkv.at[slot],
                send_sem=osend_sem, recv_sem=kv_sem.at[n, part],
                device_id=(dp, dev), device_id_type=MESH).start()

        send_dev(partner[1], 0)
        for k in range(1, N_CHIP):
            for r in range(2):
                send_dev(2 * peer(k) + r, 2 if n == 1 and k == 3 else 1)
        rkv[slot] = obuf[G + n, tok_rows(me), :]

    with scope('senddkv'):
        for b in range(NB):
            put_block(3, b, (dk_acc[b * BQ:(b + 1) * BQ, :] * C).astype(BF16))
        send_owners(0)
        for b in range(NB):
            put_block(4, b, dv_acc[b * BQ:(b + 1) * BQ, :].astype(BF16))
        send_owners(1)

    def p_copy():
        return pltpu.make_async_remote_copy(
            src_ref=acc.at[other], dst_ref=pbuf, send_sem=ps_sem, recv_sem=pr_sem,
            device_id=partner, device_id_type=MESH)

    def wait_kv(n, part, count):
        ref = obuf.at[0, pl.ds(0, count * TOK)]
        pltpu.make_async_copy(ref, ref, kv_sem.at[n, part]).wait()

    def kv_dx(items, last=False):
        lhs, rhs = [], []
        for n, k in items:
            c = lax.rem(chip + N_CHIP - k, N_CHIP)
            for r in range(2):
                lhs.append(rkv[8 * n + 4 * r + c])
                rhs.append((wk_r, wv_r)[n][4 * r + c])
        t = dot_nt(jnp.concatenate(lhs, axis=1), jnp.concatenate(rhs, axis=1)) + acc[own, :]
        if last:
            out_ref[...] = (t + pbuf[...]).astype(BF16)
        else:
            acc[own, :] = t

    for u in range(G):
        with scope('waito'):
            part = obuf.at[u, pl.ds(0, SEQ - ROWS)]
            pltpu.make_async_copy(part, part, orecv_sem.at[u]).wait()
        with scope('dx'):
            t = dot_nt(jnp.concatenate([rin[G * j + u] for j in range(N_CHIP)], axis=1),
                       jnp.concatenate([wq_r[G * j + u] for j in range(N_CHIP)], axis=1))
            acc[...] = t if u == 0 else t + acc[...]
        if u == 0:
            with scope('kvlocal'):
                wait_kv(0, 0, 1)
                wait_kv(1, 0, 1)
                kv_dx([(0, 0), (1, 0)])
    p_copy().start()

    with scope('waitk'):
        wait_kv(0, 1, 6)
    with scope('kdx'):
        kv_dx([(0, 1), (0, 2), (0, 3)])
    with scope('waitv1'):
        wait_kv(1, 1, 4)
    with scope('vdx1'):
        kv_dx([(1, 1), (1, 2)])
    with scope('waitv2'):
        wait_kv(1, 2, 2)
    with scope('waitp'):
        p_copy().wait_recv()
    with scope('vdx2'):
        kv_dx([(1, 3)], last=True)

    with scope('final'):
        for n in range(2):
            swap_copy(n).wait_send()
        p_copy().wait_send()
        pltpu.make_async_copy(sbuf, sbuf, send_sem).wait()
        part = obuf.at[pl.ds(0, G), pl.ds(0, SEQ - ROWS)]
        pltpu.make_async_copy(part, part, osend_sem).wait()
        part = obuf.at[pl.ds(0, 2), pl.ds(0, SEQ - TOK)]
        pltpu.make_async_copy(part, part, osend_sem).wait()


def write_out(src, dst, sem):
    cp = pltpu.make_async_copy(src, dst, sem)
    cp.start()
    cp.wait()


def solution(mesh):
    row_spec = P(("dp", "cp"), None)

    def device_fn(x_in, d_y, w_q, w_k, w_v, w_o):
        dma = pltpu.SemaphoreType.DMA
        res = pl.pallas_call(
            kernel,
            out_shape=pltpu.VMEM((TOK, D), BF16),
            in_specs=[pl.BlockSpec(memory_space=pl.ANY)] * 6,
            out_specs=pl.BlockSpec(memory_space=pltpu.VMEM),
            scratch_shapes=[
                pltpu.VMEM((ROWS, D), BF16),
                pltpu.VMEM((ROWS, D), BF16),
                pltpu.VMEM((2, N_CHIP, HD, D), BF16),
                pltpu.VMEM((SLOTS, 256, 3, 4, HD), BF16),
                pltpu.VMEM((12, D, HD), BF16),
                pltpu.VMEM((8, D, HD), BF16),
                pltpu.VMEM((8, D, HD), BF16),
                pltpu.VMEM((8, 3, ROWS, HD), BF16),
                pltpu.VMEM((8, SEQ, HD), BF16),
                pltpu.VMEM((5, SEQ, HD), BF16),
                pltpu.VMEM((12, ROWS, HD), BF16),
                pltpu.VMEM((16, TOK, HD), BF16),
                pltpu.VMEM((ROWS, D), F32),
                pltpu.VMEM((TOK, D), F32),
                *[pltpu.VMEM(((b + 1) * BQ, BQ), t) for t in (F32, F32, BF16, BF16) for b in range(NB)],
                pltpu.VMEM((HD, SEQ), BF16),
                pltpu.VMEM((HD, SEQ), BF16),
                pltpu.VMEM((SEQ, HD), F32),
                pltpu.VMEM((SEQ, HD), F32),
                dma((2,)), dma((2, N_CHIP)), dma((SLOTS,)), dma((2,)), dma((2,)),
                dma, dma((8,)), dma, dma((G,)), dma((2, 3)), dma, dma,
            ],
            compiler_params=pltpu.CompilerParams(
                collective_id=0, has_side_effects=True, vmem_limit_bytes=VLIM),
        )(x_in, d_y, w_q.reshape(12, 256, 6, 4, HD), w_k.reshape(4, 256, 3, 2, 4, HD), w_v.reshape(4, 256, 3, 2, 4, HD),
          w_o.reshape(2, N_CHIP, G, HD, D))
        return pl.pallas_call(
            write_out,
            out_shape=jax.ShapeDtypeStruct((TOK, D), BF16),
            in_specs=[pl.BlockSpec(memory_space=pltpu.VMEM)],
            out_specs=pl.BlockSpec(memory_space=pl.ANY),
            scratch_shapes=[pltpu.SemaphoreType.DMA],
        )(pltpu.with_memory_space_constraint(res, pltpu.VMEM))

    return jax.shard_map(device_fn, mesh=mesh, in_specs=(row_spec, row_spec, P(), P(), P(), P()),
                         out_specs=row_spec, check_vma=False)
```

```python
import math

import jax
import jax.numpy as jnp
from jax import lax
from jax.experimental import pallas as pl
from jax.experimental.pallas import tpu as pltpu
from jax.sharding import PartitionSpec as P

MESH = pl.DeviceIdType.MESH
BF16, F32 = jnp.bfloat16, jnp.float32
NT = (((1,), (1,)), ((), ()))

N_DEV, N_CHIP, TOK, SEG = 8, 4, 128, 64
ROWS = 2 * TOK
SEQ = N_DEV * TOK
D = 3072
HD = 128
G = 3
BQ = 256
NB = SEQ // BQ
C = HD**-0.5
C2 = C * math.log2(math.e)
U_DO, U_K, U_V, U_Q = 0, 3, 4, 5
SLOTS = 12
RB = 128
ND = 3072
NV = 3072
VLIM = 66_000_000

scope = jax.named_scope


def dot_nt(a, b):
    return lax.dot_general(a, b, NT, preferred_element_type=F32)


def dot(a, b):
    return jnp.dot(a, b, preferred_element_type=F32)


def kernel(x_hbm, dy_hbm, wq_hbm, wk_hbm, wv_hbm, wo_hbm, out_ref,
           x_v, dy_v, wo_s, w_s, wq_r, wk_r, wv_r, sbuf, recv, obuf, rin, rkv, acc, pbuf,
           s0, s1, s2, s3, d0, d1, d2, d3, p0, p1, p2, p3, e0, e1, e2, e3, kt, vt, dk_acc, dv_acc,
           io_sem, wo_sem, w_sem, xs_sem, xr_sem, send_sem, recv_sem, osend_sem, orecv_sem, kv_sem, ps_sem, pr_sem):
    s_scr, dp_scr, p_scr, ds_scr = (s0, s1, s2, s3), (d0, d1, d2, d3), (p0, p1, p2, p3), (e0, e1, e2, e3)
    me = lax.axis_index("cp")
    dp = lax.axis_index("dp")
    chip = me // 2
    q = lax.rem(me, 2)
    partner = (dp, 2 * chip + 1 - q)

    def peer(k):
        return lax.rem(chip + k, N_CHIP)

    def dev_of(cc):
        return (dp, 2 * cc + q)

    barrier = pltpu.get_barrier_semaphore()
    pl.semaphore_signal(barrier, inc=1, device_id=partner, device_id_type=MESH)
    for k in range(1, N_CHIP):
        pl.semaphore_signal(barrier, inc=1, device_id=dev_of(peer(k)), device_id_type=MESH)

    def tok_rows(i):
        return pl.ds(pl.multiple_of(i * TOK, TOK), TOK)

    def chip_rows(i):
        return pl.ds(pl.multiple_of(i * ROWS, ROWS), ROWS)

    own, other = tok_rows(q), tok_rows(1 - q)

    def io_copy(n):
        src, dst = ((dy_hbm, dy_v), (x_hbm, x_v))[n]
        return pltpu.make_async_copy(src, dst.at[own], io_sem.at[n])

    def swap_copy(n):
        ref = (dy_v, x_v)[n]
        return pltpu.make_async_remote_copy(
            src_ref=ref.at[own], dst_ref=ref.at[own], send_sem=xs_sem.at[n], recv_sem=xr_sem.at[n],
            device_id=partner, device_id_type=MESH)

    def wo_copy(g, k):
        return pltpu.make_async_copy(wo_hbm.at[q, peer(k), g], wo_s.at[g % 2, k - 1], wo_sem.at[g % 2, k - 1])

    def wkv_copy(w_hbm, i, slot, half=None):
        half = q if half is None else half
        return pltpu.make_async_copy(w_hbm.at[i, :, :, half], w_s.at[slot], w_sem.at[slot])

    def wq_copy(i, slot):
        return pltpu.make_async_copy(wq_hbm.at[i, :, pl.ds(3 * q, 3)], w_s.at[slot], w_sem.at[slot])

    def wait_slot(slot):
        wkv_copy(wk_hbm, 0, slot).wait()

    io_copy(0).start()
    for k in (1, 2):
        wo_copy(0, k).start()
    dk_acc[...] = jnp.zeros_like(dk_acc)
    dv_acc[...] = jnp.zeros_like(dv_acc)
    with scope('barrier'):
        pl.semaphore_wait(barrier, N_CHIP)
    io_copy(1).start()
    for i in range(4):
        wkv_copy(wk_hbm, i, i).start()
    with scope('swapdy'):
        io_copy(0).wait()
        swap_copy(0).start()

    def relay_kv(dst, base, i, slot):
        flat = w_s.at[slot].reshape(768 * 4, HD)
        for h in range(4):
            for r in range(0, 768, RB):
                dst[base + h, pl.ds(i * 768 + r, RB), :] = flat[pl.ds(4 * r + h, RB, stride=4), :]

    def relay_q(i, slot):
        flat = w_s.at[slot].reshape(768 * 4, HD)
        for h in range(12):
            for r in range(0, 256, RB):
                wq_r[h, pl.ds(i * 256 + r, RB), :] = flat[pl.ds(12 * r + h, RB, stride=12), :]


    def send_part(unit, k, val, rows, dst_rows):
        if k == N_CHIP:
            recv[unit, dst_rows, :] = val
            return
        sbuf[unit, k - 1, rows, :] = val
        pltpu.make_async_remote_copy(
            src_ref=sbuf.at[unit, k - 1, rows], dst_ref=recv.at[unit, dst_rows],
            send_sem=send_sem, recv_sem=recv_sem.at[unit],
            device_id=dev_of(peer(k)), device_id_type=MESH).start()

    def send_rows(unit, k, val, r):
        send_part(unit, k, val, tok_rows(r), tok_rows(2 * chip + r))

    def send_block(unit, k, val):
        send_part(unit, k, val, pl.ds(0, ROWS), chip_rows(chip))

    def do0_rows(r, ks):
        w = wo_s[0, pl.ds(ks[0] - 1, len(ks))].reshape(len(ks) * HD, D)
        val = dot_nt(dy_v[tok_rows(r), :], w).astype(BF16)
        for n, k in enumerate(ks):
            send_rows(U_DO, k, val[:, n * HD:(n + 1) * HD], r)

    def do_steps(g):
        for k in range(1, 5):
            wo_copy(g, k).wait()
        val = dot_nt(dy_v[...], wo_s[g % 2].reshape(4 * HD, D)).astype(BF16)
        for k in range(1, 5):
            send_block(U_DO + g, k, val[:, (k - 1) * HD:k * HD])

    def k_rows(r):
        w = jnp.concatenate([wk_r[4 * q + peer(k)] for k in range(1, 5)], axis=1)
        val = dot(x_v[tok_rows(r), :], w).astype(BF16)
        for k in range(1, 5):
            send_rows(U_K, k, val[:, (k - 1) * HD:k * HD], r)

    def v_steps():
        w = jnp.concatenate([wv_r[4 * q + peer(k)] for k in range(1, 5)], axis=1)
        val = dot(x_v[...], w).astype(BF16)
        for k in range(1, 5):
            send_block(U_V, k, val[:, (k - 1) * HD:k * HD])

    def q_steps(g):
        w = jnp.concatenate([wq_r[3 * peer(k) + g] for k in range(1, 5)], axis=1)
        val = dot(x_v[...], w).astype(BF16)
        for k in range(1, 5):
            send_block(U_Q + g, k, val[:, (k - 1) * HD:k * HD])

    with scope('do0a'):
        for k in (1, 2):
            wo_copy(0, k).wait()
        do0_rows(q, (1, 2))
    for i in range(4):
        wkv_copy(wv_hbm, i, 4 + i).start()
    with scope('swapx'):
        io_copy(1).wait()
        swap_copy(1).start()
    with scope('relk'):
        for i in range(4):
            wait_slot(i)
            relay_kv(wk_r, 4 * q, i, i)
    for k in (3, 4):
        wo_copy(0, k).start()
    with scope('k_own'):
        k_rows(q)
    with scope('xswap'):
        swap_copy(1).wait_recv()
    with scope('k_other'):
        k_rows(1 - q)
    with scope('relv'):
        for i in range(4):
            wait_slot(4 + i)
            relay_kv(wv_r, 4 * q, i, 4 + i)
    for i in range(4):
        wq_copy(i, 8 + i).start()
    with scope('v'):
        v_steps()
    for i in range(4):
        wq_copy(4 + i, i).start()
    with scope('do0b'):
        for k in (3, 4):
            wo_copy(0, k).wait()
        do0_rows(q, (3, 4))
    for i in range(4):
        wq_copy(8 + i, 4 + i).start()
    with scope('dyswap'):
        swap_copy(0).wait_recv()
    with scope('do0c'):
        do0_rows(1 - q, (1, 2, 3, 4))
    for k in range(1, 5):
        wo_copy(1, k).start()
    with scope('relq'):
        for i in range(12):
            slot = (8 + i) % SLOTS
            wait_slot(slot)
            relay_q(i, slot)
    for k in range(1, 5):
        wo_copy(2, k).start()
    with scope('q0'):
        q_steps(0)
    for i in range(8):
        wkv_copy((wk_hbm, wv_hbm)[i // 4], i % 4, (8 + i) % SLOTS, 1 - q).start()
    for g in (1, 2):
        with scope('do12'):
            do_steps(g)
        with scope('q12'):
            q_steps(g)
    with scope('relkv2'):
        for i in range(4):
            wait_slot(8 + i)
            relay_kv(wk_r, 4 - 4 * q, i, 8 + i)
            wait_slot(i)
            relay_kv(wv_r, 4 - 4 * q, i, i)

    def wait_unit(u):
        part = recv.at[u, pl.ds(0, SEQ - ROWS)]
        pltpu.make_async_copy(part, part, recv_sem.at[u]).wait()

    with scope('waitkv'):
        wait_unit(U_K)
        wait_unit(U_V)
    def segs(b):
        out = []
        for seg in range(4 * b, 4 * b + 4):
            row = seg * TOK if seg < N_DEV else (2 * N_DEV - 1 - seg) * TOK + SEG
            out.append(slice(row, row + SEG))
        return out

    def pos_block(u, b):
        return jnp.concatenate([recv[u, r, :] for r in segs(b)], axis=0)

    def put_block(u, b, val):
        for n, r in enumerate(segs(b)):
            obuf[u, r, :] = val[n * SEG:(n + 1) * SEG]

    for b in range(NB):
        kt[:, b * BQ:(b + 1) * BQ] = pos_block(U_K, b).T
        vt[:, b * BQ:(b + 1) * BQ] = pos_block(U_V, b).T

    def send_out(u):
        slot = G * chip + u
        for k in range(1, N_CHIP):
            pltpu.make_async_remote_copy(
                src_ref=obuf.at[u, chip_rows(peer(k))], dst_ref=rin.at[slot],
                send_sem=osend_sem, recv_sem=orecv_sem.at[u],
                device_id=dev_of(peer(k)), device_id_type=MESH).start()
        rin[slot] = obuf[u, chip_rows(chip), :]

    def attn_head(g, _):
        with scope('waitq'):
            wait_unit(U_DO + g)
            wait_unit(U_Q + g)
        st = [{} for _ in range(NB)]

        def chunks(b):
            return [slice(k * BQ, (k + 1) * BQ) for k in range(b + 1)]

        def scores(b):
            qb = pos_block(U_Q + g, b)
            dob = pos_block(U_DO + g, b)
            mx = None
            for kc, ks in enumerate(chunks(b)):
                s = dot_nt(pos_block(U_K, kc), qb)
                if kc == b:
                    key = lax.broadcasted_iota(jnp.int32, (BQ, BQ), 0)
                    qry = lax.broadcasted_iota(jnp.int32, (BQ, BQ), 1)
                    s = jnp.where(key <= qry, s, -jnp.inf)
                s_scr[b][ks, :] = s
                mc = jnp.max(s.reshape(BQ // 8, 8, BQ), axis=0)
                mx = mc if mx is None else jnp.maximum(mx, mc)
            for kc, ks in enumerate(chunks(b)):
                dp_scr[b][ks, :] = dot_nt(pos_block(U_V, kc), dob)
            st[b]['m2'] = jnp.max(mx, axis=0, keepdims=True) * C2

        def probs(b):
            m2 = st[b]['m2']
            ls = None
            for ks in chunks(b):
                e = jnp.exp2(s_scr[b][ks, :] * C2 - m2)
                lc = jnp.sum(e.reshape(BQ // 8, 8, BQ), axis=0)
                ls = lc if ls is None else ls + lc
            lse2 = m2 + jnp.log2(jnp.sum(ls, axis=0, keepdims=True))
            for ks in chunks(b):
                p_scr[b][ks, :] = jnp.exp2(s_scr[b][ks, :] * C2 - lse2).astype(BF16)

        def outs(b):
            n = (b + 1) * BQ
            dob = pos_block(U_DO + g, b)
            ot = dot(vt[:, :n], p_scr[b][...]).astype(BF16)
            st[b]['delta'] = jnp.sum(dob.T.astype(F32) * ot.astype(F32), axis=0, keepdims=True)
            for ks in chunks(b):
                dv_acc[ks, :] += dot(p_scr[b][ks, :], dob)

        def dscores(b):
            delta = st[b]['delta']
            for ks in chunks(b):
                ds_scr[b][ks, :] = (p_scr[b][ks, :].astype(F32) * (dp_scr[b][ks, :] - delta)).astype(BF16)

        def grads(b):
            n = (b + 1) * BQ
            qb = pos_block(U_Q + g, b)
            for ks in chunks(b):
                dk_acc[ks, :] += dot(ds_scr[b][ks, :], qb)
            dqt = (dot(kt[:, :n], ds_scr[b][...]) * C).astype(BF16)
            put_block(g, b, dqt.T)

        with scope('attn'):
            scores(3)
            scores(2)
            probs(3)
            outs(3)
            scores(1)
            dscores(3)
            probs(2)
            grads(3)
            outs(2)
            scores(0)
            dscores(2)
            probs(1)
            grads(2)
            outs(1)
            dscores(1)
            probs(0)
            grads(1)
            outs(0)
            dscores(0)
            grads(0)

        with scope('send'):
            send_out(g)
        return 0

    lax.fori_loop(0, G, attn_head, 0)
    def send_owners(n):
        slot = 8 * n + 4 * q + chip

        def send_dev(dev, part):
            pltpu.make_async_remote_copy(
                src_ref=obuf.at[G + n, tok_rows(dev)], dst_ref=rkv.at[slot],
                send_sem=osend_sem, recv_sem=kv_sem.at[n, part],
                device_id=(dp, dev), device_id_type=MESH).start()

        send_dev(partner[1], 0)
        for k in range(1, N_CHIP):
            for r in range(2):
                send_dev(2 * peer(k) + r, k if n == 1 else 1)
        rkv[slot] = obuf[G + n, tok_rows(me), :]

    with scope('senddkv'):
        for b in range(NB):
            put_block(3, b, (dk_acc[b * BQ:(b + 1) * BQ, :] * C).astype(BF16))
        send_owners(0)
        for b in range(NB):
            put_block(4, b, dv_acc[b * BQ:(b + 1) * BQ, :].astype(BF16))
        send_owners(1)

    def p_copy():
        return pltpu.make_async_remote_copy(
            src_ref=acc.at[other], dst_ref=pbuf, send_sem=ps_sem, recv_sem=pr_sem,
            device_id=partner, device_id_type=MESH)

    def wait_kv(n, part, count):
        ref = obuf.at[0, pl.ds(0, count * TOK)]
        pltpu.make_async_copy(ref, ref, kv_sem.at[n, part]).wait()

    def kv_dx(items, last=False):
        lhs, rhs = [], []
        for n, k in items:
            c = lax.rem(chip + N_CHIP - k, N_CHIP)
            for r in range(2):
                lhs.append(rkv[8 * n + 4 * r + c])
                rhs.append((wk_r, wv_r)[n][4 * r + c])
        t = dot_nt(jnp.concatenate(lhs, axis=1), jnp.concatenate(rhs, axis=1)) + acc[own, :]
        if last:
            out_ref[...] = (t + pbuf[...]).astype(BF16)
        else:
            acc[own, :] = t

    for u in range(G):
        with scope('waito'):
            part = obuf.at[u, pl.ds(0, SEQ - ROWS)]
            pltpu.make_async_copy(part, part, orecv_sem.at[u]).wait()
        with scope('dx'):
            t = dot_nt(jnp.concatenate([rin[G * j + u] for j in range(N_CHIP)], axis=1),
                       jnp.concatenate([wq_r[G * j + u] for j in range(N_CHIP)], axis=1))
            acc[...] = t if u == 0 else t + acc[...]
        if u == 0:
            with scope('kvlocal'):
                wait_kv(0, 0, 1)
                wait_kv(1, 0, 1)
                kv_dx([(0, 0), (1, 0)])
    p_copy().start()

    with scope('waitk'):
        wait_kv(0, 1, 6)
    with scope('kdx'):
        kv_dx([(0, 1), (0, 2), (0, 3)])
    for k in (1, 2):
        with scope('waitv%d' % k):
            wait_kv(1, k, 2)
        with scope('vdx%d' % k):
            kv_dx([(1, k)])
    with scope('waitv3'):
        wait_kv(1, 3, 2)
    with scope('waitp'):
        p_copy().wait_recv()
    with scope('vdx3'):
        kv_dx([(1, 3)], last=True)

    with scope('final'):
        for n in range(2):
            swap_copy(n).wait_send()
        p_copy().wait_send()
        pltpu.make_async_copy(sbuf, sbuf, send_sem).wait()
        part = obuf.at[pl.ds(0, G), pl.ds(0, SEQ - ROWS)]
        pltpu.make_async_copy(part, part, osend_sem).wait()
        part = obuf.at[pl.ds(0, 2), pl.ds(0, SEQ - TOK)]
        pltpu.make_async_copy(part, part, osend_sem).wait()


def write_out(src, dst, sem):
    cp = pltpu.make_async_copy(src, dst, sem)
    cp.start()
    cp.wait()


def solution(mesh):
    row_spec = P(("dp", "cp"), None)

    def device_fn(x_in, d_y, w_q, w_k, w_v, w_o):
        dma = pltpu.SemaphoreType.DMA
        res = pl.pallas_call(
            kernel,
            out_shape=pltpu.VMEM((TOK, D), BF16),
            in_specs=[pl.BlockSpec(memory_space=pl.ANY)] * 6,
            out_specs=pl.BlockSpec(memory_space=pltpu.VMEM),
            scratch_shapes=[
                pltpu.VMEM((ROWS, D), BF16),
                pltpu.VMEM((ROWS, D), BF16),
                pltpu.VMEM((2, N_CHIP, HD, D), BF16),
                pltpu.VMEM((SLOTS, 256, 3, 4, HD), BF16),
                pltpu.VMEM((12, D, HD), BF16),
                pltpu.VMEM((8, D, HD), BF16),
                pltpu.VMEM((8, D, HD), BF16),
                pltpu.VMEM((8, 3, ROWS, HD), BF16),
                pltpu.VMEM((8, SEQ, HD), BF16),
                pltpu.VMEM((5, SEQ, HD), BF16),
                pltpu.VMEM((12, ROWS, HD), BF16),
                pltpu.VMEM((16, TOK, HD), BF16),
                pltpu.VMEM((ROWS, D), F32),
                pltpu.VMEM((TOK, D), F32),
                *[pltpu.VMEM(((b + 1) * BQ, BQ), t) for t in (F32, F32, BF16, BF16) for b in range(NB)],
                pltpu.VMEM((HD, SEQ), BF16),
                pltpu.VMEM((HD, SEQ), BF16),
                pltpu.VMEM((SEQ, HD), F32),
                pltpu.VMEM((SEQ, HD), F32),
                dma((2,)), dma((2, N_CHIP)), dma((SLOTS,)), dma((2,)), dma((2,)),
                dma, dma((8,)), dma, dma((G,)), dma((2, 4)), dma, dma,
            ],
            compiler_params=pltpu.CompilerParams(
                collective_id=0, has_side_effects=True, vmem_limit_bytes=VLIM),
        )(x_in, d_y, w_q.reshape(12, 256, 6, 4, HD), w_k.reshape(4, 256, 3, 2, 4, HD), w_v.reshape(4, 256, 3, 2, 4, HD),
          w_o.reshape(2, N_CHIP, G, HD, D))
        return pl.pallas_call(
            write_out,
            out_shape=jax.ShapeDtypeStruct((TOK, D), BF16),
            in_specs=[pl.BlockSpec(memory_space=pltpu.VMEM)],
            out_specs=pl.BlockSpec(memory_space=pl.ANY),
            scratch_shapes=[pltpu.SemaphoreType.DMA],
        )(pltpu.with_memory_space_constraint(res, pltpu.VMEM))

    return jax.shard_map(device_fn, mesh=mesh, in_specs=(row_spec, row_spec, P(), P(), P(), P()),
                         out_specs=row_spec, check_vma=False)
```

```python
import math

import jax
import jax.numpy as jnp
from jax import lax
from jax.experimental import pallas as pl
from jax.experimental.pallas import tpu as pltpu
from jax.sharding import PartitionSpec as P

MESH = pl.DeviceIdType.MESH
BF16, F32 = jnp.bfloat16, jnp.float32
NT = (((1,), (1,)), ((), ()))

N_DEV, N_CHIP, TOK, SEG = 8, 4, 128, 64
ROWS = 2 * TOK
SEQ = N_DEV * TOK
D = 3072
HD = 128
G = 3
BQ = 256
NB = SEQ // BQ
C = HD**-0.5
C2 = C * math.log2(math.e)
U_DO, U_K, U_V, U_Q = 0, 3, 4, 5
SLOTS = 12
RB = 128
ND = 3072
NV = 3072
VLIM = 66_000_000

scope = jax.named_scope


def dot_nt(a, b):
    return lax.dot_general(a, b, NT, preferred_element_type=F32)


def dot(a, b):
    return jnp.dot(a, b, preferred_element_type=F32)


def kernel(x_hbm, dy_hbm, wq_hbm, wk_hbm, wv_hbm, wo_hbm, out_ref,
           x_v, dy_v, wo_s, w_s, wq_r, wk_r, wv_r, sbuf, recv, obuf, rin, rkv, acc, pbuf,
           s0, s1, s2, s3, d0, d1, d2, d3, p0, p1, p2, p3, e0, e1, e2, e3, kt, vt, dk_acc, dv_acc,
           io_sem, wo_sem, w_sem, xs_sem, xr_sem, send_sem, recv_sem, osend_sem, orecv_sem, kv_sem, ps_sem, pr_sem):
    s_scr, dp_scr, p_scr, ds_scr = (s0, s1, s2, s3), (d0, d1, d2, d3), (p0, p1, p2, p3), (e0, e1, e2, e3)
    me = lax.axis_index("cp")
    dp = lax.axis_index("dp")
    chip = me // 2
    q = lax.rem(me, 2)
    partner = (dp, 2 * chip + 1 - q)

    def peer(k):
        return lax.rem(chip + k, N_CHIP)

    def dev_of(cc):
        return (dp, 2 * cc + q)

    barrier = pltpu.get_barrier_semaphore()
    pl.semaphore_signal(barrier, inc=1, device_id=partner, device_id_type=MESH)
    for k in range(1, N_CHIP):
        pl.semaphore_signal(barrier, inc=1, device_id=dev_of(peer(k)), device_id_type=MESH)

    def tok_rows(i):
        return pl.ds(pl.multiple_of(i * TOK, TOK), TOK)

    def chip_rows(i):
        return pl.ds(pl.multiple_of(i * ROWS, ROWS), ROWS)

    own, other = tok_rows(q), tok_rows(1 - q)

    def io_copy(n):
        src, dst = ((dy_hbm, dy_v), (x_hbm, x_v))[n]
        return pltpu.make_async_copy(src, dst.at[own], io_sem.at[n])

    def swap_copy(n):
        ref = (dy_v, x_v)[n]
        return pltpu.make_async_remote_copy(
            src_ref=ref.at[own], dst_ref=ref.at[own], send_sem=xs_sem.at[n], recv_sem=xr_sem.at[n],
            device_id=partner, device_id_type=MESH)

    def wo_copy(g, k):
        return pltpu.make_async_copy(wo_hbm.at[q, peer(k), g], wo_s.at[g % 2, k - 1], wo_sem.at[g % 2, k - 1])

    def wkv_copy(w_hbm, i, slot, half=None):
        half = q if half is None else half
        return pltpu.make_async_copy(w_hbm.at[i, :, :, half], w_s.at[slot], w_sem.at[slot])

    def wq_copy(i, slot):
        return pltpu.make_async_copy(wq_hbm.at[i, :, pl.ds(3 * q, 3)], w_s.at[slot], w_sem.at[slot])

    def wait_slot(slot):
        wkv_copy(wk_hbm, 0, slot).wait()

    io_copy(0).start()
    io_copy(1).start()
    for k in (1, 2):
        wo_copy(0, k).start()
    dk_acc[...] = jnp.zeros_like(dk_acc)
    dv_acc[...] = jnp.zeros_like(dv_acc)
    with scope('barrier'):
        pl.semaphore_wait(barrier, N_CHIP)
    for i in range(4):
        wkv_copy(wk_hbm, i, i).start()
    with scope('swapx'):
        io_copy(1).wait()
        swap_copy(1).start()
        io_copy(0).wait()

    def relay_kv(dst, base, i, slot):
        flat = w_s.at[slot].reshape(768 * 4, HD)
        for h in range(4):
            for r in range(0, 768, RB):
                dst[base + h, pl.ds(i * 768 + r, RB), :] = flat[pl.ds(4 * r + h, RB, stride=4), :]

    def relay_q(i, slot):
        flat = w_s.at[slot].reshape(768 * 4, HD)
        for h in range(12):
            for r in range(0, 256, RB):
                wq_r[h, pl.ds(i * 256 + r, RB), :] = flat[pl.ds(12 * r + h, RB, stride=12), :]


    def send_part(unit, k, val, rows, dst_rows):
        if k == N_CHIP:
            recv[unit, dst_rows, :] = val
            return
        sbuf[unit, k - 1, rows, :] = val
        pltpu.make_async_remote_copy(
            src_ref=sbuf.at[unit, k - 1, rows], dst_ref=recv.at[unit, dst_rows],
            send_sem=send_sem, recv_sem=recv_sem.at[unit],
            device_id=dev_of(peer(k)), device_id_type=MESH).start()

    def send_rows(unit, k, val, r):
        send_part(unit, k, val, tok_rows(r), tok_rows(2 * chip + r))

    def send_block(unit, k, val):
        send_part(unit, k, val, pl.ds(0, ROWS), chip_rows(chip))

    def do0_rows(r, ks):
        w = wo_s[0, pl.ds(ks[0] - 1, len(ks))].reshape(len(ks) * HD, D)
        val = dot_nt(dy_v[tok_rows(r), :], w).astype(BF16)
        for n, k in enumerate(ks):
            send_rows(U_DO, k, val[:, n * HD:(n + 1) * HD], r)

    def do_steps(g):
        for k in range(1, 5):
            wo_copy(g, k).wait()
        val = dot_nt(dy_v[...], wo_s[g % 2].reshape(4 * HD, D)).astype(BF16)
        for k in range(1, 5):
            send_block(U_DO + g, k, val[:, (k - 1) * HD:k * HD])

    def k_rows(r):
        w = jnp.concatenate([wk_r[4 * q + peer(k)] for k in range(1, 5)], axis=1)
        val = dot(x_v[tok_rows(r), :], w).astype(BF16)
        for k in range(1, 5):
            send_rows(U_K, k, val[:, (k - 1) * HD:k * HD], r)

    def v_steps():
        w = jnp.concatenate([wv_r[4 * q + peer(k)] for k in range(1, 5)], axis=1)
        val = dot(x_v[...], w).astype(BF16)
        for k in range(1, 5):
            send_block(U_V, k, val[:, (k - 1) * HD:k * HD])

    def q_steps(g):
        w = jnp.concatenate([wq_r[3 * peer(k) + g] for k in range(1, 5)], axis=1)
        val = dot(x_v[...], w).astype(BF16)
        for k in range(1, 5):
            send_block(U_Q + g, k, val[:, (k - 1) * HD:k * HD])

    with scope('do0a'):
        for k in (1, 2):
            wo_copy(0, k).wait()
        do0_rows(q, (1, 2))
    for i in range(4):
        wkv_copy(wv_hbm, i, 4 + i).start()
    swap_copy(0).start()
    with scope('relk'):
        for i in range(4):
            wait_slot(i)
            relay_kv(wk_r, 4 * q, i, i)
    for k in (3, 4):
        wo_copy(0, k).start()
    with scope('k_own'):
        k_rows(q)
    with scope('xswap'):
        swap_copy(1).wait_recv()
    with scope('k_other'):
        k_rows(1 - q)
    with scope('relv'):
        for i in range(4):
            wait_slot(4 + i)
            relay_kv(wv_r, 4 * q, i, 4 + i)
    for i in range(4):
        wq_copy(i, 8 + i).start()
    with scope('v'):
        v_steps()
    for i in range(4):
        wq_copy(4 + i, i).start()
    with scope('do0b'):
        for k in (3, 4):
            wo_copy(0, k).wait()
        do0_rows(q, (3, 4))
    for i in range(4):
        wq_copy(8 + i, 4 + i).start()
    with scope('dyswap'):
        swap_copy(0).wait_recv()
    with scope('do0c'):
        do0_rows(1 - q, (1, 2, 3, 4))
    for k in range(1, 5):
        wo_copy(1, k).start()
    with scope('relq'):
        for i in range(12):
            slot = (8 + i) % SLOTS
            wait_slot(slot)
            relay_q(i, slot)
    for k in range(1, 5):
        wo_copy(2, k).start()
    with scope('q0'):
        q_steps(0)
    for i in range(8):
        wkv_copy((wk_hbm, wv_hbm)[i // 4], i % 4, (8 + i) % SLOTS, 1 - q).start()
    for g in (1, 2):
        with scope('do12'):
            do_steps(g)
        with scope('q12'):
            q_steps(g)
    with scope('relkv2'):
        for i in range(4):
            wait_slot(8 + i)
            relay_kv(wk_r, 4 - 4 * q, i, 8 + i)
            wait_slot(i)
            relay_kv(wv_r, 4 - 4 * q, i, i)

    def wait_unit(u):
        part = recv.at[u, pl.ds(0, SEQ - ROWS)]
        pltpu.make_async_copy(part, part, recv_sem.at[u]).wait()

    with scope('waitkv'):
        wait_unit(U_K)
        wait_unit(U_V)
    def segs(b):
        out = []
        for seg in range(4 * b, 4 * b + 4):
            row = seg * TOK if seg < N_DEV else (2 * N_DEV - 1 - seg) * TOK + SEG
            out.append(slice(row, row + SEG))
        return out

    def pos_block(u, b):
        return jnp.concatenate([recv[u, r, :] for r in segs(b)], axis=0)

    def put_block(u, b, val):
        for n, r in enumerate(segs(b)):
            obuf[u, r, :] = val[n * SEG:(n + 1) * SEG]

    for b in range(NB):
        kt[:, b * BQ:(b + 1) * BQ] = pos_block(U_K, b).T
        vt[:, b * BQ:(b + 1) * BQ] = pos_block(U_V, b).T

    def send_out(u):
        slot = G * chip + u
        for k in range(1, N_CHIP):
            pltpu.make_async_remote_copy(
                src_ref=obuf.at[u, chip_rows(peer(k))], dst_ref=rin.at[slot],
                send_sem=osend_sem, recv_sem=orecv_sem.at[u],
                device_id=dev_of(peer(k)), device_id_type=MESH).start()
        rin[slot] = obuf[u, chip_rows(chip), :]

    def attn_head(g, _):
        with scope('waitq'):
            wait_unit(U_DO + g)
            wait_unit(U_Q + g)
        st = [{} for _ in range(NB)]

        def chunks(b):
            return [slice(k * BQ, (k + 1) * BQ) for k in range(b + 1)]

        def scores(b):
            qb = pos_block(U_Q + g, b)
            dob = pos_block(U_DO + g, b)
            mx = None
            for kc, ks in enumerate(chunks(b)):
                s = dot_nt(pos_block(U_K, kc), qb)
                if kc == b:
                    key = lax.broadcasted_iota(jnp.int32, (BQ, BQ), 0)
                    qry = lax.broadcasted_iota(jnp.int32, (BQ, BQ), 1)
                    s = jnp.where(key <= qry, s, -jnp.inf)
                s_scr[b][ks, :] = s
                mc = jnp.max(s.reshape(BQ // 8, 8, BQ), axis=0)
                mx = mc if mx is None else jnp.maximum(mx, mc)
            for kc, ks in enumerate(chunks(b)):
                dp_scr[b][ks, :] = dot_nt(pos_block(U_V, kc), dob)
            st[b]['m2'] = jnp.max(mx, axis=0, keepdims=True) * C2

        def probs(b):
            m2 = st[b]['m2']
            ls = None
            for ks in chunks(b):
                e = jnp.exp2(s_scr[b][ks, :] * C2 - m2)
                lc = jnp.sum(e.reshape(BQ // 8, 8, BQ), axis=0)
                ls = lc if ls is None else ls + lc
            lse2 = m2 + jnp.log2(jnp.sum(ls, axis=0, keepdims=True))
            for ks in chunks(b):
                p_scr[b][ks, :] = jnp.exp2(s_scr[b][ks, :] * C2 - lse2).astype(BF16)

        def outs(b):
            n = (b + 1) * BQ
            dob = pos_block(U_DO + g, b)
            ot = dot(vt[:, :n], p_scr[b][...]).astype(BF16)
            st[b]['delta'] = jnp.sum(dob.T.astype(F32) * ot.astype(F32), axis=0, keepdims=True)
            for ks in chunks(b):
                dv_acc[ks, :] += dot(p_scr[b][ks, :], dob)

        def dscores(b):
            delta = st[b]['delta']
            for ks in chunks(b):
                ds_scr[b][ks, :] = (p_scr[b][ks, :].astype(F32) * (dp_scr[b][ks, :] - delta)).astype(BF16)

        def grads(b):
            n = (b + 1) * BQ
            qb = pos_block(U_Q + g, b)
            for ks in chunks(b):
                dk_acc[ks, :] += dot(ds_scr[b][ks, :], qb)
            dqt = (dot(kt[:, :n], ds_scr[b][...]) * C).astype(BF16)
            put_block(g, b, dqt.T)

        with scope('attn'):
            scores(3)
            scores(2)
            probs(3)
            outs(3)
            scores(1)
            dscores(3)
            probs(2)
            grads(3)
            outs(2)
            scores(0)
            dscores(2)
            probs(1)
            grads(2)
            outs(1)
            dscores(1)
            probs(0)
            grads(1)
            outs(0)
            dscores(0)
            grads(0)

        with scope('send'):
            send_out(g)
        return 0

    lax.fori_loop(0, G, attn_head, 0)
    def send_owners(n):
        slot = 8 * n + 4 * q + chip

        def send_dev(dev, part):
            pltpu.make_async_remote_copy(
                src_ref=obuf.at[G + n, tok_rows(dev)], dst_ref=rkv.at[slot],
                send_sem=osend_sem, recv_sem=kv_sem.at[n, part],
                device_id=(dp, dev), device_id_type=MESH).start()

        send_dev(partner[1], 0)
        for k in range(1, N_CHIP):
            for r in range(2):
                send_dev(2 * peer(k) + r, k if n == 1 else 1)
        rkv[slot] = obuf[G + n, tok_rows(me), :]

    with scope('senddkv'):
        for b in range(NB):
            put_block(3, b, (dk_acc[b * BQ:(b + 1) * BQ, :] * C).astype(BF16))
        send_owners(0)
        for b in range(NB):
            put_block(4, b, dv_acc[b * BQ:(b + 1) * BQ, :].astype(BF16))
        send_owners(1)

    def p_copy():
        return pltpu.make_async_remote_copy(
            src_ref=acc.at[other], dst_ref=pbuf, send_sem=ps_sem, recv_sem=pr_sem,
            device_id=partner, device_id_type=MESH)

    def wait_kv(n, part, count):
        ref = obuf.at[0, pl.ds(0, count * TOK)]
        pltpu.make_async_copy(ref, ref, kv_sem.at[n, part]).wait()

    def kv_dx(items, last=False):
        lhs, rhs = [], []
        for n, k in items:
            c = lax.rem(chip + N_CHIP - k, N_CHIP)
            for r in range(2):
                lhs.append(rkv[8 * n + 4 * r + c])
                rhs.append((wk_r, wv_r)[n][4 * r + c])
        t = dot_nt(jnp.concatenate(lhs, axis=1), jnp.concatenate(rhs, axis=1)) + acc[own, :]
        if last:
            out_ref[...] = (t + pbuf[...]).astype(BF16)
        else:
            acc[own, :] = t

    for u in range(G):
        with scope('waito'):
            part = obuf.at[u, pl.ds(0, SEQ - ROWS)]
            pltpu.make_async_copy(part, part, orecv_sem.at[u]).wait()
        with scope('dx'):
            t = dot_nt(jnp.concatenate([rin[G * j + u] for j in range(N_CHIP)], axis=1),
                       jnp.concatenate([wq_r[G * j + u] for j in range(N_CHIP)], axis=1))
            acc[...] = t if u == 0 else t + acc[...]
        if u == 0:
            with scope('kvlocal'):
                wait_kv(0, 0, 1)
                wait_kv(1, 0, 1)
                kv_dx([(0, 0), (1, 0)])
    p_copy().start()

    with scope('waitk'):
        wait_kv(0, 1, 6)
    with scope('kdx'):
        kv_dx([(0, 1), (0, 2), (0, 3)])
    for k in (1, 2):
        with scope('waitv%d' % k):
            wait_kv(1, k, 2)
        with scope('vdx%d' % k):
            kv_dx([(1, k)])
    with scope('waitv3'):
        wait_kv(1, 3, 2)
    with scope('waitp'):
        p_copy().wait_recv()
    with scope('vdx3'):
        kv_dx([(1, 3)], last=True)

    with scope('final'):
        for n in range(2):
            swap_copy(n).wait_send()
        p_copy().wait_send()
        pltpu.make_async_copy(sbuf, sbuf, send_sem).wait()
        part = obuf.at[pl.ds(0, G), pl.ds(0, SEQ - ROWS)]
        pltpu.make_async_copy(part, part, osend_sem).wait()
        part = obuf.at[pl.ds(0, 2), pl.ds(0, SEQ - TOK)]
        pltpu.make_async_copy(part, part, osend_sem).wait()


def solution(mesh):
    row_spec = P(("dp", "cp"), None)

    def device_fn(x_in, d_y, w_q, w_k, w_v, w_o):
        dma = pltpu.SemaphoreType.DMA
        res = pl.pallas_call(
            kernel,
            out_shape=pltpu.VMEM((TOK, D), BF16),
            in_specs=[pl.BlockSpec(memory_space=pl.ANY)] * 6,
            out_specs=pl.BlockSpec(memory_space=pltpu.VMEM),
            scratch_shapes=[
                pltpu.VMEM((ROWS, D), BF16),
                pltpu.VMEM((ROWS, D), BF16),
                pltpu.VMEM((2, N_CHIP, HD, D), BF16),
                pltpu.VMEM((SLOTS, 256, 3, 4, HD), BF16),
                pltpu.VMEM((12, D, HD), BF16),
                pltpu.VMEM((8, D, HD), BF16),
                pltpu.VMEM((8, D, HD), BF16),
                pltpu.VMEM((8, 3, ROWS, HD), BF16),
                pltpu.VMEM((8, SEQ, HD), BF16),
                pltpu.VMEM((5, SEQ, HD), BF16),
                pltpu.VMEM((12, ROWS, HD), BF16),
                pltpu.VMEM((16, TOK, HD), BF16),
                pltpu.VMEM((ROWS, D), F32),
                pltpu.VMEM((TOK, D), F32),
                *[pltpu.VMEM(((b + 1) * BQ, BQ), t) for t in (F32, F32, BF16, BF16) for b in range(NB)],
                pltpu.VMEM((HD, SEQ), BF16),
                pltpu.VMEM((HD, SEQ), BF16),
                pltpu.VMEM((SEQ, HD), F32),
                pltpu.VMEM((SEQ, HD), F32),
                dma((2,)), dma((2, N_CHIP)), dma((SLOTS,)), dma((2,)), dma((2,)),
                dma, dma((8,)), dma, dma((G,)), dma((2, 4)), dma, dma,
            ],
            compiler_params=pltpu.CompilerParams(
                collective_id=0, has_side_effects=True, vmem_limit_bytes=VLIM),
        )(x_in, d_y, w_q.reshape(12, 256, 6, 4, HD), w_k.reshape(4, 256, 3, 2, 4, HD), w_v.reshape(4, 256, 3, 2, 4, HD),
          w_o.reshape(2, N_CHIP, G, HD, D))
        return res

    return jax.shard_map(device_fn, mesh=mesh, in_specs=(row_spec, row_spec, P(), P(), P(), P()),
                         out_specs=row_spec, check_vma=False)
```

```python
import math

import jax
import jax.numpy as jnp
from jax import lax
from jax.experimental import pallas as pl
from jax.experimental.pallas import tpu as pltpu
from jax.sharding import PartitionSpec as P

MESH = pl.DeviceIdType.MESH
BF16, F32 = jnp.bfloat16, jnp.float32
NT = (((1,), (1,)), ((), ()))

N_DEV, N_CHIP, TOK, SEG = 8, 4, 128, 64
ROWS = 2 * TOK
SEQ = N_DEV * TOK
D = 3072
HD = 128
G = 3
BQ = 256
NB = SEQ // BQ
C = HD**-0.5
C2 = C * math.log2(math.e)
U_DO, U_K, U_V, U_Q = 0, 3, 4, 5
SLOTS = 12
RB = 128
ND = 3072
NV = 3072
VLIM = 66_000_000

scope = jax.named_scope


def dot_nt(a, b):
    return lax.dot_general(a, b, NT, preferred_element_type=F32)


def dot(a, b):
    return jnp.dot(a, b, preferred_element_type=F32)


def kernel(x_hbm, dy_hbm, wq_hbm, wk_hbm, wv_hbm, wo_hbm, out_ref,
           x_v, dy_v, wo_s, w_s, wq_r, wk_r, wv_r, sbuf, recv, obuf, rin, rkv, acc, pbuf,
           s0, s1, s2, s3, d0, d1, d2, d3, p0, p1, p2, p3, e0, e1, e2, e3, kt, vt, dk_acc, dv_acc,
           io_sem, wo_sem, w_sem, xs_sem, xr_sem, send_sem, recv_sem, osend_sem, orecv_sem, kv_sem, ps_sem, pr_sem):
    s_scr, dp_scr, p_scr, ds_scr = (s0, s1, s2, s3), (d0, d1, d2, d3), (p0, p1, p2, p3), (e0, e1, e2, e3)
    me = lax.axis_index("cp")
    dp = lax.axis_index("dp")
    chip = me // 2
    q = lax.rem(me, 2)
    partner = (dp, 2 * chip + 1 - q)

    def peer(k):
        return lax.rem(chip + k, N_CHIP)

    def dev_of(cc):
        return (dp, 2 * cc + q)

    barrier = pltpu.get_barrier_semaphore()
    pl.semaphore_signal(barrier, inc=1, device_id=partner, device_id_type=MESH)
    for k in range(1, N_CHIP):
        pl.semaphore_signal(barrier, inc=1, device_id=dev_of(peer(k)), device_id_type=MESH)

    def tok_rows(i):
        return pl.ds(pl.multiple_of(i * TOK, TOK), TOK)

    def chip_rows(i):
        return pl.ds(pl.multiple_of(i * ROWS, ROWS), ROWS)

    own, other = tok_rows(q), tok_rows(1 - q)

    def io_copy(n):
        src, dst = ((dy_hbm, dy_v), (x_hbm, x_v))[n]
        return pltpu.make_async_copy(src, dst.at[own], io_sem.at[n])

    def swap_copy(n):
        ref = (dy_v, x_v)[n]
        return pltpu.make_async_remote_copy(
            src_ref=ref.at[own], dst_ref=ref.at[own], send_sem=xs_sem.at[n], recv_sem=xr_sem.at[n],
            device_id=partner, device_id_type=MESH)

    def wo_copy(g, k):
        return pltpu.make_async_copy(wo_hbm.at[q, peer(k), g], wo_s.at[g % 2, k - 1], wo_sem.at[g % 2, k - 1])

    def wkv_copy(w_hbm, i, slot, half=None):
        half = q if half is None else half
        return pltpu.make_async_copy(w_hbm.at[i, :, :, half], w_s.at[slot], w_sem.at[slot])

    def wq_copy(i, slot):
        return pltpu.make_async_copy(wq_hbm.at[i, :, pl.ds(3 * q, 3)], w_s.at[slot], w_sem.at[slot])

    def wait_slot(slot):
        wkv_copy(wk_hbm, 0, slot).wait()

    io_copy(0).start()
    io_copy(1).start()
    for k in (1, 2):
        wo_copy(0, k).start()
    dk_acc[...] = jnp.zeros_like(dk_acc)
    dv_acc[...] = jnp.zeros_like(dv_acc)
    with scope('barrier'):
        pl.semaphore_wait(barrier, N_CHIP)
    wo_copy(0, 3).start()
    for i in range(4):
        wkv_copy(wk_hbm, i, i).start()
    with scope('swapx'):
        io_copy(1).wait()
        swap_copy(1).start()
        io_copy(0).wait()

    def relay_kv(dst, base, i, slot):
        flat = w_s.at[slot].reshape(768 * 4, HD)
        for h in range(4):
            for r in range(0, 768, RB):
                dst[base + h, pl.ds(i * 768 + r, RB), :] = flat[pl.ds(4 * r + h, RB, stride=4), :]

    def relay_q(i, slot):
        flat = w_s.at[slot].reshape(768 * 4, HD)
        for h in range(12):
            for r in range(0, 256, RB):
                wq_r[h, pl.ds(i * 256 + r, RB), :] = flat[pl.ds(12 * r + h, RB, stride=12), :]


    def send_part(unit, k, val, rows, dst_rows):
        if k == N_CHIP:
            recv[unit, dst_rows, :] = val
            return
        sbuf[unit, k - 1, rows, :] = val
        pltpu.make_async_remote_copy(
            src_ref=sbuf.at[unit, k - 1, rows], dst_ref=recv.at[unit, dst_rows],
            send_sem=send_sem, recv_sem=recv_sem.at[unit],
            device_id=dev_of(peer(k)), device_id_type=MESH).start()

    def send_rows(unit, k, val, r):
        send_part(unit, k, val, tok_rows(r), tok_rows(2 * chip + r))

    def send_block(unit, k, val):
        send_part(unit, k, val, pl.ds(0, ROWS), chip_rows(chip))

    def do0_rows(r, ks):
        w = wo_s[0, pl.ds(ks[0] - 1, len(ks))].reshape(len(ks) * HD, D)
        val = dot_nt(dy_v[tok_rows(r), :], w).astype(BF16)
        for n, k in enumerate(ks):
            send_rows(U_DO, k, val[:, n * HD:(n + 1) * HD], r)

    def do_steps(g):
        for k in range(1, 5):
            wo_copy(g, k).wait()
        val = dot_nt(dy_v[...], wo_s[g % 2].reshape(4 * HD, D)).astype(BF16)
        for k in range(1, 5):
            send_block(U_DO + g, k, val[:, (k - 1) * HD:k * HD])

    def k_rows(r):
        w = jnp.concatenate([wk_r[4 * q + peer(k)] for k in range(1, 5)], axis=1)
        val = dot(x_v[tok_rows(r), :], w).astype(BF16)
        for k in range(1, 5):
            send_rows(U_K, k, val[:, (k - 1) * HD:k * HD], r)

    def v_steps():
        w = jnp.concatenate([wv_r[4 * q + peer(k)] for k in range(1, 5)], axis=1)
        val = dot(x_v[...], w).astype(BF16)
        for k in range(1, 5):
            send_block(U_V, k, val[:, (k - 1) * HD:k * HD])

    def q_steps(g):
        w = jnp.concatenate([wq_r[3 * peer(k) + g] for k in range(1, 5)], axis=1)
        val = dot(x_v[...], w).astype(BF16)
        for k in range(1, 5):
            send_block(U_Q + g, k, val[:, (k - 1) * HD:k * HD])

    with scope('do0a'):
        for k in (1, 2):
            wo_copy(0, k).wait()
        do0_rows(q, (1, 2))
    swap_copy(0).start()
    for i in range(4):
        wkv_copy(wv_hbm, i, 4 + i).start()
    with scope('do0a3'):
        wo_copy(0, 3).wait()
        do0_rows(q, (3,))
    with scope('relk'):
        for i in range(4):
            wait_slot(i)
            relay_kv(wk_r, 4 * q, i, i)
    wo_copy(0, 4).start()
    with scope('k_own'):
        k_rows(q)
    with scope('xswap'):
        swap_copy(1).wait_recv()
    with scope('k_other'):
        k_rows(1 - q)
    with scope('relv'):
        for i in range(4):
            wait_slot(4 + i)
            relay_kv(wv_r, 4 * q, i, 4 + i)
    for i in range(4):
        wq_copy(i, 8 + i).start()
    with scope('v'):
        v_steps()
    for i in range(4):
        wq_copy(4 + i, i).start()
    with scope('do0b'):
        wo_copy(0, 4).wait()
        do0_rows(q, (4,))
    for i in range(4):
        wq_copy(8 + i, 4 + i).start()
    with scope('dyswap'):
        swap_copy(0).wait_recv()
    with scope('do0c'):
        do0_rows(1 - q, (1, 2, 3, 4))
    for k in range(1, 5):
        wo_copy(1, k).start()
    with scope('relq'):
        for i in range(12):
            slot = (8 + i) % SLOTS
            wait_slot(slot)
            relay_q(i, slot)
    for k in range(1, 5):
        wo_copy(2, k).start()
    with scope('q0'):
        q_steps(0)
    for i in range(8):
        wkv_copy((wk_hbm, wv_hbm)[i // 4], i % 4, (8 + i) % SLOTS, 1 - q).start()
    for g in (1, 2):
        with scope('do12'):
            do_steps(g)
        with scope('q12'):
            q_steps(g)
    with scope('relkv2'):
        for i in range(4):
            wait_slot(8 + i)
            relay_kv(wk_r, 4 - 4 * q, i, 8 + i)
            wait_slot(i)
            relay_kv(wv_r, 4 - 4 * q, i, i)

    def wait_unit(u):
        part = recv.at[u, pl.ds(0, SEQ - ROWS)]
        pltpu.make_async_copy(part, part, recv_sem.at[u]).wait()

    with scope('waitkv'):
        wait_unit(U_K)
        wait_unit(U_V)
    def segs(b):
        out = []
        for seg in range(4 * b, 4 * b + 4):
            row = seg * TOK if seg < N_DEV else (2 * N_DEV - 1 - seg) * TOK + SEG
            out.append(slice(row, row + SEG))
        return out

    def pos_block(u, b):
        return jnp.concatenate([recv[u, r, :] for r in segs(b)], axis=0)

    def put_block(u, b, val):
        for n, r in enumerate(segs(b)):
            obuf[u, r, :] = val[n * SEG:(n + 1) * SEG]

    for b in range(NB):
        kt[:, b * BQ:(b + 1) * BQ] = pos_block(U_K, b).T
        vt[:, b * BQ:(b + 1) * BQ] = pos_block(U_V, b).T

    def send_out(u):
        slot = G * chip + u
        for k in range(1, N_CHIP):
            pltpu.make_async_remote_copy(
                src_ref=obuf.at[u, chip_rows(peer(k))], dst_ref=rin.at[slot],
                send_sem=osend_sem, recv_sem=orecv_sem.at[u],
                device_id=dev_of(peer(k)), device_id_type=MESH).start()
        rin[slot] = obuf[u, chip_rows(chip), :]

    def attn_head(g, _):
        with scope('waitq'):
            wait_unit(U_DO + g)
            wait_unit(U_Q + g)
        st = [{} for _ in range(NB)]

        def chunks(b):
            return [slice(k * BQ, (k + 1) * BQ) for k in range(b + 1)]

        def scores(b):
            qb = pos_block(U_Q + g, b)
            dob = pos_block(U_DO + g, b)
            mx = None
            for kc, ks in enumerate(chunks(b)):
                s = dot_nt(pos_block(U_K, kc), qb)
                if kc == b:
                    key = lax.broadcasted_iota(jnp.int32, (BQ, BQ), 0)
                    qry = lax.broadcasted_iota(jnp.int32, (BQ, BQ), 1)
                    s = jnp.where(key <= qry, s, -jnp.inf)
                s_scr[b][ks, :] = s
                mc = jnp.max(s.reshape(BQ // 8, 8, BQ), axis=0)
                mx = mc if mx is None else jnp.maximum(mx, mc)
            for kc, ks in enumerate(chunks(b)):
                dp_scr[b][ks, :] = dot_nt(pos_block(U_V, kc), dob)
            st[b]['m2'] = jnp.max(mx, axis=0, keepdims=True) * C2

        def probs(b):
            m2 = st[b]['m2']
            ls = None
            for ks in chunks(b):
                e = jnp.exp2(s_scr[b][ks, :] * C2 - m2)
                lc = jnp.sum(e.reshape(BQ // 8, 8, BQ), axis=0)
                ls = lc if ls is None else ls + lc
            lse2 = m2 + jnp.log2(jnp.sum(ls, axis=0, keepdims=True))
            for ks in chunks(b):
                p_scr[b][ks, :] = jnp.exp2(s_scr[b][ks, :] * C2 - lse2).astype(BF16)

        def outs(b):
            n = (b + 1) * BQ
            dob = pos_block(U_DO + g, b)
            ot = dot(vt[:, :n], p_scr[b][...]).astype(BF16)
            st[b]['delta'] = jnp.sum(dob.T.astype(F32) * ot.astype(F32), axis=0, keepdims=True)
            for ks in chunks(b):
                dv_acc[ks, :] += dot(p_scr[b][ks, :], dob)

        def dscores(b):
            delta = st[b]['delta']
            for ks in chunks(b):
                ds_scr[b][ks, :] = (p_scr[b][ks, :].astype(F32) * (dp_scr[b][ks, :] - delta)).astype(BF16)

        def grads(b):
            n = (b + 1) * BQ
            qb = pos_block(U_Q + g, b)
            for ks in chunks(b):
                dk_acc[ks, :] += dot(ds_scr[b][ks, :], qb)
            dqt = (dot(kt[:, :n], ds_scr[b][...]) * C).astype(BF16)
            put_block(g, b, dqt.T)

        with scope('attn'):
            scores(3)
            scores(2)
            probs(3)
            outs(3)
            scores(1)
            dscores(3)
            probs(2)
            grads(3)
            outs(2)
            scores(0)
            dscores(2)
            probs(1)
            grads(2)
            outs(1)
            dscores(1)
            probs(0)
            grads(1)
            outs(0)
            dscores(0)
            grads(0)

        with scope('send'):
            send_out(g)
        return 0

    lax.fori_loop(0, G, attn_head, 0)
    def send_owners(n):
        slot = 8 * n + 4 * q + chip

        def send_dev(dev, part):
            pltpu.make_async_remote_copy(
                src_ref=obuf.at[G + n, tok_rows(dev)], dst_ref=rkv.at[slot],
                send_sem=osend_sem, recv_sem=kv_sem.at[n, part],
                device_id=(dp, dev), device_id_type=MESH).start()

        send_dev(partner[1], 0)
        for k in range(1, N_CHIP):
            for r in range(2):
                send_dev(2 * peer(k) + r, k if n == 1 else 1)
        rkv[slot] = obuf[G + n, tok_rows(me), :]

    with scope('senddkv'):
        for b in range(NB):
            put_block(3, b, (dk_acc[b * BQ:(b + 1) * BQ, :] * C).astype(BF16))
        send_owners(0)
        for b in range(NB):
            put_block(4, b, dv_acc[b * BQ:(b + 1) * BQ, :].astype(BF16))
        send_owners(1)

    def p_copy():
        return pltpu.make_async_remote_copy(
            src_ref=acc.at[other], dst_ref=pbuf, send_sem=ps_sem, recv_sem=pr_sem,
            device_id=partner, device_id_type=MESH)

    def wait_kv(n, part, count):
        ref = obuf.at[0, pl.ds(0, count * TOK)]
        pltpu.make_async_copy(ref, ref, kv_sem.at[n, part]).wait()

    def kv_dx(items, last=False):
        lhs, rhs = [], []
        for n, k in items:
            c = lax.rem(chip + N_CHIP - k, N_CHIP)
            for r in range(2):
                lhs.append(rkv[8 * n + 4 * r + c])
                rhs.append((wk_r, wv_r)[n][4 * r + c])
        t = dot_nt(jnp.concatenate(lhs, axis=1), jnp.concatenate(rhs, axis=1)) + acc[own, :]
        if last:
            out_ref[...] = (t + pbuf[...]).astype(BF16)
        else:
            acc[own, :] = t

    for u in range(G):
        with scope('waito'):
            part = obuf.at[u, pl.ds(0, SEQ - ROWS)]
            pltpu.make_async_copy(part, part, orecv_sem.at[u]).wait()
        with scope('dx'):
            t = dot_nt(jnp.concatenate([rin[G * j + u] for j in range(N_CHIP)], axis=1),
                       jnp.concatenate([wq_r[G * j + u] for j in range(N_CHIP)], axis=1))
            acc[...] = t if u == 0 else t + acc[...]
        if u == 0:
            with scope('kvlocal'):
                wait_kv(0, 0, 1)
                wait_kv(1, 0, 1)
                kv_dx([(0, 0), (1, 0)])
    p_copy().start()

    with scope('waitk'):
        wait_kv(0, 1, 6)
    with scope('kdx'):
        kv_dx([(0, 1), (0, 2), (0, 3)])
    for k in (1, 2):
        with scope('waitv%d' % k):
            wait_kv(1, k, 2)
        with scope('vdx%d' % k):
            kv_dx([(1, k)])
    with scope('waitv3'):
        wait_kv(1, 3, 2)
    with scope('waitp'):
        p_copy().wait_recv()
    with scope('vdx3'):
        kv_dx([(1, 3)], last=True)

    with scope('final'):
        for n in range(2):
            swap_copy(n).wait_send()
        p_copy().wait_send()
        pltpu.make_async_copy(sbuf, sbuf, send_sem).wait()
        part = obuf.at[pl.ds(0, G), pl.ds(0, SEQ - ROWS)]
        pltpu.make_async_copy(part, part, osend_sem).wait()
        part = obuf.at[pl.ds(0, 2), pl.ds(0, SEQ - TOK)]
        pltpu.make_async_copy(part, part, osend_sem).wait()


def solution(mesh):
    row_spec = P(("dp", "cp"), None)

    def device_fn(x_in, d_y, w_q, w_k, w_v, w_o):
        dma = pltpu.SemaphoreType.DMA
        res = pl.pallas_call(
            kernel,
            out_shape=pltpu.VMEM((TOK, D), BF16),
            in_specs=[pl.BlockSpec(memory_space=pl.ANY)] * 6,
            out_specs=pl.BlockSpec(memory_space=pltpu.VMEM),
            scratch_shapes=[
                pltpu.VMEM((ROWS, D), BF16),
                pltpu.VMEM((ROWS, D), BF16),
                pltpu.VMEM((2, N_CHIP, HD, D), BF16),
                pltpu.VMEM((SLOTS, 256, 3, 4, HD), BF16),
                pltpu.VMEM((12, D, HD), BF16),
                pltpu.VMEM((8, D, HD), BF16),
                pltpu.VMEM((8, D, HD), BF16),
                pltpu.VMEM((8, 3, ROWS, HD), BF16),
                pltpu.VMEM((8, SEQ, HD), BF16),
                pltpu.VMEM((5, SEQ, HD), BF16),
                pltpu.VMEM((12, ROWS, HD), BF16),
                pltpu.VMEM((16, TOK, HD), BF16),
                pltpu.VMEM((ROWS, D), F32),
                pltpu.VMEM((TOK, D), F32),
                *[pltpu.VMEM(((b + 1) * BQ, BQ), t) for t in (F32, F32, BF16, BF16) for b in range(NB)],
                pltpu.VMEM((HD, SEQ), BF16),
                pltpu.VMEM((HD, SEQ), BF16),
                pltpu.VMEM((SEQ, HD), F32),
                pltpu.VMEM((SEQ, HD), F32),
                dma((2,)), dma((2, N_CHIP)), dma((SLOTS,)), dma((2,)), dma((2,)),
                dma, dma((8,)), dma, dma((G,)), dma((2, 4)), dma, dma,
            ],
            compiler_params=pltpu.CompilerParams(
                collective_id=0, has_side_effects=True, vmem_limit_bytes=VLIM),
        )(x_in, d_y, w_q.reshape(12, 256, 6, 4, HD), w_k.reshape(4, 256, 3, 2, 4, HD), w_v.reshape(4, 256, 3, 2, 4, HD),
          w_o.reshape(2, N_CHIP, G, HD, D))
        return res

    return jax.shard_map(device_fn, mesh=mesh, in_specs=(row_spec, row_spec, P(), P(), P(), P()),
                         out_specs=row_spec, check_vma=False)
```

```python
import math

import jax
import jax.numpy as jnp
from jax import lax
from jax.experimental import pallas as pl
from jax.experimental.pallas import tpu as pltpu
from jax.sharding import PartitionSpec as P

MESH = pl.DeviceIdType.MESH
BF16, F32 = jnp.bfloat16, jnp.float32
NT = (((1,), (1,)), ((), ()))

N_DEV, N_CHIP, TOK, SEG = 8, 4, 128, 64
ROWS = 2 * TOK
SEQ = N_DEV * TOK
D = 3072
HD = 128
G = 3
BQ = 256
NB = SEQ // BQ
C = HD**-0.5
C2 = C * math.log2(math.e)
U_DO, U_K, U_V, U_Q = 0, 3, 4, 5
SLOTS = 12
RB = 128
ND = 3072
NV = 3072
VLIM = 66_000_000

scope = jax.named_scope


def dot_nt(a, b):
    return lax.dot_general(a, b, NT, preferred_element_type=F32)


def dot(a, b):
    return jnp.dot(a, b, preferred_element_type=F32)


def kernel(x_hbm, dy_hbm, wq_hbm, wk_hbm, wv_hbm, wo_hbm, out_ref,
           x_v, dy_v, wo_s, w_s, wq_r, wk_r, wv_r, sbuf, recv, obuf, rin, rkv, acc, pbuf,
           s0, s1, s2, s3, d0, d1, d2, d3, p0, p1, p2, p3, e0, e1, e2, e3, kt, vt, dk_acc, dv_acc,
           io_sem, wo_sem, w_sem, xs_sem, xr_sem, send_sem, recv_sem, osend_sem, orecv_sem, kv_sem, ps_sem, pr_sem):
    s_scr, dp_scr, p_scr, ds_scr = (s0, s1, s2, s3), (d0, d1, d2, d3), (p0, p1, p2, p3), (e0, e1, e2, e3)
    me = lax.axis_index("cp")
    dp = lax.axis_index("dp")
    chip = me // 2
    q = lax.rem(me, 2)
    partner = (dp, 2 * chip + 1 - q)

    def peer(k):
        return lax.rem(chip + k, N_CHIP)

    def dev_of(cc):
        return (dp, 2 * cc + q)

    barrier = pltpu.get_barrier_semaphore()
    pl.semaphore_signal(barrier, inc=1, device_id=partner, device_id_type=MESH)
    for k in range(1, N_CHIP):
        pl.semaphore_signal(barrier, inc=1, device_id=dev_of(peer(k)), device_id_type=MESH)

    def tok_rows(i):
        return pl.ds(pl.multiple_of(i * TOK, TOK), TOK)

    def chip_rows(i):
        return pl.ds(pl.multiple_of(i * ROWS, ROWS), ROWS)

    own, other = tok_rows(q), tok_rows(1 - q)

    def io_copy(n):
        src, dst = ((dy_hbm, dy_v), (x_hbm, x_v))[n]
        return pltpu.make_async_copy(src, dst.at[own], io_sem.at[n])

    def swap_copy(n):
        ref = (dy_v, x_v)[n]
        return pltpu.make_async_remote_copy(
            src_ref=ref.at[own], dst_ref=ref.at[own], send_sem=xs_sem.at[n], recv_sem=xr_sem.at[n],
            device_id=partner, device_id_type=MESH)

    def wo_copy(g, k):
        return pltpu.make_async_copy(wo_hbm.at[q, peer(k), g], wo_s.at[g % 2, k - 1], wo_sem.at[g % 2, k - 1])

    def wkv_copy(w_hbm, i, slot, half=None):
        half = q if half is None else half
        return pltpu.make_async_copy(w_hbm.at[i, :, :, half], w_s.at[slot], w_sem.at[slot])

    def wq_copy(i, slot):
        return pltpu.make_async_copy(wq_hbm.at[i, :, pl.ds(3 * q, 3)], w_s.at[slot], w_sem.at[slot])

    def wait_slot(slot):
        wkv_copy(wk_hbm, 0, slot).wait()

    io_copy(0).start()
    io_copy(1).start()
    for k in (1, 2):
        wo_copy(0, k).start()
    dk_acc[...] = jnp.zeros_like(dk_acc)
    dv_acc[...] = jnp.zeros_like(dv_acc)
    with scope('barrier'):
        pl.semaphore_wait(barrier, N_CHIP)
    for i in range(4):
        wkv_copy(wk_hbm, i, i).start()
    with scope('swapx'):
        io_copy(1).wait()
        swap_copy(1).start()
        io_copy(0).wait()

    def relay_kv(dst, base, i, slot):
        flat = w_s.at[slot].reshape(768 * 4, HD)
        for h in range(4):
            for r in range(0, 768, RB):
                dst[base + h, pl.ds(i * 768 + r, RB), :] = flat[pl.ds(4 * r + h, RB, stride=4), :]

    def relay_q(i, slot):
        flat = w_s.at[slot].reshape(768 * 4, HD)
        for h in range(12):
            for r in range(0, 256, RB):
                wq_r[h, pl.ds(i * 256 + r, RB), :] = flat[pl.ds(12 * r + h, RB, stride=12), :]


    def send_part(unit, k, val, rows, dst_rows):
        if k == N_CHIP:
            recv[unit, dst_rows, :] = val
            return
        sbuf[unit, k - 1, rows, :] = val
        pltpu.make_async_remote_copy(
            src_ref=sbuf.at[unit, k - 1, rows], dst_ref=recv.at[unit, dst_rows],
            send_sem=send_sem, recv_sem=recv_sem.at[unit],
            device_id=dev_of(peer(k)), device_id_type=MESH).start()

    def send_rows(unit, k, val, r):
        send_part(unit, k, val, tok_rows(r), tok_rows(2 * chip + r))

    def send_block(unit, k, val):
        send_part(unit, k, val, pl.ds(0, ROWS), chip_rows(chip))

    def do0_rows(r, ks):
        w = wo_s[0, pl.ds(ks[0] - 1, len(ks))].reshape(len(ks) * HD, D)
        val = dot_nt(dy_v[tok_rows(r), :], w).astype(BF16)
        for n, k in enumerate(ks):
            send_rows(U_DO, k, val[:, n * HD:(n + 1) * HD], r)

    def do_steps(g):
        for k in range(1, 5):
            wo_copy(g, k).wait()
        val = dot_nt(dy_v[...], wo_s[g % 2].reshape(4 * HD, D)).astype(BF16)
        for k in range(1, 5):
            send_block(U_DO + g, k, val[:, (k - 1) * HD:k * HD])

    def k_rows(r):
        w = jnp.concatenate([wk_r[4 * q + peer(k)] for k in range(1, 5)], axis=1)
        val = dot(x_v[tok_rows(r), :], w).astype(BF16)
        for k in range(1, 5):
            send_rows(U_K, k, val[:, (k - 1) * HD:k * HD], r)

    def v_steps():
        w = jnp.concatenate([wv_r[4 * q + peer(k)] for k in range(1, 5)], axis=1)
        val = dot(x_v[...], w).astype(BF16)
        for k in range(1, 5):
            send_block(U_V, k, val[:, (k - 1) * HD:k * HD])

    def q_steps(g):
        w = jnp.concatenate([wq_r[3 * peer(k) + g] for k in range(1, 5)], axis=1)
        val = dot(x_v[...], w).astype(BF16)
        for k in range(1, 5):
            send_block(U_Q + g, k, val[:, (k - 1) * HD:k * HD])

    with scope('do0a'):
        for k in (1, 2):
            wo_copy(0, k).wait()
        do0_rows(q, (1, 2))
    with scope('relk'):
        for i in range(4):
            wait_slot(i)
            relay_kv(wk_r, 4 * q, i, i)
    for i in range(4):
        wkv_copy(wv_hbm, i, 4 + i).start()
    with scope('k_own'):
        k_rows(q)
    for k in (3, 4):
        wo_copy(0, k).start()
    swap_copy(0).start()
    with scope('xswap'):
        swap_copy(1).wait_recv()
    with scope('k_other'):
        k_rows(1 - q)
    with scope('relv'):
        for i in range(4):
            wait_slot(4 + i)
            relay_kv(wv_r, 4 * q, i, 4 + i)
    for i in range(4):
        wq_copy(i, 8 + i).start()
    with scope('v'):
        v_steps()
    for i in range(4):
        wq_copy(4 + i, i).start()
    with scope('do0b'):
        for k in (3, 4):
            wo_copy(0, k).wait()
        do0_rows(q, (3, 4))
    for i in range(4):
        wq_copy(8 + i, 4 + i).start()
    with scope('dyswap'):
        swap_copy(0).wait_recv()
    with scope('do0c'):
        do0_rows(1 - q, (1, 2, 3, 4))
    for k in range(1, 5):
        wo_copy(1, k).start()
    with scope('relq'):
        for i in range(12):
            slot = (8 + i) % SLOTS
            wait_slot(slot)
            relay_q(i, slot)
    for k in range(1, 5):
        wo_copy(2, k).start()
    with scope('q0'):
        q_steps(0)
    for i in range(8):
        wkv_copy((wk_hbm, wv_hbm)[i // 4], i % 4, (8 + i) % SLOTS, 1 - q).start()
    for g in (1, 2):
        with scope('do12'):
            do_steps(g)
        with scope('q12'):
            q_steps(g)
    with scope('relkv2'):
        for i in range(4):
            wait_slot(8 + i)
            relay_kv(wk_r, 4 - 4 * q, i, 8 + i)
            wait_slot(i)
            relay_kv(wv_r, 4 - 4 * q, i, i)

    def wait_unit(u):
        part = recv.at[u, pl.ds(0, SEQ - ROWS)]
        pltpu.make_async_copy(part, part, recv_sem.at[u]).wait()

    with scope('waitkv'):
        wait_unit(U_K)
        wait_unit(U_V)
    def segs(b):
        out = []
        for seg in range(4 * b, 4 * b + 4):
            row = seg * TOK if seg < N_DEV else (2 * N_DEV - 1 - seg) * TOK + SEG
            out.append(slice(row, row + SEG))
        return out

    def pos_block(u, b):
        return jnp.concatenate([recv[u, r, :] for r in segs(b)], axis=0)

    def put_block(u, b, val):
        for n, r in enumerate(segs(b)):
            obuf[u, r, :] = val[n * SEG:(n + 1) * SEG]

    for b in range(NB):
        kt[:, b * BQ:(b + 1) * BQ] = pos_block(U_K, b).T
        vt[:, b * BQ:(b + 1) * BQ] = pos_block(U_V, b).T

    def send_out(u):
        slot = G * chip + u
        for k in range(1, N_CHIP):
            pltpu.make_async_remote_copy(
                src_ref=obuf.at[u, chip_rows(peer(k))], dst_ref=rin.at[slot],
                send_sem=osend_sem, recv_sem=orecv_sem.at[u],
                device_id=dev_of(peer(k)), device_id_type=MESH).start()
        rin[slot] = obuf[u, chip_rows(chip), :]

    def attn_head(g, _):
        with scope('waitq'):
            wait_unit(U_DO + g)
            wait_unit(U_Q + g)
        st = [{} for _ in range(NB)]

        def chunks(b):
            return [slice(k * BQ, (k + 1) * BQ) for k in range(b + 1)]

        def scores(b):
            qb = pos_block(U_Q + g, b)
            dob = pos_block(U_DO + g, b)
            mx = None
            for kc, ks in enumerate(chunks(b)):
                s = dot_nt(pos_block(U_K, kc), qb)
                if kc == b:
                    key = lax.broadcasted_iota(jnp.int32, (BQ, BQ), 0)
                    qry = lax.broadcasted_iota(jnp.int32, (BQ, BQ), 1)
                    s = jnp.where(key <= qry, s, -jnp.inf)
                s_scr[b][ks, :] = s
                mc = jnp.max(s.reshape(BQ // 8, 8, BQ), axis=0)
                mx = mc if mx is None else jnp.maximum(mx, mc)
            for kc, ks in enumerate(chunks(b)):
                dp_scr[b][ks, :] = dot_nt(pos_block(U_V, kc), dob)
            st[b]['m2'] = jnp.max(mx, axis=0, keepdims=True) * C2

        def probs(b):
            m2 = st[b]['m2']
            ls = None
            for ks in chunks(b):
                e = jnp.exp2(s_scr[b][ks, :] * C2 - m2)
                lc = jnp.sum(e.reshape(BQ // 8, 8, BQ), axis=0)
                ls = lc if ls is None else ls + lc
            lse2 = m2 + jnp.log2(jnp.sum(ls, axis=0, keepdims=True))
            for ks in chunks(b):
                p_scr[b][ks, :] = jnp.exp2(s_scr[b][ks, :] * C2 - lse2).astype(BF16)

        def outs(b):
            n = (b + 1) * BQ
            dob = pos_block(U_DO + g, b)
            ot = dot(vt[:, :n], p_scr[b][...]).astype(BF16)
            st[b]['delta'] = jnp.sum(dob.T.astype(F32) * ot.astype(F32), axis=0, keepdims=True)
            for ks in chunks(b):
                dv_acc[ks, :] += dot(p_scr[b][ks, :], dob)

        def dscores(b):
            delta = st[b]['delta']
            for ks in chunks(b):
                ds_scr[b][ks, :] = (p_scr[b][ks, :].astype(F32) * (dp_scr[b][ks, :] - delta)).astype(BF16)

        def grads(b):
            n = (b + 1) * BQ
            qb = pos_block(U_Q + g, b)
            for ks in chunks(b):
                dk_acc[ks, :] += dot(ds_scr[b][ks, :], qb)
            dqt = (dot(kt[:, :n], ds_scr[b][...]) * C).astype(BF16)
            put_block(g, b, dqt.T)

        with scope('attn'):
            scores(3)
            scores(2)
            probs(3)
            outs(3)
            scores(1)
            dscores(3)
            probs(2)
            grads(3)
            outs(2)
            scores(0)
            dscores(2)
            probs(1)
            grads(2)
            outs(1)
            dscores(1)
            probs(0)
            grads(1)
            outs(0)
            dscores(0)
            grads(0)

        with scope('send'):
            send_out(g)
        return 0

    lax.fori_loop(0, G, attn_head, 0)
    def send_owners(n):
        slot = 8 * n + 4 * q + chip

        def send_dev(dev, part):
            pltpu.make_async_remote_copy(
                src_ref=obuf.at[G + n, tok_rows(dev)], dst_ref=rkv.at[slot],
                send_sem=osend_sem, recv_sem=kv_sem.at[n, part],
                device_id=(dp, dev), device_id_type=MESH).start()

        send_dev(partner[1], 0)
        for k in range(1, N_CHIP):
            for r in range(2):
                send_dev(2 * peer(k) + r, k if n == 1 else 1)
        rkv[slot] = obuf[G + n, tok_rows(me), :]

    with scope('senddkv'):
        for b in range(NB):
            put_block(3, b, (dk_acc[b * BQ:(b + 1) * BQ, :] * C).astype(BF16))
        send_owners(0)
        for b in range(NB):
            put_block(4, b, dv_acc[b * BQ:(b + 1) * BQ, :].astype(BF16))
        send_owners(1)

    def p_copy():
        return pltpu.make_async_remote_copy(
            src_ref=acc.at[other], dst_ref=pbuf, send_sem=ps_sem, recv_sem=pr_sem,
            device_id=partner, device_id_type=MESH)

    def wait_kv(n, part, count):
        ref = obuf.at[0, pl.ds(0, count * TOK)]
        pltpu.make_async_copy(ref, ref, kv_sem.at[n, part]).wait()

    def kv_dx(items, last=False):
        lhs, rhs = [], []
        for n, k in items:
            c = lax.rem(chip + N_CHIP - k, N_CHIP)
            for r in range(2):
                lhs.append(rkv[8 * n + 4 * r + c])
                rhs.append((wk_r, wv_r)[n][4 * r + c])
        t = dot_nt(jnp.concatenate(lhs, axis=1), jnp.concatenate(rhs, axis=1)) + acc[own, :]
        if last:
            out_ref[...] = (t + pbuf[...]).astype(BF16)
        else:
            acc[own, :] = t

    for u in range(G):
        with scope('waito'):
            part = obuf.at[u, pl.ds(0, SEQ - ROWS)]
            pltpu.make_async_copy(part, part, orecv_sem.at[u]).wait()
        with scope('dx'):
            t = dot_nt(jnp.concatenate([rin[G * j + u] for j in range(N_CHIP)], axis=1),
                       jnp.concatenate([wq_r[G * j + u] for j in range(N_CHIP)], axis=1))
            acc[...] = t if u == 0 else t + acc[...]
        if u == 0:
            with scope('kvlocal'):
                wait_kv(0, 0, 1)
                wait_kv(1, 0, 1)
                kv_dx([(0, 0), (1, 0)])
    p_copy().start()

    with scope('waitk'):
        wait_kv(0, 1, 6)
    with scope('kdx'):
        kv_dx([(0, 1), (0, 2), (0, 3)])
    for k in (1, 2):
        with scope('waitv%d' % k):
            wait_kv(1, k, 2)
        with scope('vdx%d' % k):
            kv_dx([(1, k)])
    with scope('waitv3'):
        wait_kv(1, 3, 2)
    with scope('waitp'):
        p_copy().wait_recv()
    with scope('vdx3'):
        kv_dx([(1, 3)], last=True)

    with scope('final'):
        for n in range(2):
            swap_copy(n).wait_send()
        p_copy().wait_send()
        pltpu.make_async_copy(sbuf, sbuf, send_sem).wait()
        part = obuf.at[pl.ds(0, G), pl.ds(0, SEQ - ROWS)]
        pltpu.make_async_copy(part, part, osend_sem).wait()
        part = obuf.at[pl.ds(0, 2), pl.ds(0, SEQ - TOK)]
        pltpu.make_async_copy(part, part, osend_sem).wait()


def solution(mesh):
    row_spec = P(("dp", "cp"), None)

    def device_fn(x_in, d_y, w_q, w_k, w_v, w_o):
        dma = pltpu.SemaphoreType.DMA
        res = pl.pallas_call(
            kernel,
            out_shape=pltpu.VMEM((TOK, D), BF16),
            in_specs=[pl.BlockSpec(memory_space=pl.ANY)] * 6,
            out_specs=pl.BlockSpec(memory_space=pltpu.VMEM),
            scratch_shapes=[
                pltpu.VMEM((ROWS, D), BF16),
                pltpu.VMEM((ROWS, D), BF16),
                pltpu.VMEM((2, N_CHIP, HD, D), BF16),
                pltpu.VMEM((SLOTS, 256, 3, 4, HD), BF16),
                pltpu.VMEM((12, D, HD), BF16),
                pltpu.VMEM((8, D, HD), BF16),
                pltpu.VMEM((8, D, HD), BF16),
                pltpu.VMEM((8, 3, ROWS, HD), BF16),
                pltpu.VMEM((8, SEQ, HD), BF16),
                pltpu.VMEM((5, SEQ, HD), BF16),
                pltpu.VMEM((12, ROWS, HD), BF16),
                pltpu.VMEM((16, TOK, HD), BF16),
                pltpu.VMEM((ROWS, D), F32),
                pltpu.VMEM((TOK, D), F32),
                *[pltpu.VMEM(((b + 1) * BQ, BQ), t) for t in (F32, F32, BF16, BF16) for b in range(NB)],
                pltpu.VMEM((HD, SEQ), BF16),
                pltpu.VMEM((HD, SEQ), BF16),
                pltpu.VMEM((SEQ, HD), F32),
                pltpu.VMEM((SEQ, HD), F32),
                dma((2,)), dma((2, N_CHIP)), dma((SLOTS,)), dma((2,)), dma((2,)),
                dma, dma((8,)), dma, dma((G,)), dma((2, 4)), dma, dma,
            ],
            compiler_params=pltpu.CompilerParams(
                collective_id=0, has_side_effects=True, vmem_limit_bytes=VLIM),
        )(x_in, d_y, w_q.reshape(12, 256, 6, 4, HD), w_k.reshape(4, 256, 3, 2, 4, HD), w_v.reshape(4, 256, 3, 2, 4, HD),
          w_o.reshape(2, N_CHIP, G, HD, D))
        return res

    return jax.shard_map(device_fn, mesh=mesh, in_specs=(row_spec, row_spec, P(), P(), P(), P()),
                         out_specs=row_spec, check_vma=False)
```

```python
import math

import jax
import jax.numpy as jnp
from jax import lax
from jax.experimental import pallas as pl
from jax.experimental.pallas import tpu as pltpu
from jax.sharding import PartitionSpec as P

MESH = pl.DeviceIdType.MESH
BF16, F32 = jnp.bfloat16, jnp.float32
NT = (((1,), (1,)), ((), ()))

N_DEV, N_CHIP, TOK, SEG = 8, 4, 128, 64
ROWS = 2 * TOK
SEQ = N_DEV * TOK
D = 3072
HD = 128
G = 3
BQ = 256
NB = SEQ // BQ
C = HD**-0.5
C2 = C * math.log2(math.e)
U_DO, U_K, U_V, U_Q = 0, 3, 4, 5
SLOTS = 12
RB = 128
ND = 3072
NV = 3072
VLIM = 66_000_000

scope = jax.named_scope


def dot_nt(a, b):
    return lax.dot_general(a, b, NT, preferred_element_type=F32)


def dot(a, b):
    return jnp.dot(a, b, preferred_element_type=F32)


def kernel(x_hbm, dy_hbm, wq_hbm, wk_hbm, wv_hbm, wo_hbm, out_ref,
           x_v, dy_v, wo_s, w_s, wq_r, wk_r, wv_r, sbuf, recv, obuf, rin, rkv, acc, pbuf,
           s0, s1, s2, s3, d0, d1, d2, d3, p0, p1, p2, p3, e0, e1, e2, e3, kt, vt, dk_acc, dv_acc,
           io_sem, wo_sem, w_sem, xs_sem, xr_sem, send_sem, recv_sem, osend_sem, orecv_sem, kv_sem, ps_sem, pr_sem):
    s_scr, dp_scr, p_scr, ds_scr = (s0, s1, s2, s3), (d0, d1, d2, d3), (p0, p1, p2, p3), (e0, e1, e2, e3)
    me = lax.axis_index("cp")
    dp = lax.axis_index("dp")
    chip = me // 2
    q = lax.rem(me, 2)
    partner = (dp, 2 * chip + 1 - q)

    def peer(k):
        return lax.rem(chip + k, N_CHIP)

    def dev_of(cc):
        return (dp, 2 * cc + q)

    barrier = pltpu.get_barrier_semaphore()
    pl.semaphore_signal(barrier, inc=1, device_id=partner, device_id_type=MESH)
    for k in range(1, N_CHIP):
        pl.semaphore_signal(barrier, inc=1, device_id=dev_of(peer(k)), device_id_type=MESH)

    def tok_rows(i):
        return pl.ds(pl.multiple_of(i * TOK, TOK), TOK)

    def chip_rows(i):
        return pl.ds(pl.multiple_of(i * ROWS, ROWS), ROWS)

    own, other = tok_rows(q), tok_rows(1 - q)

    def io_copy(n):
        src, dst = ((dy_hbm, dy_v), (x_hbm, x_v))[n]
        return pltpu.make_async_copy(src, dst.at[own], io_sem.at[n])

    def swap_copy(n):
        ref = (dy_v, x_v)[n]
        return pltpu.make_async_remote_copy(
            src_ref=ref.at[own], dst_ref=ref.at[own], send_sem=xs_sem.at[n], recv_sem=xr_sem.at[n],
            device_id=partner, device_id_type=MESH)

    def wo_copy(g, k):
        return pltpu.make_async_copy(wo_hbm.at[q, peer(k), g], wo_s.at[g % 2, k - 1], wo_sem.at[g % 2, k - 1])

    def wkv_copy(w_hbm, i, slot, half=None):
        half = q if half is None else half
        return pltpu.make_async_copy(w_hbm.at[i, :, :, half], w_s.at[slot], w_sem.at[slot])

    def wq_copy(i, slot):
        return pltpu.make_async_copy(wq_hbm.at[i, :, pl.ds(3 * q, 3)], w_s.at[slot], w_sem.at[slot])

    def wait_slot(slot):
        wkv_copy(wk_hbm, 0, slot).wait()

    io_copy(0).start()
    io_copy(1).start()
    for k in (1, 2):
        wo_copy(0, k).start()
    dk_acc[...] = jnp.zeros_like(dk_acc)
    dv_acc[...] = jnp.zeros_like(dv_acc)
    with scope('barrier'):
        pl.semaphore_wait(barrier, N_CHIP)
    for i in range(4):
        wkv_copy(wk_hbm, i, i).start()
    with scope('swapx'):
        io_copy(1).wait()
        swap_copy(1).start()
        io_copy(0).wait()

    def relay_kv(dst, base, i, slot):
        flat = w_s.at[slot].reshape(768 * 4, HD)
        for h in range(4):
            for r in range(0, 768, RB):
                dst[base + h, pl.ds(i * 768 + r, RB), :] = flat[pl.ds(4 * r + h, RB, stride=4), :]

    def relay_q(i, slot):
        flat = w_s.at[slot].reshape(768 * 4, HD)
        for h in range(12):
            for r in range(0, 256, RB):
                wq_r[h, pl.ds(i * 256 + r, RB), :] = flat[pl.ds(12 * r + h, RB, stride=12), :]


    def send_part(unit, k, val, rows, dst_rows):
        if k == N_CHIP:
            recv[unit, dst_rows, :] = val
            return
        sbuf[unit, k - 1, rows, :] = val
        pltpu.make_async_remote_copy(
            src_ref=sbuf.at[unit, k - 1, rows], dst_ref=recv.at[unit, dst_rows],
            send_sem=send_sem, recv_sem=recv_sem.at[unit],
            device_id=dev_of(peer(k)), device_id_type=MESH).start()

    def send_rows(unit, k, val, r):
        send_part(unit, k, val, tok_rows(r), tok_rows(2 * chip + r))

    def send_block(unit, k, val):
        send_part(unit, k, val, pl.ds(0, ROWS), chip_rows(chip))

    def do0_rows(r, ks):
        w = wo_s[0, pl.ds(ks[0] - 1, len(ks))].reshape(len(ks) * HD, D)
        val = dot_nt(dy_v[tok_rows(r), :], w).astype(BF16)
        for n, k in enumerate(ks):
            send_rows(U_DO, k, val[:, n * HD:(n + 1) * HD], r)

    def do_steps(g):
        for k in range(1, 5):
            wo_copy(g, k).wait()
        val = dot_nt(dy_v[...], wo_s[g % 2].reshape(4 * HD, D)).astype(BF16)
        for k in range(1, 5):
            send_block(U_DO + g, k, val[:, (k - 1) * HD:k * HD])

    def k_rows(r):
        w = jnp.concatenate([wk_r[4 * q + peer(k)] for k in range(1, 5)], axis=1)
        val = dot(x_v[tok_rows(r), :], w).astype(BF16)
        for k in range(1, 5):
            send_rows(U_K, k, val[:, (k - 1) * HD:k * HD], r)

    def v_steps():
        w = jnp.concatenate([wv_r[4 * q + peer(k)] for k in range(1, 5)], axis=1)
        val = dot(x_v[...], w).astype(BF16)
        for k in range(1, 5):
            send_block(U_V, k, val[:, (k - 1) * HD:k * HD])

    def q_steps(g):
        w = jnp.concatenate([wq_r[3 * peer(k) + g] for k in range(1, 5)], axis=1)
        val = dot(x_v[...], w).astype(BF16)
        for k in range(1, 5):
            send_block(U_Q + g, k, val[:, (k - 1) * HD:k * HD])

    with scope('do0a'):
        for k in (1, 2):
            wo_copy(0, k).wait()
        do0_rows(q, (1, 2))
    for i in range(4):
        wkv_copy(wv_hbm, i, 4 + i).start()
    with scope('relk'):
        for i in range(4):
            wait_slot(i)
            relay_kv(wk_r, 4 * q, i, i)
    for k in (3, 4):
        wo_copy(0, k).start()
    with scope('k_own'):
        k_rows(q)
    swap_copy(0).start()
    with scope('xswap'):
        swap_copy(1).wait_recv()
    with scope('k_other'):
        k_rows(1 - q)
    with scope('relv'):
        for i in range(4):
            wait_slot(4 + i)
            relay_kv(wv_r, 4 * q, i, 4 + i)
    for i in range(4):
        wq_copy(i, 8 + i).start()
    with scope('v'):
        v_steps()
    for i in range(4):
        wq_copy(4 + i, i).start()
    with scope('do0b'):
        for k in (3, 4):
            wo_copy(0, k).wait()
        do0_rows(q, (3, 4))
    for i in range(4):
        wq_copy(8 + i, 4 + i).start()
    with scope('dyswap'):
        swap_copy(0).wait_recv()
    with scope('do0c'):
        do0_rows(1 - q, (1, 2, 3, 4))
    for k in range(1, 5):
        wo_copy(1, k).start()
    with scope('relq'):
        for i in range(12):
            slot = (8 + i) % SLOTS
            wait_slot(slot)
            relay_q(i, slot)
    for k in range(1, 5):
        wo_copy(2, k).start()
    with scope('q0'):
        q_steps(0)
    for i in range(8):
        wkv_copy((wk_hbm, wv_hbm)[i // 4], i % 4, (8 + i) % SLOTS, 1 - q).start()
    for g in (1, 2):
        with scope('do12'):
            do_steps(g)
        with scope('q12'):
            q_steps(g)
    with scope('relkv2'):
        for i in range(4):
            wait_slot(8 + i)
            relay_kv(wk_r, 4 - 4 * q, i, 8 + i)
            wait_slot(i)
            relay_kv(wv_r, 4 - 4 * q, i, i)

    def wait_unit(u):
        part = recv.at[u, pl.ds(0, SEQ - ROWS)]
        pltpu.make_async_copy(part, part, recv_sem.at[u]).wait()

    with scope('waitkv'):
        wait_unit(U_K)
        wait_unit(U_V)
    def segs(b):
        out = []
        for seg in range(4 * b, 4 * b + 4):
            row = seg * TOK if seg < N_DEV else (2 * N_DEV - 1 - seg) * TOK + SEG
            out.append(slice(row, row + SEG))
        return out

    def pos_block(u, b):
        return jnp.concatenate([recv[u, r, :] for r in segs(b)], axis=0)

    def put_block(u, b, val):
        for n, r in enumerate(segs(b)):
            obuf[u, r, :] = val[n * SEG:(n + 1) * SEG]

    for b in range(NB):
        kt[:, b * BQ:(b + 1) * BQ] = pos_block(U_K, b).T
        vt[:, b * BQ:(b + 1) * BQ] = pos_block(U_V, b).T

    def send_out(u):
        slot = G * chip + u
        for k in range(1, N_CHIP):
            pltpu.make_async_remote_copy(
                src_ref=obuf.at[u, chip_rows(peer(k))], dst_ref=rin.at[slot],
                send_sem=osend_sem, recv_sem=orecv_sem.at[u],
                device_id=dev_of(peer(k)), device_id_type=MESH).start()
        rin[slot] = obuf[u, chip_rows(chip), :]

    def attn_head(g, _):
        with scope('waitq'):
            wait_unit(U_DO + g)
            wait_unit(U_Q + g)
        st = [{} for _ in range(NB)]

        def chunks(b):
            return [slice(k * BQ, (k + 1) * BQ) for k in range(b + 1)]

        def scores(b):
            qb = pos_block(U_Q + g, b)
            dob = pos_block(U_DO + g, b)
            mx = None
            for kc, ks in enumerate(chunks(b)):
                s = dot_nt(pos_block(U_K, kc), qb)
                if kc == b:
                    key = lax.broadcasted_iota(jnp.int32, (BQ, BQ), 0)
                    qry = lax.broadcasted_iota(jnp.int32, (BQ, BQ), 1)
                    s = jnp.where(key <= qry, s, -jnp.inf)
                s_scr[b][ks, :] = s
                mc = jnp.max(s.reshape(BQ // 8, 8, BQ), axis=0)
                mx = mc if mx is None else jnp.maximum(mx, mc)
            for kc, ks in enumerate(chunks(b)):
                dp_scr[b][ks, :] = dot_nt(pos_block(U_V, kc), dob)
            st[b]['m2'] = jnp.max(mx, axis=0, keepdims=True) * C2

        def probs(b):
            m2 = st[b]['m2']
            ls = None
            for ks in chunks(b):
                e = jnp.exp2(s_scr[b][ks, :] * C2 - m2)
                lc = jnp.sum(e.reshape(BQ // 8, 8, BQ), axis=0)
                ls = lc if ls is None else ls + lc
            lse2 = m2 + jnp.log2(jnp.sum(ls, axis=0, keepdims=True))
            for ks in chunks(b):
                p_scr[b][ks, :] = jnp.exp2(s_scr[b][ks, :] * C2 - lse2).astype(BF16)

        def outs(b):
            n = (b + 1) * BQ
            dob = pos_block(U_DO + g, b)
            ot = dot(vt[:, :n], p_scr[b][...]).astype(BF16)
            st[b]['delta'] = jnp.sum(dob.T.astype(F32) * ot.astype(F32), axis=0, keepdims=True)
            for ks in chunks(b):
                dv_acc[ks, :] += dot(p_scr[b][ks, :], dob)

        def dscores(b):
            delta = st[b]['delta']
            for ks in chunks(b):
                ds_scr[b][ks, :] = (p_scr[b][ks, :].astype(F32) * (dp_scr[b][ks, :] - delta)).astype(BF16)

        def grads(b):
            n = (b + 1) * BQ
            qb = pos_block(U_Q + g, b)
            for ks in chunks(b):
                dk_acc[ks, :] += dot(ds_scr[b][ks, :], qb)
            dqt = (dot(kt[:, :n], ds_scr[b][...]) * C).astype(BF16)
            put_block(g, b, dqt.T)

        with scope('attn'):
            scores(3)
            scores(2)
            probs(3)
            outs(3)
            scores(1)
            dscores(3)
            probs(2)
            grads(3)
            outs(2)
            scores(0)
            dscores(2)
            probs(1)
            grads(2)
            outs(1)
            dscores(1)
            probs(0)
            grads(1)
            outs(0)
            dscores(0)
            grads(0)

        with scope('send'):
            send_out(g)
        return 0

    lax.fori_loop(0, G, attn_head, 0)
    def send_owners(n):
        slot = 8 * n + 4 * q + chip

        def send_dev(dev, part):
            pltpu.make_async_remote_copy(
                src_ref=obuf.at[G + n, tok_rows(dev)], dst_ref=rkv.at[slot],
                send_sem=osend_sem, recv_sem=kv_sem.at[n, part],
                device_id=(dp, dev), device_id_type=MESH).start()

        send_dev(partner[1], 0)
        for k in range(1, N_CHIP):
            for r in range(2):
                send_dev(2 * peer(k) + r, k if n == 1 else 1)
        rkv[slot] = obuf[G + n, tok_rows(me), :]

    with scope('senddkv'):
        for b in range(NB):
            put_block(3, b, (dk_acc[b * BQ:(b + 1) * BQ, :] * C).astype(BF16))
        send_owners(0)
        for b in range(NB):
            put_block(4, b, dv_acc[b * BQ:(b + 1) * BQ, :].astype(BF16))
        send_owners(1)

    def p_copy():
        return pltpu.make_async_remote_copy(
            src_ref=acc.at[other], dst_ref=pbuf, send_sem=ps_sem, recv_sem=pr_sem,
            device_id=partner, device_id_type=MESH)

    def wait_kv(n, part, count):
        ref = obuf.at[0, pl.ds(0, count * TOK)]
        pltpu.make_async_copy(ref, ref, kv_sem.at[n, part]).wait()

    def kv_dx(items, last=False):
        lhs, rhs = [], []
        for n, k in items:
            c = lax.rem(chip + N_CHIP - k, N_CHIP)
            for r in range(2):
                lhs.append(rkv[8 * n + 4 * r + c])
                rhs.append((wk_r, wv_r)[n][4 * r + c])
        t = dot_nt(jnp.concatenate(lhs, axis=1), jnp.concatenate(rhs, axis=1)) + acc[own, :]
        if last:
            out_ref[...] = (t + pbuf[...]).astype(BF16)
        else:
            acc[own, :] = t

    for u in range(G):
        with scope('waito'):
            part = obuf.at[u, pl.ds(0, SEQ - ROWS)]
            pltpu.make_async_copy(part, part, orecv_sem.at[u]).wait()
        with scope('dx'):
            t = dot_nt(jnp.concatenate([rin[G * j + u] for j in range(N_CHIP)], axis=1),
                       jnp.concatenate([wq_r[G * j + u] for j in range(N_CHIP)], axis=1))
            acc[...] = t if u == 0 else t + acc[...]
        if u == 0:
            with scope('kvlocal'):
                wait_kv(0, 0, 1)
                wait_kv(1, 0, 1)
                kv_dx([(0, 0), (1, 0)])
    p_copy().start()

    with scope('waitk'):
        wait_kv(0, 1, 6)
    with scope('kdx'):
        kv_dx([(0, 1), (0, 2), (0, 3)])
    for k in (1, 2):
        with scope('waitv%d' % k):
            wait_kv(1, k, 2)
        with scope('vdx%d' % k):
            kv_dx([(1, k)])
    with scope('waitv3'):
        wait_kv(1, 3, 2)
    with scope('waitp'):
        p_copy().wait_recv()
    with scope('vdx3'):
        kv_dx([(1, 3)], last=True)

    with scope('final'):
        for n in range(2):
            swap_copy(n).wait_send()
        p_copy().wait_send()
        pltpu.make_async_copy(sbuf, sbuf, send_sem).wait()
        part = obuf.at[pl.ds(0, G), pl.ds(0, SEQ - ROWS)]
        pltpu.make_async_copy(part, part, osend_sem).wait()
        part = obuf.at[pl.ds(0, 2), pl.ds(0, SEQ - TOK)]
        pltpu.make_async_copy(part, part, osend_sem).wait()


def solution(mesh):
    row_spec = P(("dp", "cp"), None)

    def device_fn(x_in, d_y, w_q, w_k, w_v, w_o):
        dma = pltpu.SemaphoreType.DMA
        res = pl.pallas_call(
            kernel,
            out_shape=pltpu.VMEM((TOK, D), BF16),
            in_specs=[pl.BlockSpec(memory_space=pl.ANY)] * 6,
            out_specs=pl.BlockSpec(memory_space=pltpu.VMEM),
            scratch_shapes=[
                pltpu.VMEM((ROWS, D), BF16),
                pltpu.VMEM((ROWS, D), BF16),
                pltpu.VMEM((2, N_CHIP, HD, D), BF16),
                pltpu.VMEM((SLOTS, 256, 3, 4, HD), BF16),
                pltpu.VMEM((12, D, HD), BF16),
                pltpu.VMEM((8, D, HD), BF16),
                pltpu.VMEM((8, D, HD), BF16),
                pltpu.VMEM((8, 3, ROWS, HD), BF16),
                pltpu.VMEM((8, SEQ, HD), BF16),
                pltpu.VMEM((5, SEQ, HD), BF16),
                pltpu.VMEM((12, ROWS, HD), BF16),
                pltpu.VMEM((16, TOK, HD), BF16),
                pltpu.VMEM((ROWS, D), F32),
                pltpu.VMEM((TOK, D), F32),
                *[pltpu.VMEM(((b + 1) * BQ, BQ), t) for t in (F32, F32, BF16, BF16) for b in range(NB)],
                pltpu.VMEM((HD, SEQ), BF16),
                pltpu.VMEM((HD, SEQ), BF16),
                pltpu.VMEM((SEQ, HD), F32),
                pltpu.VMEM((SEQ, HD), F32),
                dma((2,)), dma((2, N_CHIP)), dma((SLOTS,)), dma((2,)), dma((2,)),
                dma, dma((8,)), dma, dma((G,)), dma((2, 4)), dma, dma,
            ],
            compiler_params=pltpu.CompilerParams(
                collective_id=0, has_side_effects=True, vmem_limit_bytes=VLIM),
        )(x_in, d_y, w_q.reshape(12, 256, 6, 4, HD), w_k.reshape(4, 256, 3, 2, 4, HD), w_v.reshape(4, 256, 3, 2, 4, HD),
          w_o.reshape(2, N_CHIP, G, HD, D))
        return res

    return jax.shard_map(device_fn, mesh=mesh, in_specs=(row_spec, row_spec, P(), P(), P(), P()),
                         out_specs=row_spec, check_vma=False)
```
